32 devices in a mesh: gx: 4 (over z), gy: 4 (over y, x), gz: 2 (over core).
Axes of the slice: x: 2, y: 2, z: 4, core: 2. Of those that a mesh axis runs over, the one named last changes fastest.
Arguments:
- chi_field: float32 [32, 128, 256], P('gx', 'gy', 'gz'), may hold values from 0.5 to 2.5, as said below
- metric: float32 [6, 32, 128, 256], P(None, 'gx', 'gy', 'gz'), may hold values from -0.3 to 1.5, as said below
- curvature: float32 [6, 32, 128, 256], P(None, 'gx', 'gy', 'gz'), may hold values from -1.6 to 1.6
- trace_curvature: float32 [32, 128, 256], P('gx', 'gy', 'gz'), may hold values from -3 to 3
- gamma_field: float32 [3, 32, 128, 256], P(None, 'gx', 'gy', 'gz'), may hold values from -1.6 to 1.6
Outputs:
- hamiltonian: float32 [32, 128, 256], P('gx', 'gy', 'gz')
- momentum: float32 [3, 32, 128, 256], P(None, 'gx', 'gy', 'gz')
- constraint_norms: float32 [2], replicated
The draws below stay inside these ranges and needn't reach their ends.
Inputs may be any that keep to these rules, and one draw needn't show every extreme that they name: `chi_field`: positive. `metric`: at every cell the symmetric 3x3 matrix built from the six components is positive definite with a dominant diagonal.
All inputs are finite; a program needn't handle non-finite values.
Results may differ from the reference program's by a relative error of at most 0.0003.
Values sent between devices are 32-bit elements; how exact they have to be, the bound alone decides.
A program may use at most 128 MiB of HBM per device.

```python
import math
import jax
import jax.numpy as jnp
from jax import lax

CX = 8
NX = 32
NY = 128
NZ = 256
N_GX = 4


def ramp_level():
    xs = jnp.arange(NX, dtype=jnp.float32) / NX
    ys = jnp.arange(NY, dtype=jnp.float32) / NY
    zs = jnp.arange(NZ, dtype=jnp.float32) / NZ
    level = (xs[:, None, None] + ys[None, :, None] + zs[None, None, :]) / 3.0
    return jnp.exp(math.log(3.0) * level)


def draw_chi_field(key, part):
    noise = jax.random.uniform(key, (NX, NY, NZ), jnp.float32, -1.0, 1.0)
    value = 0.12 * ramp_level() * noise
    return jnp.exp(value)


def draw_metric(key, part):
    noise = jax.random.uniform(key, (6, NX, NY, NZ), jnp.float32, -1.0, 1.0)
    identity = jnp.array([1.0, 0.0, 0.0, 1.0, 0.0, 1.0], dtype=jnp.float32)[:, None, None, None]
    value = 0.05 * ramp_level()[None] * noise
    return identity + value


def draw_curvature(key, part):
    noise = jax.random.uniform(key, (6, NX, NY, NZ), jnp.float32, -1.0, 1.0)
    return 0.3 * ramp_level()[None] * noise


def draw_trace_curvature(key, part):
    noise = jax.random.uniform(key, (NX, NY, NZ), jnp.float32, -1.0, 1.0)
    value = 0.5 * ramp_level() * noise
    return value


def draw_gamma_field(key, part):
    noise = jax.random.uniform(key, (3, NX, NY, NZ), jnp.float32, -1.0, 1.0)
    return 0.3 * ramp_level()[None] * noise


def setup_inputs(seed: int = 0) -> dict:
    keys = jax.random.split(jax.random.key(seed), 6)
    return {
        "chi_field": draw_chi_field(jax.random.fold_in(keys[5], 71), 0),
        "metric": draw_metric(jax.random.fold_in(keys[5], 71), 0),
        "curvature": draw_curvature(jax.random.fold_in(keys[5], 71), 0),
        "trace_curvature": draw_trace_curvature(jax.random.fold_in(keys[5], 71), 0),
        "gamma_field": draw_gamma_field(jax.random.fold_in(keys[5], 71), 0),
    }


pair_index = ((0, 1, 2), (1, 3, 4), (2, 4, 5))
first_taps = ((-2, 1.0 / 12.0), (-1, -8.0 / 12.0), (1, 8.0 / 12.0), (2, -1.0 / 12.0))
second_taps = ((-2, -1.0 / 12.0), (-1, 16.0 / 12.0), (0, -30.0 / 12.0), (1, 16.0 / 12.0), (2, -1.0 / 12.0))

def window(padded, offsets):
    sx = padded.shape[-3] - 4
    sy = padded.shape[-2] - 4
    sz = padded.shape[-1] - 4
    return padded[..., 2 + offsets[0]:2 + offsets[0] + sx, 2 + offsets[1]:2 + offsets[1] + sy, 2 + offsets[2]:2 + offsets[2] + sz]

def shifted(pairs):
    places = [0, 0, 0]
    for axis_num, step in pairs:
        places[axis_num] = places[axis_num] + step
    return tuple(places)

def first_diff(padded, axis_num):
    summed = None
    for step, weight in first_taps:
        term = weight * window(padded, shifted(((axis_num, step),)))
        summed = term if summed is None else summed + term
    return summed

def second_diff(padded, a, b):
    summed = None
    if a == b:
        for step, weight in second_taps:
            term = weight * window(padded, shifted(((a, step),)))
            summed = term if summed is None else summed + term
        return summed
    for step_a, weight_a in first_taps:
        for step_b, weight_b in first_taps:
            term = weight_a * weight_b * window(padded, shifted(((a, step_a), (b, step_b))))
            summed = term if summed is None else summed + term
    return summed

def constraints(geo_pad, rest_pad):
    centre = window(geo_pad, (0, 0, 0))
    remainder = window(rest_pad, (0, 0, 0))
    conformal = centre[0]
    trace_curv = remainder[6]
    geo_first = [first_diff(geo_pad, a) for a in range(3)]
    rest_first = [first_diff(rest_pad, a) for a in range(3)]
    geo_second = {}
    for a in range(3):
        for b in range(a, 3):
            geo_second[a, b] = second_diff(geo_pad, a, b)

    def metric_at(i, j):
        return centre[1 + pair_index[i][j]]

    def curv_at(i, j):
        return remainder[pair_index[i][j]]

    def metric_grad(i, j, a):
        return geo_first[a][1 + pair_index[i][j]]

    def metric_hess(i, j, a, b):
        return geo_second[min(a, b), max(a, b)][1 + pair_index[i][j]]

    def chi_hess(a, b):
        return geo_second[min(a, b), max(a, b)][0]

    def curv_grad(i, j, a):
        return rest_first[a][pair_index[i][j]]
    chi_grad = [geo_first[a][0] for a in range(3)]
    trace_grad = [rest_first[a][6] for a in range(3)]
    g00, g01, g02 = (metric_at(0, 0), metric_at(0, 1), metric_at(0, 2))
    g11, g12, g22 = (metric_at(1, 1), metric_at(1, 2), metric_at(2, 2))
    minor00 = g11 * g22 - g12 * g12
    minor01 = g02 * g12 - g01 * g22
    minor02 = g01 * g12 - g02 * g11
    minor11 = g00 * g22 - g02 * g02
    minor12 = g01 * g02 - g00 * g12
    minor22 = g00 * g11 - g01 * g01
    determinant = g00 * minor00 + g01 * minor01 + g02 * minor02
    scale = 1.0 / determinant
    inverse_list = [minor00 * scale, minor01 * scale, minor02 * scale, minor11 * scale, minor12 * scale, minor22 * scale]

    def inv_at(i, j):
        return inverse_list[pair_index[i][j]]
    christ_low = [[[None] * 3 for i in range(3)] for k in range(3)]
    for k in range(3):
        for i in range(3):
            for j in range(i, 3):
                value = 0.5 * (metric_grad(k, j, i) + metric_grad(k, i, j) - metric_grad(i, j, k))
                christ_low[k][i][j] = value
                christ_low[k][j][i] = value
    christ_up = [[[None] * 3 for i in range(3)] for k in range(3)]
    for k in range(3):
        for i in range(3):
            for j in range(i, 3):
                value = inv_at(k, 0) * christ_low[0][i][j] + inv_at(k, 1) * christ_low[1][i][j] + inv_at(k, 2) * christ_low[2][i][j]
                christ_up[k][i][j] = value
                christ_up[k][j][i] = value
    gamma_calc = []
    for k in range(3):
        summed = None
        for i in range(3):
            for j in range(3):
                term = inv_at(i, j) * christ_up[k][i][j]
                summed = term if summed is None else summed + term
        gamma_calc.append(summed)
    cov_hess = [[None] * 3 for i in range(3)]
    for i in range(3):
        for j in range(i, 3):
            value = chi_hess(i, j) - (christ_up[0][i][j] * chi_grad[0] + christ_up[1][i][j] * chi_grad[1] + christ_up[2][i][j] * chi_grad[2])
            cov_hess[i][j] = value
            cov_hess[j][i] = value
    laplace = None
    grad_sq = None
    for l in range(3):
        for m in range(3):
            term = inv_at(l, m) * cov_hess[l][m]
            laplace = term if laplace is None else laplace + term
            term = inv_at(l, m) * chi_grad[l] * chi_grad[m]
            grad_sq = term if grad_sq is None else grad_sq + term
    scalar_sum = None
    for i in range(3):
        for j in range(i, 3):
            ricci = None
            for l in range(3):
                for m in range(3):
                    term = -0.5 * inv_at(l, m) * metric_hess(i, j, l, m)
                    ricci = term if ricci is None else ricci + term
            for k in range(3):
                ricci = ricci + 0.5 * (metric_at(k, i) * rest_first[j][7 + k] + metric_at(k, j) * rest_first[i][7 + k])
                ricci = ricci + 0.5 * gamma_calc[k] * (christ_low[i][j][k] + christ_low[j][i][k])
            for l in range(3):
                for m in range(3):
                    inner = None
                    for k in range(3):
                        term = christ_up[k][l][i] * christ_low[j][k][m] + christ_up[k][l][j] * christ_low[i][k][m] + christ_up[k][i][m] * christ_low[k][l][j]
                        inner = term if inner is None else inner + term
                    ricci = ricci + inv_at(l, m) * inner
            conf_part = (cov_hess[i][j] + metric_at(i, j) * laplace) / (2.0 * conformal) - (chi_grad[i] * chi_grad[j] + 3.0 * metric_at(i, j) * grad_sq) / (4.0 * conformal * conformal)
            weight = 1.0 if i == j else 2.0
            term = weight * inv_at(i, j) * (ricci + conf_part)
            scalar_sum = term if scalar_sum is None else scalar_sum + term
    mixed = [[None] * 3 for i in range(3)]
    for i in range(3):
        for j in range(3):
            mixed[i][j] = curv_at(i, 0) * inv_at(0, j) + curv_at(i, 1) * inv_at(1, j) + curv_at(i, 2) * inv_at(2, j)
    square_sum = None
    for i in range(3):
        for j in range(3):
            term = mixed[i][j] * mixed[j][i]
            square_sum = term if square_sum is None else square_sum + term
    hamilton = conformal * scalar_sum + 2.0 / 3.0 * trace_curv * trace_curv - square_sum
    momentum_list = []
    for i in range(3):
        summed = None
        for j in range(3):
            for k in range(3):
                term = inv_at(j, k) * curv_grad(k, i, j)
                summed = term if summed is None else summed + term
        for l in range(3):
            summed = summed - gamma_calc[l] * curv_at(l, i)
            for j in range(3):
                summed = summed - christ_up[l][j][i] * mixed[l][j]
        along = mixed[i][0] * chi_grad[0] + mixed[i][1] * chi_grad[1] + mixed[i][2] * chi_grad[2]
        summed = summed - 2.0 / 3.0 * trace_grad[i] - 1.5 * along / conformal
        momentum_list.append(summed)
    return (hamilton, jnp.stack(momentum_list))

def reference(chi_field, metric, curvature, trace_curvature, gamma_field):
    geometry = jnp.concatenate([chi_field[None], metric], 0)
    remainder = jnp.concatenate([curvature, trace_curvature[None], gamma_field], 0)
    geo_pad = jnp.pad(geometry, ((0, 0), (2, 2), (2, 2), (2, 2)), mode='wrap')
    rest_pad = jnp.pad(remainder, ((0, 0), (2, 2), (2, 2), (2, 2)), mode='wrap')

    def one_slab(index):
        start = (index * CX).astype(jnp.int32)
        geo_slab = lax.dynamic_slice_in_dim(geo_pad, start, CX + 4, 1)
        rest_slab = lax.dynamic_slice_in_dim(rest_pad, start, CX + 4, 1)
        hamilton, momentum = constraints(geo_slab, rest_slab)
        ham_sq = lax.optimization_barrier(jnp.sum(lax.optimization_barrier(jnp.sum(lax.optimization_barrier(jnp.sum(hamilton * hamilton, axis=2)), axis=1)), axis=0))
        mom_sq = lax.optimization_barrier(jnp.sum(lax.optimization_barrier(jnp.sum(lax.optimization_barrier(jnp.sum(lax.optimization_barrier(jnp.sum(momentum * momentum, axis=3)), axis=2)), axis=1)), axis=0))
        return (hamilton, momentum, ham_sq, mom_sq)
    hamilton, momentum, ham_sq, mom_sq = lax.map(one_slab, jnp.arange(N_GX, dtype=jnp.int32))
    hamilton = hamilton.reshape(chi_field.shape)
    momentum = jnp.moveaxis(momentum, 1, 0).reshape(gamma_field.shape)
    cell_count = chi_field.size
    sums = jnp.stack([jnp.sum(ham_sq), jnp.sum(mom_sq)])
    norms = jnp.sqrt(sums / jnp.array([cell_count, 3 * cell_count], dtype=jnp.float32))
    return (hamilton, momentum, norms)
```

```python
import functools

import jax
import jax.numpy as jnp
import numpy as np
from jax import lax
from jax.experimental import pallas as pl
from jax.experimental.pallas import tpu as pltpu
from jax.sharding import PartitionSpec as P

pair_index = ((0, 1, 2), (1, 3, 4), (2, 4, 5))
MESH = pl.DeviceIdType.MESH
CHI, MET, CURV, TRK, GX, GY, GZ = 0, 1, 7, 13, 14, 15, 16
GEO = 7
Z_FIELDS = tuple(range(14)) + (GZ,)
TOP = 8


def first(m2, m1, p1, p2):
    return 8.0 * (p1 - m1) - (p2 - m2)


def second(m2, m1, c, p1, p2):
    return 16.0 * (p1 + m1) - (p2 + m2) - 30.0 * c


def total_of(terms):
    terms = list(terms)
    while len(terms) > 1:
        terms = [
            terms[n] + terms[n + 1] if n + 1 < len(terms) else terms[n]
            for n in range(0, len(terms), 2)
        ]
    return terms[0]


def sym(values, i, j):
    return values[pair_index[i][j]]


def contract(gu, values):
    return total_of(
        [gu[n] * values[n] for n in (0, 3, 5)]
        + [2.0 * total_of(gu[n] * values[n] for n in (1, 2, 4))]
    )


def z_weights():
    weights = np.zeros((len(Z_FIELDS), 256, 256), np.float32)
    for n in range(len(Z_FIELDS)):
        for z in range(128):
            for step, one, two in ((-2, 1, -1), (-1, -8, 16), (0, 0, -30), (1, 8, 16), (2, -1, -1)):
                at = z + step
                row = at if 0 <= at < 128 else 128 + 4 * n + (at + 2 if at < 0 else at - 126)
                weights[n, row, z] = one
                weights[n, row, 128 + z] = two
    return weights


def split(value):
    high = value.astype(jnp.bfloat16)
    return high, (value - high.astype(jnp.float32)).astype(jnp.bfloat16)


def along_z(value, packed, weights):
    parts = [jnp.concatenate([a, b], 1) for a, b in zip(split(value), split(packed))]
    return sum(jnp.dot(part, weights, preferred_element_type=jnp.float32) for part in parts)


def inverse(metric):
    g00, g01, g02, g11, g12, g22 = metric
    m00 = g11 * g22 - g12 * g12
    m01 = g02 * g12 - g01 * g22
    m02 = g01 * g12 - g02 * g11
    m11 = g00 * g22 - g02 * g02
    m12 = g01 * g02 - g00 * g12
    m22 = g00 * g11 - g01 * g01
    scale = 1.0 / (g00 * m00 + g01 * m01 + g02 * m02)
    return [m * scale for m in (m00, m01, m02, m11, m12, m22)]


def cell_math(load, load_dx, load_dy, load_z, load_zz, load_xz, load_yz, load_part):
    zpos = {f: n for n, f in enumerate(Z_FIELDS)}
    gu = inverse([load(MET + n, 0, 0) for n in range(6)])
    gu_hess = [12.0 * gu[n] if n in (0, 3, 5) else 2.0 * gu[n] for n in range(6)]

    def geo(f):
        c = load(f, 0, 0)
        xs = [load(f, s, 0) for s in (-2, -1, 1, 2)]
        ys = [load(f, 0, s) for s in (-2, -1, 1, 2)]
        dx = load_dx(f, 0)
        dy, dz = load_dy(f), load_z(f)
        dxx = second(xs[0], xs[1], c, xs[2], xs[3])
        dyy = second(ys[0], ys[1], c, ys[2], ys[3])
        dzz = load_zz(f)
        dxy = first(*(load_dx(f, s) for s in (-2, -1, 1, 2)))
        dxz, dyz = load_xz(f), load_yz(f)
        hess = (dxx, dxy, dxz, dyy, dyz, dzz)
        return (dx, dy, dz), total_of(gu_hess[n] * hess[n] for n in range(6))

    chi = load(CHI, 0, 0)
    dchi, chi_box = geo(CHI)
    grads = [[None] * 6 for _ in range(3)]
    boxes = []
    for n in range(6):
        d, box = geo(MET + n)
        for a in range(3):
            grads[a][n] = d[a]
        boxes.append(box)
    metric_box = contract(gu, boxes)

    raised = [
        [[total_of(sym(gu, b, l) * sym(grads[k], l, j) for l in range(3)) for j in range(3)] for b in range(3)]
        for k in range(3)
    ]
    trace = [raised[k][0][0] + raised[k][1][1] + raised[k][2][2] for k in range(3)]
    lower = [
        raised[0][0][l] + raised[1][1][l] + raised[2][2][l] - 0.5 * trace[l] for l in range(3)
    ]
    gd = [total_of(sym(gu, k, l) * lower[l] for l in range(3)) for k in range(3)]

    def trace_of(k, l):
        return total_of(raised[k][a][b] * raised[l][b][a] for a in range(3) for b in range(3))

    square = contract(gu, [trace_of(k, l) for k in range(3) for l in range(k, 3)])

    def cross_of(k, b):
        left, right = raised[k][b], raised[b][k]
        up = [total_of(sym(gu, c, j) * right[j] for j in range(3)) for c in range(3)]
        return total_of(left[c] * up[c] for c in range(3))

    cross = (
        cross_of(0, 0)
        + cross_of(1, 1)
        + cross_of(2, 2)
        + 2.0 * (cross_of(0, 1) + cross_of(0, 2) + cross_of(1, 2))
    )
    chi_up = [total_of(sym(gu, k, l) * dchi[l] for l in range(3)) for k in range(3)]
    grad_sq = total_of(chi_up[k] * dchi[k] for k in range(3))
    laplace = chi_box - total_of(gd[k] * dchi[k] for k in range(3))
    drift = total_of(gd[k] * trace[k] for k in range(3))

    def dx_of(f):
        return first(*(load(f, s, 0) for s in (-2, -1, 1, 2)))

    def dy_of(f):
        return first(*(load(f, 0, s) for s in (-2, -1, 1, 2)))

    def dz_of(f):
        return load_z(zpos[f])

    div = dx_of(GX) + dy_of(GY) + dz_of(GZ)
    inv_chi = 1.0 / chi
    curv = [load(CURV + n, 0, 0) for n in range(6)]
    mixed = [
        [total_of(sym(curv, i, k) * sym(gu, k, j) for k in range(3)) for j in range(3)] for i in range(3)
    ]
    curv_up = [
        total_of(sym(gu, i, a) * mixed[a][j] for a in range(3)) for i in range(3) for j in range(i, 3)
    ]
    curv_sq = contract(curv, curv_up)
    trk = load(TRK, 0, 0)
    ham = (
        chi * ((0.25 * square + 0.5 * (cross + drift - metric_box)) * (1.0 / 144.0) + div * (1.0 / 12.0))
        + (2.0 * laplace - 2.5 * grad_sq * inv_chi) * (1.0 / 144.0)
        + (2.0 / 3.0) * trk * trk
        - curv_sq
    )
    push = [gd[l] + 1.5 * inv_chi * chi_up[l] for l in range(3)]
    curv_grads = [[op(CURV + n) for n in range(6)] for op in (dx_of, dy_of, dz_of)]
    trace_grads = [op(TRK) for op in (dx_of, dy_of, dz_of)]
    momentum = []
    for i in range(3):
        parts = total_of(sym(gu, j, k) * sym(curv_grads[j], k, i) for j in range(3) for k in range(3))
        parts = parts + load_part(i)
        parts = parts - total_of(sym(curv, l, i) * push[l] for l in range(3))
        parts = parts - 0.5 * contract(curv_up, grads[i]) - (2.0 / 3.0) * trace_grads[i]
        momentum.append(parts * (1.0 / 12.0))
    return ham, momentum


def kernel(
    sizes,
    chi_in, met_in, curv_in, trk_in, gam_in, weights_in,
    ham_out, mom_out, total_out,
    cells, packed, pack_own, pack_left, pack_right, slope, sums,
    part_out, part, weights, z_one, z_two, y_one, yz_two, xz_two,
    slots_x, slots_y,
    load_sem, xs, xr, ys, yr, zs, zr, es, er, pxs, pxr, pys, pyr,
    rxs, rxr, rys, ryr, cs, cr,
):
    nx, ny, nz = sizes
    cx, cy = chi_in.shape[0], chi_in.shape[1]
    names = ("gx", "gy", "gz")
    me = [lax.axis_index(a) for a in names]

    def moved(axis, step):
        return lax.rem(me[axis] + step + sizes[axis], sizes[axis])

    def peer(axes, steps):
        where = list(me)
        if isinstance(axes, int):
            axes, steps = (axes,), (steps,)
        for axis, step in zip(axes, steps):
            where[axis] = moved(axis, step)
        return tuple(where)

    def hops(axes):
        return [step for step in np.ndindex(*(sizes[a] for a in axes)) if any(step)]

    def place_in(axes, steps=None):
        index = 0
        for axis, step in zip(axes, steps or (0,) * len(axes)):
            index = index * sizes[axis] + moved(axis, step)
        return index

    own_x, own_y = pl.ds(2, cx), pl.ds(TOP, cy)
    loads = [
        pltpu.make_async_copy(src, dst, load_sem.at[n])
        for n, (src, dst) in enumerate(
            (
                (chi_in, cells.at[CHI, own_x, own_y]),
                (met_in, cells.at[pl.ds(MET, 6), own_x, own_y]),
                (curv_in, cells.at[pl.ds(CURV, 6), own_x, own_y]),
                (trk_in, cells.at[TRK, own_x, own_y]),
                (gam_in, cells.at[pl.ds(GX, 3), own_x, own_y]),
                (weights_in, weights),
            )
        )
    ]
    for copy in loads:
        copy.start()
    barrier = pltpu.get_barrier_semaphore()
    for axes in ((1, 2), (0,)):
        for step in hops(axes):
            pl.semaphore_signal(barrier, inc=1, device_id=peer(axes, step), device_id_type=MESH)
    pl.semaphore_wait(barrier, ny * nz + nx - 2)

    def send(src, dst, send_sem, recv_sem, axis, step):
        copy = pltpu.make_async_remote_copy(
            src_ref=src, dst_ref=dst, send_sem=send_sem, recv_sem=recv_sem,
            device_id=peer(axis, step), device_id_type=MESH,
        )
        copy.start()
        return copy

    for copy in loads[:5]:
        copy.wait()
    low_x, high_x = pl.ds(2, 2), pl.ds(cx, 2)
    x_faces = []
    for n, fields in enumerate((pl.ds(0, GEO), pl.ds(GX, 1))):
        x_faces += [
            send(cells.at[fields, high_x, own_y], cells.at[fields, pl.ds(0, 2), own_y], xs.at[2 * n], xr.at[2 * n], 0, 1),
            send(cells.at[fields, low_x, own_y], cells.at[fields, pl.ds(cx + 2, 2), own_y], xs.at[2 * n + 1], xr.at[2 * n + 1], 0, -1),
        ]
    low_y, high_y = pl.ds(TOP, 2), pl.ds(TOP + cy - 2, 2)
    before_y, after_y = pl.ds(TOP - 2, 2), pl.ds(TOP + cy, 2)
    y_faces = [
        send(cells.at[pl.ds(0, 16), own_x, high_y], cells.at[pl.ds(0, 16), own_x, before_y], ys.at[0], yr.at[0], 1, 1),
        send(cells.at[pl.ds(0, 16), own_x, low_y], cells.at[pl.ds(0, 16), own_x, after_y], ys.at[1], yr.at[1], 1, -1),
    ]
    tiles = cy // 8
    lane = lax.broadcasted_iota(jnp.int32, (8, 128), 1)

    def pack(step, carry):
        x, y = step // tiles, lax.rem(step, tiles) * 8
        rows = pl.ds(pl.multiple_of(TOP + y, 8), 8)
        value = jnp.zeros((8, 128), jnp.float32)
        group = lax.shift_right_logical(lane, 2)
        for n, f in enumerate(Z_FIELDS):
            value = jnp.where(group == n, pltpu.roll(cells[f, x + 2, rows], 4 * n + 2, 1), value)
        pack_own[x, pl.ds(pl.multiple_of(y, 8), 8)] = value
        return carry

    lax.fori_loop(0, cx * tiles, pack, 0)
    z_faces = [
        send(pack_own, pack_left, zs.at[0], zr.at[0], 2, 1),
        send(pack_own, pack_right, zs.at[1], zr.at[1], 2, -1),
    ]
    for copy in z_faces:
        copy.wait_recv()

    def merge(x, carry):
        wide = lax.broadcasted_iota(jnp.int32, (cy, 128), 1)
        packed[x + 2, own_y] = jnp.where((wide & 2) == 0, pack_left[x], pack_right[x])
        return carry

    lax.fori_loop(0, cx, merge, 0)
    px_faces = [
        send(packed.at[high_x, own_y], packed.at[pl.ds(0, 2), own_y], pxs.at[0], pxr.at[0], 0, 1),
        send(packed.at[low_x, own_y], packed.at[pl.ds(cx + 2, 2), own_y], pxs.at[1], pxr.at[1], 0, -1),
    ]
    py_faces = [
        send(packed.at[own_x, high_y], packed.at[own_x, before_y], pys.at[0], pyr.at[0], 1, 1),
        send(packed.at[own_x, low_y], packed.at[own_x, after_y], pys.at[1], pyr.at[1], 1, -1),
    ]
    edges = []
    for n, rows in enumerate((before_y, after_y)):
        y_faces[n].wait_recv()
        edges += [
            send(cells.at[pl.ds(0, GEO), high_x, rows], cells.at[pl.ds(0, GEO), pl.ds(0, 2), rows], es.at[2 * n], er.at[2 * n], 0, 1),
            send(cells.at[pl.ds(0, GEO), low_x, rows], cells.at[pl.ds(0, GEO), pl.ds(cx + 2, 2), rows], es.at[2 * n + 1], er.at[2 * n + 1], 0, -1),
        ]
    for copy in py_faces:
        copy.wait_recv()

    sums[...] = jnp.zeros_like(sums)
    loads[5].wait()
    flat = (cx * cy, 128)

    def geo_z(f, carry):
        mid = packed[own_x, own_y].reshape(flat)
        both = along_z(cells[f, own_x, own_y].reshape(flat), mid, weights[f])
        z_one[f] = both[:, :128].reshape(cx, cy, 128)
        z_two[f] = both[:, 128:].reshape(cx, cy, 128)
        dy = first(*(cells[f, own_x, pl.ds(TOP + s, cy)] for s in (-2, -1, 1, 2)))
        dy_packed = first(*(packed[own_x, pl.ds(TOP + s, cy)] for s in (-2, -1, 1, 2)))
        y_one[f] = dy
        yz_two[f] = along_z(dy.reshape(flat), dy_packed.reshape(flat), weights[f, :, :128]).reshape(cx, cy, 128)
        return carry

    lax.fori_loop(0, GEO, geo_z, 0)

    def rest_z(n, carry):
        f = jnp.where(n == 14, GZ, n)
        mid = packed[own_x, own_y].reshape(flat)
        z_one[n] = along_z(cells[f, own_x, own_y].reshape(flat), mid, weights[n, :, :128]).reshape(cx, cy, 128)
        return carry

    lax.fori_loop(GEO, len(Z_FIELDS), rest_z, 0)

    part[:, pl.ds(2, cx - 4)] = jnp.zeros((3, cx - 4, cy, 128), jnp.float32)
    missing = jnp.zeros((7, 2, cy, 128), jnp.float32)
    cells[pl.ds(CURV, 7), pl.ds(0, 2), own_y] = missing
    cells[pl.ds(CURV, 7), pl.ds(cx + 2, 2), own_y] = missing
    x_faces[0].wait_recv()
    x_faces[1].wait_recv()

    def offer(t, carry):
        rows = pl.ds(pl.multiple_of(TOP + t * 8, 8), 8)
        out_rows = pl.ds(pl.multiple_of(t * 8, 8), 8)
        for side, far, near, at, behind, sign in ((0, 0, 1, 2, 3, 1.0), (1, cx + 3, cx + 2, cx + 1, cx, -1.0)):
            edge = [cells[CURV + n, at, rows] * sign for n in range(7)]
            second_edge = [cells[CURV + n, behind, rows] * sign for n in range(7)]
            for place, slot, values in (
                (near, 1 - side, [8.0 * a - b for a, b in zip(edge, second_edge)]),
                (far, side, [-a for a in edge]),
            ):
                gu = inverse([cells[MET + n, place, rows] for n in range(6)])
                for i in range(3):
                    value = total_of(sym(gu, 0, k) * sym(values, k, i) for k in range(3))
                    if i == 0:
                        value = value - (2.0 / 3.0) * values[6]
                    part_out[side, i, slot, out_rows] = value
        return carry

    lax.fori_loop(0, tiles, offer, 0)
    part_faces = [
        send(part_out.at[0], part.at[:, pl.ds(cx - 2, 2)], cs.at[0], cr.at[0], 0, -1),
        send(part_out.at[1], part.at[:, pl.ds(0, 2)], cs.at[1], cr.at[1], 0, 1),
    ]

    def group(step, carry):
        base = lax.rem(2 * step + 2, cx)

        @pl.when(2 * step == cx - 4)
        def _():
            for copy in x_faces[2:] + px_faces + edges + part_faces:
                copy.wait_recv()

        def slopes(f, inner):
            slope[f] = first(*(cells[f, pl.ds(base + 2 + s, 2)] for s in (-2, -1, 1, 2)))
            dx = slope[f, :, own_y].reshape(2 * cy, 128)
            dx_packed = first(*(packed[pl.ds(base + 2 + s, 2), own_y] for s in (-2, -1, 1, 2)))
            xz_two[f] = along_z(dx, dx_packed.reshape(2 * cy, 128), weights[f, :, :128]).reshape(2, cy, 128)
            return inner

        lax.fori_loop(0, GEO, slopes, 0)

        def tile(n, inner):
            half, y = n // tiles, lax.rem(n, tiles) * 8
            x = base + half
            rows = pl.ds(pl.multiple_of(y, 8), 8)
            ham, momentum = cell_math(
                lambda f, sx, sy: cells[f, x + 2 + sx, pl.ds(TOP + y + sy, 8)],
                lambda f, sy: slope[f, half, pl.ds(TOP + y + sy, 8)],
                lambda f: y_one[f, x, rows],
                lambda f: z_one[f, x, rows],
                lambda f: z_two[f, x, rows],
                lambda f: xz_two[f, half, rows],
                lambda f: yz_two[f, x, rows],
                lambda i: part[i, x, rows],
            )
            ham_out[x, rows] = ham
            for i in range(3):
                mom_out[i, x, rows] = momentum[i]
            sums[0] += ham * ham
            sums[1] += momentum[0] * momentum[0] + momentum[1] * momentum[1] + momentum[2] * momentum[2]
            return inner

        lax.fori_loop(0, 2 * tiles, tile, 0)
        return carry

    lax.fori_loop(0, cx // 2, group, 0)

    row = lax.broadcasted_iota(jnp.int32, (8, 128), 0)
    ham_sum = jnp.sum(sums[0], axis=0, keepdims=True)
    mom_sum = jnp.sum(sums[1], axis=0, keepdims=True)
    total = jnp.where(row == 0, ham_sum, jnp.where(row == 1, mom_sum, 0.0))
    pending = []
    for axes, slots, ss, rs in (((1, 2), slots_y, rys, ryr), ((0,), slots_x, rxs, rxr)):
        here = place_in(axes)
        slots[here] = total
        others = hops(axes)
        for n, step in enumerate(others):
            pending.append(send(slots.at[here], slots.at[here], ss.at[n], rs.at[here], axes, step))
        for n, step in enumerate(others):
            source = place_in(axes, step)
            pltpu.make_async_remote_copy(
                src_ref=slots.at[source], dst_ref=slots.at[source], send_sem=ss.at[n],
                recv_sem=rs.at[source], device_id=peer(axes, step), device_id_type=MESH,
            ).wait_recv()
        total = total_of(slots[n] for n in range(len(others) + 1))
    total_out[...] = total
    for copy in x_faces + y_faces + z_faces + px_faces + py_faces + edges + part_faces + pending:
        copy.wait_send()


def deliver(count, ham_in, mom_in, total_in, ham_out, mom_out, norm_out, norm, sems):
    copies = [
        pltpu.make_async_copy(mom_in, mom_out, sems.at[0]),
        pltpu.make_async_copy(ham_in, ham_out, sems.at[1]),
    ]
    for copy in copies:
        copy.start()
    row = lax.broadcasted_iota(jnp.int32, (8, 128), 0)
    rates = jnp.where(row == 0, 1.0 / count, 1.0 / (3.0 * count))
    root = jnp.sqrt(jnp.sum(total_in[...] * rates, axis=1, keepdims=True))
    norm[0] = root[0, 0]
    norm[1] = root[1, 0]
    copies.append(pltpu.make_async_copy(norm, norm_out, sems.at[2]))
    copies[2].start()
    for copy in copies:
        copy.wait()


def on_device(chi_field, metric, curvature, trace_curvature, gamma_field):
    sizes = tuple(lax.axis_size(a) for a in ("gx", "gy", "gz"))
    cx, cy, cz = chi_field.shape
    dma = pltpu.SemaphoreType.DMA
    vmem = pl.BlockSpec(memory_space=pltpu.VMEM)
    block = (cx + 4, cy + 2 * TOP, cz)
    hbm = pl.BlockSpec(memory_space=pltpu.HBM)
    ham, momentum, total = pl.pallas_call(
        functools.partial(kernel, sizes),
        out_shape=(
            pltpu.VMEM(chi_field.shape, jnp.float32),
            pltpu.VMEM(gamma_field.shape, jnp.float32),
            pltpu.VMEM((8, 128), jnp.float32),
        ),
        in_specs=[pl.BlockSpec(memory_space=pltpu.HBM)] * 6,
        out_specs=(vmem, vmem, vmem),
        scratch_shapes=[
            pltpu.VMEM((17,) + block, jnp.float32),
            pltpu.VMEM(block, jnp.float32),
            pltpu.VMEM((cx, cy, cz), jnp.float32),
            pltpu.VMEM((cx, cy, cz), jnp.float32),
            pltpu.VMEM((cx, cy, cz), jnp.float32),
            pltpu.VMEM((GEO, 2) + block[1:], jnp.float32),
            pltpu.VMEM((2, 8, 128), jnp.float32),
            pltpu.VMEM((2, 3, 2, cy, cz), jnp.float32),
            pltpu.VMEM((3, cx, cy, cz), jnp.float32),
            pltpu.VMEM((len(Z_FIELDS), 256, 256), jnp.bfloat16),
            pltpu.VMEM((len(Z_FIELDS), cx, cy, cz), jnp.float32),
            pltpu.VMEM((GEO, cx, cy, cz), jnp.float32),
            pltpu.VMEM((GEO, cx, cy, cz), jnp.float32),
            pltpu.VMEM((GEO, cx, cy, cz), jnp.float32),
            pltpu.VMEM((GEO, 2, cy, cz), jnp.float32),
        ]
        + [pltpu.VMEM((n, 8, 128), jnp.float32) for n in (sizes[0], sizes[1] * sizes[2])]
        + [dma((6,)), dma((4,)), dma((4,)), dma((2,)), dma((2,)), dma((2,)), dma((2,))]
        + [dma((4,)), dma((4,)), dma((2,)), dma((2,)), dma((2,)), dma((2,))]
        + [dma((n,)) for n in (sizes[0], sizes[1] * sizes[2], 2) for _ in range(2)],
        compiler_params=pltpu.CompilerParams(
            collective_id=0, has_side_effects=True, vmem_limit_bytes=67043328 - 16 * chi_field.size - 16384
        ),
    )(chi_field, metric, curvature, trace_curvature, gamma_field, jnp.asarray(z_weights(), jnp.bfloat16))
    count = float(chi_field.size * sizes[0] * sizes[1] * sizes[2])
    return pl.pallas_call(
        functools.partial(deliver, count),
        out_shape=(
            jax.ShapeDtypeStruct(chi_field.shape, jnp.float32),
            jax.ShapeDtypeStruct(gamma_field.shape, jnp.float32),
            jax.ShapeDtypeStruct((2,), jnp.float32),
        ),
        in_specs=[vmem, vmem, vmem],
        out_specs=(hbm, hbm, hbm),
        scratch_shapes=[pltpu.SMEM((2,), jnp.float32), pltpu.SemaphoreType.DMA((3,))],
    )(*(pltpu.with_memory_space_constraint(v, pltpu.VMEM) for v in (ham, momentum, total)))


def solution(mesh):
    return jax.shard_map(
        on_device,
        mesh=mesh,
        in_specs=(
            P("gx", "gy", "gz"),
            P(None, "gx", "gy", "gz"),
            P(None, "gx", "gy", "gz"),
            P("gx", "gy", "gz"),
            P(None, "gx", "gy", "gz"),
        ),
        out_specs=(P("gx", "gy", "gz"), P(None, "gx", "gy", "gz"), P()),
        check_vma=False,
    )
```

```python
import functools

import jax
import jax.numpy as jnp
import numpy as np
from jax import lax
from jax.experimental import pallas as pl
from jax.experimental.pallas import tpu as pltpu
from jax.sharding import PartitionSpec as P

pair_index = ((0, 1, 2), (1, 3, 4), (2, 4, 5))
MESH = pl.DeviceIdType.MESH
GX, CHI, MET, CURV, TRK, GY, GZ = 0, 1, 2, 8, 14, 15, 16
GEO = 7
Z_FIELDS = tuple(range(CHI, GY)) + (GZ,)
TOP = 8


def first(m2, m1, p1, p2):
    return 8.0 * (p1 - m1) - (p2 - m2)


def second(m2, m1, c, p1, p2):
    return 16.0 * (p1 + m1) - (p2 + m2) - 30.0 * c


def total_of(terms):
    terms = list(terms)
    while len(terms) > 1:
        terms = [
            terms[n] + terms[n + 1] if n + 1 < len(terms) else terms[n]
            for n in range(0, len(terms), 2)
        ]
    return terms[0]


def sym(values, i, j):
    return values[pair_index[i][j]]


def contract(gu, values):
    return total_of(
        [gu[n] * values[n] for n in (0, 3, 5)]
        + [2.0 * total_of(gu[n] * values[n] for n in (1, 2, 4))]
    )


def z_weights():
    weights = np.zeros((len(Z_FIELDS), 256, 256), np.float32)
    for n in range(len(Z_FIELDS)):
        for z in range(128):
            for step, one, two in ((-2, 1, -1), (-1, -8, 16), (0, 0, -30), (1, 8, 16), (2, -1, -1)):
                at = z + step
                row = at if 0 <= at < 128 else 128 + 4 * n + (at + 2 if at < 0 else at - 126)
                weights[n, row, z] = one
                weights[n, row, 128 + z] = two
    return weights


def split(value):
    high = value.astype(jnp.bfloat16)
    return high, (value - high.astype(jnp.float32)).astype(jnp.bfloat16)


def along_z(value, packed, weights):
    parts = [jnp.concatenate([a, b], 1) for a, b in zip(split(value), packed)]
    return sum(jnp.dot(part, weights, preferred_element_type=jnp.float32) for part in parts)


def inverse(metric):
    g00, g01, g02, g11, g12, g22 = metric
    m00 = g11 * g22 - g12 * g12
    m01 = g02 * g12 - g01 * g22
    m02 = g01 * g12 - g02 * g11
    m11 = g00 * g22 - g02 * g02
    m12 = g01 * g02 - g00 * g12
    m22 = g00 * g11 - g01 * g01
    scale = 1.0 / (g00 * m00 + g01 * m01 + g02 * m02)
    return [m * scale for m in (m00, m01, m02, m11, m12, m22)]


def cell_math(load, load_dx, load_dy, load_z, load_zz, load_xz, load_yz):
    zpos = {f: n for n, f in enumerate(Z_FIELDS)}
    gu = inverse([load(MET + n, 0, 0) for n in range(6)])
    gu_hess = [12.0 * gu[n] if n in (0, 3, 5) else 2.0 * gu[n] for n in range(6)]

    def geo(f):
        c = load(f, 0, 0)
        xs = [load(f, s, 0) for s in (-2, -1, 1, 2)]
        ys = [load(f, 0, s) for s in (-2, -1, 1, 2)]
        n = zpos[f]
        dx = load_dx(n, 0)
        dy, dz = load_dy(n), load_z(n)
        dxx = second(xs[0], xs[1], c, xs[2], xs[3])
        dyy = second(ys[0], ys[1], c, ys[2], ys[3])
        dzz = load_zz(n)
        dxy = first(*(load_dx(n, s) for s in (-2, -1, 1, 2)))
        dxz, dyz = load_xz(n), load_yz(n)
        hess = (dxx, dxy, dxz, dyy, dyz, dzz)
        return (dx, dy, dz), total_of(gu_hess[n] * hess[n] for n in range(6))

    chi = load(CHI, 0, 0)
    dchi, chi_box = geo(CHI)
    grads = [[None] * 6 for _ in range(3)]
    boxes = []
    for n in range(6):
        d, box = geo(MET + n)
        for a in range(3):
            grads[a][n] = d[a]
        boxes.append(box)
    metric_box = contract(gu, boxes)

    raised = [
        [[total_of(sym(gu, b, l) * sym(grads[k], l, j) for l in range(3)) for j in range(3)] for b in range(3)]
        for k in range(3)
    ]
    trace = [raised[k][0][0] + raised[k][1][1] + raised[k][2][2] for k in range(3)]
    lower = [
        raised[0][0][l] + raised[1][1][l] + raised[2][2][l] - 0.5 * trace[l] for l in range(3)
    ]
    gd = [total_of(sym(gu, k, l) * lower[l] for l in range(3)) for k in range(3)]

    def trace_of(k, l):
        return total_of(raised[k][a][b] * raised[l][b][a] for a in range(3) for b in range(3))

    square = contract(gu, [trace_of(k, l) for k in range(3) for l in range(k, 3)])

    def cross_of(k, b):
        left, right = raised[k][b], raised[b][k]
        up = [total_of(sym(gu, c, j) * right[j] for j in range(3)) for c in range(3)]
        return total_of(left[c] * up[c] for c in range(3))

    cross = (
        cross_of(0, 0)
        + cross_of(1, 1)
        + cross_of(2, 2)
        + 2.0 * (cross_of(0, 1) + cross_of(0, 2) + cross_of(1, 2))
    )
    chi_up = [total_of(sym(gu, k, l) * dchi[l] for l in range(3)) for k in range(3)]
    grad_sq = total_of(chi_up[k] * dchi[k] for k in range(3))
    laplace = chi_box - total_of(gd[k] * dchi[k] for k in range(3))
    drift = total_of(gd[k] * trace[k] for k in range(3))

    def dx_of(f):
        return first(*(load(f, s, 0) for s in (-2, -1, 1, 2)))

    def dy_of(f):
        return first(*(load(f, 0, s) for s in (-2, -1, 1, 2)))

    def dz_of(f):
        return load_z(zpos[f])

    div = dx_of(GX) + dy_of(GY) + dz_of(GZ)
    inv_chi = 1.0 / chi
    curv = [load(CURV + n, 0, 0) for n in range(6)]
    mixed = [
        [total_of(sym(curv, i, k) * sym(gu, k, j) for k in range(3)) for j in range(3)] for i in range(3)
    ]
    curv_up = [
        total_of(sym(gu, i, a) * mixed[a][j] for a in range(3)) for i in range(3) for j in range(i, 3)
    ]
    curv_sq = contract(curv, curv_up)
    trk = load(TRK, 0, 0)
    ham = (
        chi * ((0.25 * square + 0.5 * (cross + drift - metric_box)) * (1.0 / 144.0) + div * (1.0 / 12.0))
        + (2.0 * laplace - 2.5 * grad_sq * inv_chi) * (1.0 / 144.0)
        + (2.0 / 3.0) * trk * trk
        - curv_sq
    )
    push = [gd[l] + 1.5 * inv_chi * chi_up[l] for l in range(3)]
    curv_grads = [[op(CURV + n) for n in range(6)] for op in (dx_of, dy_of, dz_of)]
    trace_grads = [op(TRK) for op in (dx_of, dy_of, dz_of)]
    momentum = []
    for i in range(3):
        parts = total_of(sym(gu, j, k) * sym(curv_grads[j], k, i) for j in range(3) for k in range(3))
        parts = parts - total_of(sym(curv, l, i) * push[l] for l in range(3))
        parts = parts - 0.5 * contract(curv_up, grads[i]) - (2.0 / 3.0) * trace_grads[i]
        momentum.append(parts * (1.0 / 12.0))
    return ham, momentum


def kernel(
    sizes,
    chi_in, met_in, curv_in, trk_in, gam_in, weights_in,
    ham_out, mom_out, total_out,
    cells, packed, pack_own, pack_left, pack_right, edge_own, edge_left, edge_right, slope, sums,
    part_out, part, weights, z_one, z_two, y_one, yz_two, xz_two, mid_split, dy_split, dx_split,
    slots_x, slots_y,
    load_sem, xs, xr, ys, yr, zs, zr, es, er, pys, pyr, ezs, ezr,
    rxs, rxr, rys, ryr, cs, cr,
):
    nx, ny, nz = sizes
    cx, cy = chi_in.shape[0], chi_in.shape[1]
    names = ("gx", "gy", "gz")
    me = [lax.axis_index(a) for a in names]

    def moved(axis, step):
        return lax.rem(me[axis] + step + sizes[axis], sizes[axis])

    def peer(axes, steps):
        where = list(me)
        if isinstance(axes, int):
            axes, steps = (axes,), (steps,)
        for axis, step in zip(axes, steps):
            where[axis] = moved(axis, step)
        return tuple(where)

    def hops(axes):
        return [step for step in np.ndindex(*(sizes[a] for a in axes)) if any(step)]

    def place_in(axes, steps=None):
        index = 0
        for axis, step in zip(axes, steps or (0,) * len(axes)):
            index = index * sizes[axis] + moved(axis, step)
        return index

    own_x, own_y = pl.ds(2, cx), pl.ds(TOP, cy)
    loads = [
        pltpu.make_async_copy(src, dst, load_sem.at[n])
        for n, (src, dst) in enumerate(
            (
                (met_in, cells.at[pl.ds(MET, 6), own_x, own_y]),
                (chi_in, cells.at[CHI, own_x, own_y]),
                (gam_in.at[0], cells.at[GX, own_x, own_y]),
                (curv_in, cells.at[pl.ds(CURV, 6), own_x, own_y]),
                (trk_in, cells.at[TRK, own_x, own_y]),
                (gam_in.at[pl.ds(1, 2)], cells.at[pl.ds(GY, 2), own_x, own_y]),
                (weights_in, weights),
            )
        )
    ]
    for copy in loads:
        copy.start()
    barrier = pltpu.get_barrier_semaphore()
    for axes in ((1, 2), (0,)):
        for step in hops(axes):
            pl.semaphore_signal(barrier, inc=1, device_id=peer(axes, step), device_id_type=MESH)
    pl.semaphore_wait(barrier, ny * nz + nx - 2)

    def send(src, dst, send_sem, recv_sem, axis, step):
        copy = pltpu.make_async_remote_copy(
            src_ref=src, dst_ref=dst, send_sem=send_sem, recv_sem=recv_sem,
            device_id=peer(axis, step), device_id_type=MESH,
        )
        copy.start()
        return copy

    low_x, high_x = pl.ds(2, 2), pl.ds(cx, 2)
    before_x, after_x = pl.ds(0, 2), pl.ds(cx + 2, 2)
    low_y, high_y = pl.ds(TOP, 2), pl.ds(TOP + cy - 2, 2)
    before_y, after_y = pl.ds(TOP - 2, 2), pl.ds(TOP + cy, 2)
    x_faces, y_faces = [], []

    def send_x(fields):
        n = len(x_faces)
        x_faces.extend((
            send(cells.at[fields, high_x, own_y], cells.at[fields, before_x, own_y], xs.at[n], xr.at[n], 0, 1),
            send(cells.at[fields, low_x, own_y], cells.at[fields, after_x, own_y], xs.at[n + 1], xr.at[n + 1], 0, -1),
        ))

    def send_y(fields):
        n = len(y_faces)
        y_faces.extend((
            send(cells.at[fields, own_x, high_y], cells.at[fields, own_x, before_y], ys.at[n], yr.at[n], 1, 1),
            send(cells.at[fields, own_x, low_y], cells.at[fields, own_x, after_y], ys.at[n + 1], yr.at[n + 1], 1, -1),
        ))

    loads[0].wait()
    send_x(pl.ds(MET, 6))
    loads[1].wait()
    send_x(pl.ds(CHI, 1))
    send_y(pl.ds(CHI, GEO))
    loads[2].wait()
    send_x(pl.ds(GX, 1))
    for copy in loads[3:6]:
        copy.wait()
    send_y(pl.ds(CURV, 8))

    tiles = cy // 8
    group = lax.shift_right_logical(lax.broadcasted_iota(jnp.int32, (8, 128), 1), 2)
    far_side = (lax.broadcasted_iota(jnp.int32, (cy, 128), 1) & 2) != 0

    def packing(fields, target, layer):
        def pack(step, carry):
            at, y = step // tiles, lax.rem(step, tiles) * 8
            rows = pl.ds(pl.multiple_of(TOP + y, 8), 8)
            x = layer(at)
            picked = [
                jnp.where(group == n, pltpu.roll(cells[f, x, rows], 4 * n + 2, 1), 0.0)
                for n, f in enumerate(fields)
            ]
            target[at, pl.ds(pl.multiple_of(y, 8), 8)] = total_of(picked)
            return carry

        lax.fori_loop(0, target.shape[0] * tiles, pack, 0, unroll=4)

    packing(Z_FIELDS, pack_own, lambda at: at + 2)
    z_faces = [
        send(pack_own, pack_left, zs.at[0], zr.at[0], 2, 1),
        send(pack_own, pack_right, zs.at[1], zr.at[1], 2, -1),
    ]
    sums[...] = jnp.zeros_like(sums)
    missing = jnp.zeros((7, 2, cy, 128), jnp.float32)
    cells[pl.ds(CURV, 7), before_x, own_y] = missing
    cells[pl.ds(CURV, 7), after_x, own_y] = missing
    for copy in z_faces:
        copy.wait_recv()

    def keep_split(target, value, at=0):
        for n, half in enumerate(split(value)):
            target[n, pl.ds(at, value.shape[0])] = half

    def merge(x, carry):
        value = jnp.where(far_side, pack_right[x], pack_left[x])
        packed[x + 2, own_y] = value
        keep_split(mid_split, value, pl.multiple_of(x * cy, cy))
        return carry

    lax.fori_loop(0, cx, merge, 0)
    py_faces = [
        send(packed.at[own_x, high_y], packed.at[own_x, before_y], pys.at[0], pyr.at[0], 1, 1),
        send(packed.at[own_x, low_y], packed.at[own_x, after_y], pys.at[1], pyr.at[1], 1, -1),
    ]
    loads[6].wait()
    flat = (cx * cy, 128)

    def geo_z(n, carry):
        both = along_z(cells[n + CHI, own_x, own_y].reshape(flat), mid_split[...], weights[n])
        z_one[n] = both[:, :128].reshape(cx, cy, 128)
        z_two[n] = both[:, 128:].reshape(cx, cy, 128)
        return carry

    lax.fori_loop(0, GEO, geo_z, 0, unroll=7)

    def rest_z(n, carry):
        f = n + CHI + n // (GY - CHI)
        z_one[n] = along_z(
            cells[f, own_x, own_y].reshape(flat), mid_split[...], weights[n, :, :128]
        ).reshape(cx, cy, 128)
        return carry

    lax.fori_loop(GEO, len(Z_FIELDS), rest_z, 0, unroll=8)

    for copy in y_faces[:2] + py_faces:
        copy.wait_recv()
    keep_split(dy_split, first(*(packed[own_x, pl.ds(TOP + s, cy)] for s in (-2, -1, 1, 2))).reshape(flat))

    def geo_y(n, carry):
        dy = first(*(cells[n + CHI, own_x, pl.ds(TOP + s, cy)] for s in (-2, -1, 1, 2)))
        y_one[n] = dy
        yz_two[n] = along_z(dy.reshape(flat), dy_split[...], weights[n, :, :128]).reshape(cx, cy, 128)
        return carry

    lax.fori_loop(0, GEO, geo_y, 0, unroll=7)

    def slopes(pieces):
        rows = [count * cy for _, count in pieces]
        at = 0
        for (base, count), size in zip(pieces, rows):
            values = first(*(packed[pl.ds(base + 2 + s, count), own_y] for s in (-2, -1, 1, 2)))
            keep_split(dx_split, values.reshape(size, 128), at)
            at += size
        total = at

        def one(n, carry):
            values = []
            for (base, count), size in zip(pieces, rows):
                dx = first(*(cells[n + CHI, pl.ds(base + 2 + s, count), pl.ds(TOP - 8, cy + 16)] for s in (-2, -1, 1, 2)))
                slope[n, pl.ds(base, count)] = dx
                values.append(dx[:, TOP : TOP + cy].reshape(size, 128))
            both = along_z(jnp.concatenate(values, 0), dx_split[:, :total], weights[n, :, :128])
            at = 0
            for (base, count), size in zip(pieces, rows):
                xz_two[n, pl.ds(base, count)] = both[at : at + size].reshape(count, cy, 128)
                at += size
            return carry

        lax.fori_loop(0, GEO, one, 0, unroll=7)

    def tile_at(x, y):
        rows = pl.ds(pl.multiple_of(y, 8), 8)
        ham, momentum = cell_math(
            lambda f, sx, sy: cells[f, x + 2 + sx, pl.ds(TOP + y + sy, 8)],
            lambda n, sy: slope[n, x, pl.ds(TOP + y + sy, 8)],
            lambda n: y_one[n, x, rows],
            lambda n: z_one[n, x, rows],
            lambda n: z_two[n, x, rows],
            lambda n: xz_two[n, x, rows],
            lambda n: yz_two[n, x, rows],
        )
        ham_out[x, rows] = ham
        for i in range(3):
            mom_out[i, x, rows] = momentum[i]
        sums[0] += ham * ham
        return momentum

    def inner(n, carry):
        momentum = tile_at(2 + n // tiles, lax.rem(n, tiles) * 8)
        sums[1] += momentum[0] * momentum[0] + momentum[1] * momentum[1] + momentum[2] * momentum[2]
        return carry

    def outer(n, carry):
        tile_at(outer_x(n // tiles), lax.rem(n, tiles) * 8)
        return carry

    def outer_x(at):
        return at + at // 2 * (cx - 4)

    slopes(((2, cx - 4),))
    for copy in y_faces[2:]:
        copy.wait_recv()
    inner_tiles = (cx - 4) * tiles
    cut = inner_tiles * 8 // 16, inner_tiles * 12 // 16
    lax.fori_loop(0, cut[0], inner, 0)
    for copy in x_faces[:2]:
        copy.wait_recv()

    def offer(t, carry):
        rows = pl.ds(pl.multiple_of(TOP + t * 8, 8), 8)
        out_rows = pl.ds(pl.multiple_of(t * 8, 8), 8)
        for side, far, near, at, behind, sign in ((0, 0, 1, 2, 3, 1.0), (1, cx + 3, cx + 2, cx + 1, cx, -1.0)):
            edge = [cells[CURV + n, at, rows] * sign for n in range(7)]
            second_edge = [cells[CURV + n, behind, rows] * sign for n in range(7)]
            for place, slot, values in (
                (near, 1 - side, [8.0 * a - b for a, b in zip(edge, second_edge)]),
                (far, side, [-a for a in edge]),
            ):
                gu = inverse([cells[MET + n, place, rows] for n in range(6)])
                for i in range(3):
                    value = total_of(sym(gu, 0, k) * sym(values, k, i) for k in range(3))
                    if i == 0:
                        value = value - (2.0 / 3.0) * values[6]
                    part_out[side, i, slot, out_rows] = value * (1.0 / 12.0)
        return carry

    lax.fori_loop(0, tiles, offer, 0)
    part_faces = [
        send(part_out.at[0], part.at[:, pl.ds(2, 2)], cs.at[0], cr.at[0], 0, -1),
        send(part_out.at[1], part.at[:, pl.ds(0, 2)], cs.at[1], cr.at[1], 0, 1),
    ]
    lax.fori_loop(cut[0], cut[1], inner, 0)
    for copy in x_faces[2:4]:
        copy.wait_recv()
    geo = pl.ds(CHI, GEO)
    edges = []
    for layers in (before_x, after_x):
        n = len(edges)
        edges += [
            send(cells.at[geo, layers, high_y], cells.at[geo, layers, before_y], es.at[n], er.at[n], 1, 1),
            send(cells.at[geo, layers, low_y], cells.at[geo, layers, after_y], es.at[n + 1], er.at[n + 1], 1, -1),
        ]
    packing(Z_FIELDS[:GEO], edge_own, lambda at: at + at // 2 * cx)
    edge_z = [
        send(edge_own, edge_left, ezs.at[0], ezr.at[0], 2, 1),
        send(edge_own, edge_right, ezs.at[1], ezr.at[1], 2, -1),
    ]
    lax.fori_loop(cut[1], inner_tiles, inner, 0)
    for copy in edge_z:
        copy.wait_recv()
    for at in range(4):
        packed[at + at // 2 * cx, own_y] = jnp.where(far_side, edge_right[at], edge_left[at])
    for copy in edges:
        copy.wait_recv()
    slopes(((0, 2), (cx - 2, 2)))
    for copy in x_faces[4:]:
        copy.wait_recv()
    lax.fori_loop(0, 4 * tiles, outer, 0)
    for copy in part_faces:
        copy.wait_recv()

    def finish(n, carry):
        at, rows = n // tiles, pl.ds(pl.multiple_of(lax.rem(n, tiles) * 8, 8), 8)
        x = outer_x(at)
        momentum = [mom_out[i, x, rows] + part[i, at, rows] for i in range(3)]
        for i in range(3):
            mom_out[i, x, rows] = momentum[i]
        sums[1] += momentum[0] * momentum[0] + momentum[1] * momentum[1] + momentum[2] * momentum[2]
        return carry

    lax.fori_loop(0, 4 * tiles, finish, 0, unroll=4)

    row = lax.broadcasted_iota(jnp.int32, (8, 128), 0)
    ham_sum = jnp.sum(sums[0], axis=0, keepdims=True)
    mom_sum = jnp.sum(sums[1], axis=0, keepdims=True)
    total = jnp.where(row == 0, ham_sum, jnp.where(row == 1, mom_sum, 0.0))
    pending = []
    for axes, slots, ss, rs in (((1, 2), slots_y, rys, ryr), ((0,), slots_x, rxs, rxr)):
        here = place_in(axes)
        slots[here] = total
        others = hops(axes)
        for n, step in enumerate(others):
            pending.append(send(slots.at[here], slots.at[here], ss.at[n], rs.at[here], axes, step))
        for n, step in enumerate(others):
            source = place_in(axes, step)
            pltpu.make_async_remote_copy(
                src_ref=slots.at[source], dst_ref=slots.at[source], send_sem=ss.at[n],
                recv_sem=rs.at[source], device_id=peer(axes, step), device_id_type=MESH,
            ).wait_recv()
        total = total_of(slots[n] for n in range(len(others) + 1))
    total_out[...] = total
    for copy in x_faces + y_faces + z_faces + py_faces + edges + edge_z + part_faces + pending:
        copy.wait_send()


def deliver(count, ham_in, mom_in, total_in, ham_out, mom_out, norm_out, norm, sems):
    copies = [
        pltpu.make_async_copy(mom_in, mom_out, sems.at[0]),
        pltpu.make_async_copy(ham_in, ham_out, sems.at[1]),
    ]
    for copy in copies:
        copy.start()
    row = lax.broadcasted_iota(jnp.int32, (8, 128), 0)
    rates = jnp.where(row == 0, 1.0 / count, 1.0 / (3.0 * count))
    root = jnp.sqrt(jnp.sum(total_in[...] * rates, axis=1, keepdims=True))
    norm[0] = root[0, 0]
    norm[1] = root[1, 0]
    copies.append(pltpu.make_async_copy(norm, norm_out, sems.at[2]))
    copies[2].start()
    for copy in copies:
        copy.wait()


def on_device(chi_field, metric, curvature, trace_curvature, gamma_field):
    sizes = tuple(lax.axis_size(a) for a in ("gx", "gy", "gz"))
    cx, cy, cz = chi_field.shape
    dma = pltpu.SemaphoreType.DMA
    vmem = pl.BlockSpec(memory_space=pltpu.VMEM)
    block = (cx + 4, cy + 2 * TOP, cz)
    hbm = pl.BlockSpec(memory_space=pltpu.HBM)
    ham, momentum, total = pl.pallas_call(
        functools.partial(kernel, sizes),
        out_shape=(
            pltpu.VMEM(chi_field.shape, jnp.float32),
            pltpu.VMEM(gamma_field.shape, jnp.float32),
            pltpu.VMEM((8, 128), jnp.float32),
        ),
        in_specs=[pl.BlockSpec(memory_space=pltpu.HBM)] * 6,
        out_specs=(vmem, vmem, vmem),
        scratch_shapes=[
            pltpu.VMEM((17,) + block, jnp.float32),
            pltpu.VMEM(block, jnp.float32),
        ]
        + [pltpu.VMEM((cx, cy, cz), jnp.float32)] * 3
        + [pltpu.VMEM((4, cy, cz), jnp.float32)] * 3
        + [
            pltpu.VMEM((GEO, cx) + block[1:], jnp.float32),
            pltpu.VMEM((2, 8, 128), jnp.float32),
            pltpu.VMEM((2, 3, 2, cy, cz), jnp.float32),
            pltpu.VMEM((3, 4, cy, cz), jnp.float32),
            pltpu.VMEM((len(Z_FIELDS), 256, 256), jnp.bfloat16),
            pltpu.VMEM((len(Z_FIELDS), cx, cy, cz), jnp.float32),
        ]
        + [pltpu.VMEM((GEO, cx, cy, cz), jnp.float32)] * 4
        + [pltpu.VMEM((2, cx * cy, cz), jnp.bfloat16)] * 3
        + [pltpu.VMEM((n, 8, 128), jnp.float32) for n in (sizes[0], sizes[1] * sizes[2])]
        + [dma((n,)) for n in (7, 6, 6, 4, 4, 2, 2, 4, 4, 2, 2, 2, 2)]
        + [dma((n,)) for n in (sizes[0], sizes[1] * sizes[2], 2) for _ in range(2)],
        compiler_params=pltpu.CompilerParams(
            collective_id=0, has_side_effects=True, vmem_limit_bytes=67043328 - 16 * chi_field.size - 16384
        ),
    )(chi_field, metric, curvature, trace_curvature, gamma_field, jnp.asarray(z_weights(), jnp.bfloat16))
    count = float(chi_field.size * sizes[0] * sizes[1] * sizes[2])
    return pl.pallas_call(
        functools.partial(deliver, count),
        out_shape=(
            jax.ShapeDtypeStruct(chi_field.shape, jnp.float32),
            jax.ShapeDtypeStruct(gamma_field.shape, jnp.float32),
            jax.ShapeDtypeStruct((2,), jnp.float32),
        ),
        in_specs=[vmem, vmem, vmem],
        out_specs=(hbm, hbm, hbm),
        scratch_shapes=[pltpu.SMEM((2,), jnp.float32), pltpu.SemaphoreType.DMA((3,))],
    )(*(pltpu.with_memory_space_constraint(v, pltpu.VMEM) for v in (ham, momentum, total)))


def solution(mesh):
    return jax.shard_map(
        on_device,
        mesh=mesh,
        in_specs=(
            P("gx", "gy", "gz"),
            P(None, "gx", "gy", "gz"),
            P(None, "gx", "gy", "gz"),
            P("gx", "gy", "gz"),
            P(None, "gx", "gy", "gz"),
        ),
        out_specs=(P("gx", "gy", "gz"), P(None, "gx", "gy", "gz"), P()),
        check_vma=False,
    )
```

```python
import functools

import jax
import jax.numpy as jnp
import numpy as np
from jax import lax
from jax.experimental import pallas as pl
from jax.experimental.pallas import tpu as pltpu
from jax.sharding import PartitionSpec as P

pair_index = ((0, 1, 2), (1, 3, 4), (2, 4, 5))
MESH = pl.DeviceIdType.MESH
GX, CHI, MET, CURV, TRK, GY, GZ = 0, 1, 2, 8, 14, 15, 16
GEO = 7
Z_FIELDS = tuple(range(CHI, GY)) + (GZ,)
TOP = 8


def first(m2, m1, p1, p2):
    return 8.0 * (p1 - m1) - (p2 - m2)


def second(m2, m1, c, p1, p2):
    return 16.0 * (p1 + m1) - (p2 + m2) - 30.0 * c


def total_of(terms):
    terms = list(terms)
    while len(terms) > 1:
        terms = [
            terms[n] + terms[n + 1] if n + 1 < len(terms) else terms[n]
            for n in range(0, len(terms), 2)
        ]
    return terms[0]


def sym(values, i, j):
    return values[pair_index[i][j]]


def contract(gu, values):
    return total_of(
        [gu[n] * values[n] for n in (0, 3, 5)]
        + [2.0 * total_of(gu[n] * values[n] for n in (1, 2, 4))]
    )


def z_weights():
    weights = np.zeros((len(Z_FIELDS), 256, 256), np.float32)
    for n in range(len(Z_FIELDS)):
        for z in range(128):
            for step, one, two in ((-2, 1, -1), (-1, -8, 16), (0, 0, -30), (1, 8, 16), (2, -1, -1)):
                at = z + step
                row = at if 0 <= at < 128 else 128 + 4 * n + (at + 2 if at < 0 else at - 126)
                weights[n, row, z] = one
                weights[n, row, 128 + z] = two
    return weights


def split(value):
    high = value.astype(jnp.bfloat16)
    return high, (value - high.astype(jnp.float32)).astype(jnp.bfloat16)


def along_z(value, packed, weights):
    parts = [jnp.concatenate([a, b], 1) for a, b in zip(split(value), packed)]
    return sum(jnp.dot(part, weights, preferred_element_type=jnp.float32) for part in parts)


def inverse(metric):
    g00, g01, g02, g11, g12, g22 = metric
    m00 = g11 * g22 - g12 * g12
    m01 = g02 * g12 - g01 * g22
    m02 = g01 * g12 - g02 * g11
    m11 = g00 * g22 - g02 * g02
    m12 = g01 * g02 - g00 * g12
    m22 = g00 * g11 - g01 * g01
    scale = 1.0 / (g00 * m00 + g01 * m01 + g02 * m02)
    return [m * scale for m in (m00, m01, m02, m11, m12, m22)]


def cell_math(load, load_dx, load_dy, load_z, load_zz, load_xz, load_yz):
    zpos = {f: n for n, f in enumerate(Z_FIELDS)}
    gu = inverse([load(MET + n, 0, 0) for n in range(6)])
    gu_hess = [12.0 * gu[n] if n in (0, 3, 5) else 2.0 * gu[n] for n in range(6)]

    def geo(f):
        c = load(f, 0, 0)
        xs = [load(f, s, 0) for s in (-2, -1, 1, 2)]
        ys = [load(f, 0, s) for s in (-2, -1, 1, 2)]
        n = zpos[f]
        dx = load_dx(n, 0)
        dy, dz = load_dy(n), load_z(n)
        dxx = second(xs[0], xs[1], c, xs[2], xs[3])
        dyy = second(ys[0], ys[1], c, ys[2], ys[3])
        dzz = load_zz(n)
        dxy = first(*(load_dx(n, s) for s in (-2, -1, 1, 2)))
        dxz, dyz = load_xz(n), load_yz(n)
        hess = (dxx, dxy, dxz, dyy, dyz, dzz)
        return (dx, dy, dz), total_of(gu_hess[n] * hess[n] for n in range(6))

    chi = load(CHI, 0, 0)
    dchi, chi_box = geo(CHI)
    grads = [[None] * 6 for _ in range(3)]
    boxes = []
    for n in range(6):
        d, box = geo(MET + n)
        for a in range(3):
            grads[a][n] = d[a]
        boxes.append(box)
    metric_box = contract(gu, boxes)

    raised = [
        [[total_of(sym(gu, b, l) * sym(grads[k], l, j) for l in range(3)) for j in range(3)] for b in range(3)]
        for k in range(3)
    ]
    trace = [raised[k][0][0] + raised[k][1][1] + raised[k][2][2] for k in range(3)]
    lower = [
        raised[0][0][l] + raised[1][1][l] + raised[2][2][l] - 0.5 * trace[l] for l in range(3)
    ]
    gd = [total_of(sym(gu, k, l) * lower[l] for l in range(3)) for k in range(3)]

    def trace_of(k, l):
        return total_of(raised[k][a][b] * raised[l][b][a] for a in range(3) for b in range(3))

    square = contract(gu, [trace_of(k, l) for k in range(3) for l in range(k, 3)])

    def cross_of(k, b):
        left, right = raised[k][b], raised[b][k]
        up = [total_of(sym(gu, c, j) * right[j] for j in range(3)) for c in range(3)]
        return total_of(left[c] * up[c] for c in range(3))

    cross = (
        cross_of(0, 0)
        + cross_of(1, 1)
        + cross_of(2, 2)
        + 2.0 * (cross_of(0, 1) + cross_of(0, 2) + cross_of(1, 2))
    )
    chi_up = [total_of(sym(gu, k, l) * dchi[l] for l in range(3)) for k in range(3)]
    grad_sq = total_of(chi_up[k] * dchi[k] for k in range(3))
    laplace = chi_box - total_of(gd[k] * dchi[k] for k in range(3))
    drift = total_of(gd[k] * trace[k] for k in range(3))

    def dx_of(f):
        return first(*(load(f, s, 0) for s in (-2, -1, 1, 2)))

    def dy_of(f):
        return first(*(load(f, 0, s) for s in (-2, -1, 1, 2)))

    def dz_of(f):
        return load_z(zpos[f])

    div = dx_of(GX) + dy_of(GY) + dz_of(GZ)
    inv_chi = 1.0 / chi
    curv = [load(CURV + n, 0, 0) for n in range(6)]
    mixed = [
        [total_of(sym(curv, i, k) * sym(gu, k, j) for k in range(3)) for j in range(3)] for i in range(3)
    ]
    curv_up = [
        total_of(sym(gu, i, a) * mixed[a][j] for a in range(3)) for i in range(3) for j in range(i, 3)
    ]
    curv_sq = contract(curv, curv_up)
    trk = load(TRK, 0, 0)
    ham = (
        chi * ((0.25 * square + 0.5 * (cross + drift - metric_box)) * (1.0 / 144.0) + div * (1.0 / 12.0))
        + (2.0 * laplace - 2.5 * grad_sq * inv_chi) * (1.0 / 144.0)
        + (2.0 / 3.0) * trk * trk
        - curv_sq
    )
    push = [gd[l] + 1.5 * inv_chi * chi_up[l] for l in range(3)]
    curv_grads = [[op(CURV + n) for n in range(6)] for op in (dx_of, dy_of, dz_of)]
    trace_grads = [op(TRK) for op in (dx_of, dy_of, dz_of)]
    momentum = []
    for i in range(3):
        parts = total_of(sym(gu, j, k) * sym(curv_grads[j], k, i) for j in range(3) for k in range(3))
        parts = parts - total_of(sym(curv, l, i) * push[l] for l in range(3))
        parts = parts - 0.5 * contract(curv_up, grads[i]) - (2.0 / 3.0) * trace_grads[i]
        momentum.append(parts * (1.0 / 12.0))
    return ham, momentum


def kernel(
    sizes,
    chi_in, met_in, curv_in, trk_in, gam_in, weights_in,
    ham_out, mom_out, total_out,
    cells, packed, pack_own, pack_left, pack_right, edge_own, edge_left, edge_right, slope, sums,
    part_out, part, weights, z_one, z_two, y_one, yz_two, xz_two, mid_split, dy_split, dx_split,
    slots_x, slots_y,
    load_sem, xs, xr, ys, yr, zs, zr, es, er, pys, pyr, ezs, ezr,
    rxs, rxr, rys, ryr, cs, cr,
):
    nx, ny, nz = sizes
    cx, cy = chi_in.shape[0], chi_in.shape[1]
    names = ("gx", "gy", "gz")
    me = [lax.axis_index(a) for a in names]

    def moved(axis, step):
        return lax.rem(me[axis] + step + sizes[axis], sizes[axis])

    def peer(axes, steps):
        where = list(me)
        if isinstance(axes, int):
            axes, steps = (axes,), (steps,)
        for axis, step in zip(axes, steps):
            where[axis] = moved(axis, step)
        return tuple(where)

    def hops(axes):
        return [step for step in np.ndindex(*(sizes[a] for a in axes)) if any(step)]

    def place_in(axes, steps=None):
        index = 0
        for axis, step in zip(axes, steps or (0,) * len(axes)):
            index = index * sizes[axis] + moved(axis, step)
        return index

    own_x, own_y = pl.ds(2, cx), pl.ds(TOP, cy)
    loads = [
        pltpu.make_async_copy(src, dst, load_sem.at[n])
        for n, (src, dst) in enumerate(
            (
                (met_in, cells.at[pl.ds(MET, 6), own_x, own_y]),
                (chi_in, cells.at[CHI, own_x, own_y]),
                (gam_in.at[0], cells.at[GX, own_x, own_y]),
                (curv_in, cells.at[pl.ds(CURV, 6), own_x, own_y]),
                (trk_in, cells.at[TRK, own_x, own_y]),
                (gam_in.at[pl.ds(1, 2)], cells.at[pl.ds(GY, 2), own_x, own_y]),
                (weights_in, weights),
            )
        )
    ]
    for copy in loads[:6]:
        copy.start()
    barrier = pltpu.get_barrier_semaphore()
    for axes in ((1, 2), (0,)):
        for step in hops(axes):
            pl.semaphore_signal(barrier, inc=1, device_id=peer(axes, step), device_id_type=MESH)
    pl.semaphore_wait(barrier, ny * nz + nx - 2)

    def send(src, dst, send_sem, recv_sem, axis, step):
        copy = pltpu.make_async_remote_copy(
            src_ref=src, dst_ref=dst, send_sem=send_sem, recv_sem=recv_sem,
            device_id=peer(axis, step), device_id_type=MESH,
        )
        copy.start()
        return copy

    low_x, high_x = pl.ds(2, 2), pl.ds(cx, 2)
    before_x, after_x = pl.ds(0, 2), pl.ds(cx + 2, 2)
    low_y, high_y = pl.ds(TOP, 2), pl.ds(TOP + cy - 2, 2)
    before_y, after_y = pl.ds(TOP - 2, 2), pl.ds(TOP + cy, 2)
    x_faces, y_faces = [], []

    def send_x(fields):
        n = len(x_faces)
        x_faces.extend((
            send(cells.at[fields, high_x, own_y], cells.at[fields, before_x, own_y], xs.at[n], xr.at[n], 0, 1),
            send(cells.at[fields, low_x, own_y], cells.at[fields, after_x, own_y], xs.at[n + 1], xr.at[n + 1], 0, -1),
        ))

    def send_y(fields):
        n = len(y_faces)
        y_faces.extend((
            send(cells.at[fields, own_x, high_y], cells.at[fields, own_x, before_y], ys.at[n], yr.at[n], 1, 1),
            send(cells.at[fields, own_x, low_y], cells.at[fields, own_x, after_y], ys.at[n + 1], yr.at[n + 1], 1, -1),
        ))

    loads[0].wait()
    send_x(pl.ds(MET, 6))
    loads[1].wait()
    send_x(pl.ds(CHI, 1))
    send_y(pl.ds(CHI, GEO))
    loads[2].wait()
    send_x(pl.ds(GX, 1))
    for copy in loads[3:6]:
        copy.wait()
    send_y(pl.ds(CURV, 8))
    loads[6].start()

    tiles = cy // 8
    group = lax.shift_right_logical(lax.broadcasted_iota(jnp.int32, (8, 128), 1), 2)
    far_side = (lax.broadcasted_iota(jnp.int32, (cy, 128), 1) & 2) != 0

    def packing(fields, target, layer):
        def pack(step, carry):
            at, y = step // tiles, lax.rem(step, tiles) * 8
            rows = pl.ds(pl.multiple_of(TOP + y, 8), 8)
            x = layer(at)
            picked = [
                jnp.where(group == n, pltpu.roll(cells[f, x, rows], 4 * n + 2, 1), 0.0)
                for n, f in enumerate(fields)
                if f is not None
            ]
            target[at, pl.ds(pl.multiple_of(y, 8), 8)] = total_of(picked)
            return carry

        lax.fori_loop(0, target.shape[0] * tiles, pack, 0, unroll=4)

    packing(Z_FIELDS, pack_own, lambda at: at + 2)

    def send_z(own, left, right, send_sem, recv_sem):
        faces = [send(own, left, send_sem.at[0], recv_sem.at[0], 2, 1)]
        if nz > 2:
            faces.append(send(own, right, send_sem.at[1], recv_sem.at[1], 2, -1))
        return faces

    def joined(left, right, at):
        return jnp.where(far_side, right[at], left[at]) if nz > 2 else left[at]

    z_faces = send_z(pack_own, pack_left, pack_right, zs, zr)
    sums[...] = jnp.zeros_like(sums)
    missing = jnp.zeros((7, 2, cy, 128), jnp.float32)
    cells[pl.ds(CURV, 7), before_x, own_y] = missing
    cells[pl.ds(CURV, 7), after_x, own_y] = missing
    for copy in z_faces:
        copy.wait_recv()

    def keep_split(target, value, at=0):
        for n, half in enumerate(split(value)):
            target[n, pl.ds(at, value.shape[0])] = half

    def merge(x, carry):
        value = joined(pack_left, pack_right, x)
        packed[x + 2, own_y] = value
        keep_split(mid_split, value, pl.multiple_of(x * cy, cy))
        return carry

    lax.fori_loop(0, cx, merge, 0)
    py_faces = [
        send(packed.at[own_x, high_y], packed.at[own_x, before_y], pys.at[0], pyr.at[0], 1, 1),
        send(packed.at[own_x, low_y], packed.at[own_x, after_y], pys.at[1], pyr.at[1], 1, -1),
    ]
    loads[6].wait()
    flat = (cx * cy, 128)

    def geo_z(n, carry):
        both = along_z(cells[n + CHI, own_x, own_y].reshape(flat), mid_split[...], weights[n])
        z_one[n] = both[:, :128].reshape(cx, cy, 128)
        z_two[n] = both[:, 128:].reshape(cx, cy, 128)
        return carry

    lax.fori_loop(0, GEO, geo_z, 0, unroll=7)

    def rest_z(n, carry):
        f = n + CHI + n // (GY - CHI)
        z_one[n] = along_z(
            cells[f, own_x, own_y].reshape(flat), mid_split[...], weights[n, :, :128]
        ).reshape(cx, cy, 128)
        return carry

    lax.fori_loop(GEO, len(Z_FIELDS), rest_z, 0, unroll=8)

    def rises(pieces):
        rows = [cx * count for _, count in pieces]
        at = 0
        for (row, count), size in zip(pieces, rows):
            values = first(*(packed[own_x, pl.ds(TOP + row + s, count)] for s in (-2, -1, 1, 2)))
            keep_split(dy_split, values.reshape(size, 128), at)
            at += size
        total = at

        def one(n, carry):
            values = []
            for (row, count), size in zip(pieces, rows):
                dy = first(*(cells[n + CHI, own_x, pl.ds(TOP + row + s, count)] for s in (-2, -1, 1, 2)))
                y_one[n, :, pl.ds(row, count)] = dy
                values.append(dy.reshape(size, 128))
            both = along_z(jnp.concatenate(values, 0), dy_split[:, :total], weights[n, :, :128])
            at = 0
            for (row, count), size in zip(pieces, rows):
                yz_two[n, :, pl.ds(row, count)] = both[at : at + size].reshape(cx, count, 128)
                at += size
            return carry

        lax.fori_loop(0, GEO, one, 0, unroll=7)

    def slopes(pieces):
        rows = [count * cy for _, count in pieces]
        at = 0
        for (base, count), size in zip(pieces, rows):
            values = first(*(packed[pl.ds(base + 2 + s, count), own_y] for s in (-2, -1, 1, 2)))
            keep_split(dx_split, values.reshape(size, 128), at)
            at += size
        total = at

        def one(n, carry):
            values = []
            for (base, count), size in zip(pieces, rows):
                dx = first(*(cells[n + CHI, pl.ds(base + 2 + s, count), own_y] for s in (-2, -1, 1, 2)))
                slope[n, pl.ds(base, count), own_y] = dx
                values.append(dx.reshape(size, 128))
            both = along_z(jnp.concatenate(values, 0), dx_split[:, :total], weights[n, :, :128])
            at = 0
            for (base, count), size in zip(pieces, rows):
                xz_two[n, pl.ds(base, count)] = both[at : at + size].reshape(count, cy, 128)
                at += size
            return carry

        lax.fori_loop(0, GEO, one, 0, unroll=7)

    def tile_at(x, y):
        rows = pl.ds(pl.multiple_of(y, 8), 8)
        ham, momentum = cell_math(
            lambda f, sx, sy: cells[f, x + 2 + sx, pl.ds(TOP + y + sy, 8)],
            lambda n, sy: slope[n, x, pl.ds(TOP + y + sy, 8)],
            lambda n: y_one[n, x, rows],
            lambda n: z_one[n, x, rows],
            lambda n: z_two[n, x, rows],
            lambda n: xz_two[n, x, rows],
            lambda n: yz_two[n, x, rows],
        )
        ham_out[x, rows] = ham
        for i in range(3):
            mom_out[i, x, rows] = momentum[i]
        sums[0] += ham * ham
        return momentum

    def rims(pieces):
        def one(n, carry):
            for base, count in pieces:
                for rows in (pl.ds(TOP - 8, 8), pl.ds(TOP + cy, 8)):
                    slope[n, pl.ds(base, count), rows] = first(
                        *(cells[n + CHI, pl.ds(base + 2 + s, count), rows] for s in (-2, -1, 1, 2))
                    )
            return carry

        lax.fori_loop(0, GEO, one, 0, unroll=7)

    def outer_x(at):
        return at + at // 2 * (cx - 4)

    def run(layers, layer, count, row, square):
        def one(n, carry):
            momentum = tile_at(layer(n // count), row(lax.rem(n, count)))
            if square:
                sums[1] += momentum[0] * momentum[0] + momentum[1] * momentum[1] + momentum[2] * momentum[2]
            return carry

        lax.fori_loop(0, layers * count, one, 0)

    inner = (cx - 4, lambda at: at + 2)
    outer = (4, outer_x)
    middle = (tiles - 2, lambda at: 8 * at + 8)
    rim = (2, lambda at: at * (cy - 8))
    rises(((8, cy - 16),))
    slopes(((2, cx - 4),))
    run(*inner, *middle, True)
    for copy in y_faces[:2] + py_faces:
        copy.wait_recv()
    rises(((0, 8), (cy - 8, 8)))
    rims(((2, cx - 4),))
    for copy in y_faces[2:]:
        copy.wait_recv()
    run(*inner, *rim, True)
    for copy in x_faces[:2]:
        copy.wait_recv()

    def offer(t, carry):
        rows = pl.ds(pl.multiple_of(TOP + t * 8, 8), 8)
        out_rows = pl.ds(pl.multiple_of(t * 8, 8), 8)
        for side, far, near, at, behind, sign in ((0, 0, 1, 2, 3, 1.0), (1, cx + 3, cx + 2, cx + 1, cx, -1.0)):
            edge = [cells[CURV + n, at, rows] * sign for n in range(7)]
            second_edge = [cells[CURV + n, behind, rows] * sign for n in range(7)]
            for place, slot, values in (
                (near, 1 - side, [8.0 * a - b for a, b in zip(edge, second_edge)]),
                (far, side, [-a for a in edge]),
            ):
                gu = inverse([cells[MET + n, place, rows] for n in range(6)])
                for i in range(3):
                    value = total_of(sym(gu, 0, k) * sym(values, k, i) for k in range(3))
                    if i == 0:
                        value = value - (2.0 / 3.0) * values[6]
                    part_out[side, i, slot, out_rows] = value * (1.0 / 12.0)
        return carry

    lax.fori_loop(0, tiles, offer, 0)
    part_faces = [
        send(part_out.at[0], part.at[:, pl.ds(2, 2)], cs.at[0], cr.at[0], 0, -1),
        send(part_out.at[1], part.at[:, pl.ds(0, 2)], cs.at[1], cr.at[1], 0, 1),
    ]
    edges, edge_z = [], []

    def relay(fields):
        for layers in (before_x, after_x):
            n = len(edges)
            edges.extend((
                send(cells.at[fields, layers, high_y], cells.at[fields, layers, before_y], es.at[n], er.at[n], 1, 1),
                send(cells.at[fields, layers, low_y], cells.at[fields, layers, after_y], es.at[n + 1], er.at[n + 1], 1, -1),
            ))

    def relay_z(fields):
        n = len(edge_z)
        packing(fields, edge_own.at[n], lambda at: at + at // 2 * cx)
        edge_z.append(send_z(edge_own.at[n], edge_left.at[n], edge_right.at[n], ezs.at[n], ezr.at[n]))

    relay(pl.ds(MET, 6))
    relay_z((None,) + tuple(range(MET, CURV)))
    for copy in x_faces[2:4]:
        copy.wait_recv()
    relay(pl.ds(CHI, 1))
    relay_z((CHI,))
    for copy in edge_z[0] + edge_z[1]:
        copy.wait_recv()
    for at in range(4):
        packed[at + at // 2 * cx, own_y] = joined(edge_left.at[0], edge_right.at[0], at) + joined(edge_left.at[1], edge_right.at[1], at)
    slopes(((0, 2), (cx - 2, 2)))
    for copy in x_faces[4:]:
        copy.wait_recv()
    run(*outer, *middle, False)
    for copy in edges:
        copy.wait_recv()
    rims(((0, 2), (cx - 2, 2)))
    run(*outer, *rim, False)
    for copy in part_faces:
        copy.wait_recv()

    def finish(n, carry):
        at, rows = n // tiles, pl.ds(pl.multiple_of(lax.rem(n, tiles) * 8, 8), 8)
        x = outer_x(at)
        momentum = [mom_out[i, x, rows] + part[i, at, rows] for i in range(3)]
        for i in range(3):
            mom_out[i, x, rows] = momentum[i]
        sums[1] += momentum[0] * momentum[0] + momentum[1] * momentum[1] + momentum[2] * momentum[2]
        return carry

    lax.fori_loop(0, 4 * tiles, finish, 0, unroll=4)

    lane = lax.broadcasted_iota(jnp.int32, (8, 128), 1)
    folded = [sums[n] + pltpu.roll(sums[n], 64, 1) for n in range(2)]
    total = jnp.sum(jnp.where(lane < 64, folded[0], folded[1]), axis=0, keepdims=True)
    line = pl.ds(0, 1)
    pending = []
    for axes, slots, ss, rs in (((1, 2), slots_y, rys, ryr), ((0,), slots_x, rxs, rxr)):
        here = place_in(axes)
        slots[here, line] = total
        others = hops(axes)
        for n, step in enumerate(others):
            pending.append(send(slots.at[here, line], slots.at[here, line], ss.at[n], rs.at[here], axes, step))
        for n, step in enumerate(others):
            source = place_in(axes, step)
            pltpu.make_async_remote_copy(
                src_ref=slots.at[source, line], dst_ref=slots.at[source, line], send_sem=ss.at[n],
                recv_sem=rs.at[source], device_id=peer(axes, step), device_id_type=MESH,
            ).wait_recv()
        total = total_of(slots[n, line] for n in range(len(others) + 1))
    total_out[...] = total
    for copy in x_faces + y_faces + z_faces + py_faces + edges + edge_z[0] + edge_z[1] + part_faces + pending:
        copy.wait_send()


def deliver(count, ham_in, mom_in, total_in, ham_out, mom_out, norm_out, norm, sems):
    copies = [
        pltpu.make_async_copy(mom_in, mom_out, sems.at[0]),
        pltpu.make_async_copy(ham_in, ham_out, sems.at[1]),
    ]
    for copy in copies:
        copy.start()
    total = total_in[...]
    lane = lax.broadcasted_iota(jnp.int32, total.shape, 1)
    for n, (part, cells) in enumerate(((lane < 64, count), (lane >= 64, 3.0 * count))):
        root = jnp.sqrt(jnp.sum(jnp.where(part, total, 0.0), axis=1, keepdims=True) * (1.0 / cells))
        norm[n] = root[0, 0]
    copies.append(pltpu.make_async_copy(norm, norm_out, sems.at[2]))
    copies[2].start()
    for copy in copies:
        copy.wait()


def on_device(chi_field, metric, curvature, trace_curvature, gamma_field):
    sizes = tuple(lax.axis_size(a) for a in ("gx", "gy", "gz"))
    cx, cy, cz = chi_field.shape
    dma = pltpu.SemaphoreType.DMA
    vmem = pl.BlockSpec(memory_space=pltpu.VMEM)
    block = (cx + 4, cy + 2 * TOP, cz)
    hbm = pl.BlockSpec(memory_space=pltpu.HBM)
    ham, momentum, total = pl.pallas_call(
        functools.partial(kernel, sizes),
        out_shape=(
            pltpu.VMEM(chi_field.shape, jnp.float32),
            pltpu.VMEM(gamma_field.shape, jnp.float32),
            pltpu.VMEM((1, 128), jnp.float32),
        ),
        in_specs=[pl.BlockSpec(memory_space=pltpu.HBM)] * 6,
        out_specs=(vmem, vmem, vmem),
        scratch_shapes=[
            pltpu.VMEM((17,) + block, jnp.float32),
            pltpu.VMEM(block, jnp.float32),
        ]
        + [pltpu.VMEM((cx, cy, cz), jnp.float32)] * 3
        + [pltpu.VMEM((2, 4, cy, cz), jnp.float32)] * 3
        + [
            pltpu.VMEM((GEO, cx) + block[1:], jnp.float32),
            pltpu.VMEM((2, 8, 128), jnp.float32),
            pltpu.VMEM((2, 3, 2, cy, cz), jnp.float32),
            pltpu.VMEM((3, 4, cy, cz), jnp.float32),
            pltpu.VMEM((len(Z_FIELDS), 256, 256), jnp.bfloat16),
            pltpu.VMEM((len(Z_FIELDS), cx, cy, cz), jnp.float32),
        ]
        + [pltpu.VMEM((GEO, cx, cy, cz), jnp.float32)] * 4
        + [pltpu.VMEM((2, cx * cy, cz), jnp.bfloat16)] * 3
        + [pltpu.VMEM((n, 8, 128), jnp.float32) for n in (sizes[0], sizes[1] * sizes[2])]
        + [dma((n,)) for n in (7, 6, 6, 4, 4, 2, 2, 8, 8, 2, 2)]
        + [dma((2, 2))] * 2
        + [dma((n,)) for n in (sizes[0], sizes[1] * sizes[2], 2) for _ in range(2)],
        compiler_params=pltpu.CompilerParams(
            collective_id=0, has_side_effects=True, vmem_limit_bytes=67043328 - 16 * chi_field.size - 16384
        ),
    )(chi_field, metric, curvature, trace_curvature, gamma_field, jnp.asarray(z_weights(), jnp.bfloat16))
    count = float(chi_field.size * sizes[0] * sizes[1] * sizes[2])
    return pl.pallas_call(
        functools.partial(deliver, count),
        out_shape=(
            jax.ShapeDtypeStruct(chi_field.shape, jnp.float32),
            jax.ShapeDtypeStruct(gamma_field.shape, jnp.float32),
            jax.ShapeDtypeStruct((2,), jnp.float32),
        ),
        in_specs=[vmem, vmem, vmem],
        out_specs=(hbm, hbm, hbm),
        scratch_shapes=[pltpu.SMEM((2,), jnp.float32), pltpu.SemaphoreType.DMA((3,))],
    )(*(pltpu.with_memory_space_constraint(v, pltpu.VMEM) for v in (ham, momentum, total)))


def solution(mesh):
    return jax.shard_map(
        on_device,
        mesh=mesh,
        in_specs=(
            P("gx", "gy", "gz"),
            P(None, "gx", "gy", "gz"),
            P(None, "gx", "gy", "gz"),
            P("gx", "gy", "gz"),
            P(None, "gx", "gy", "gz"),
        ),
        out_specs=(P("gx", "gy", "gz"), P(None, "gx", "gy", "gz"), P()),
        check_vma=False,
    )
```

```python
import functools

import jax
import jax.numpy as jnp
import numpy as np
from jax import lax
from jax.experimental import pallas as pl
from jax.experimental.pallas import tpu as pltpu
from jax.sharding import PartitionSpec as P

pair_index = ((0, 1, 2), (1, 3, 4), (2, 4, 5))
MESH = pl.DeviceIdType.MESH
GX, CHI, MET, CURV, TRK, GY, GZ = 0, 1, 2, 8, 14, 15, 16
GEO = 7
Z_FIELDS = tuple(range(CHI, GY)) + (GZ,)
TOP = 8


def first(m2, m1, p1, p2):
    return 8.0 * (p1 - m1) - (p2 - m2)


def second(m2, m1, c, p1, p2):
    return 16.0 * (p1 + m1) - (p2 + m2) - 30.0 * c


def total_of(terms):
    terms = list(terms)
    while len(terms) > 1:
        terms = [
            terms[n] + terms[n + 1] if n + 1 < len(terms) else terms[n]
            for n in range(0, len(terms), 2)
        ]
    return terms[0]


def sym(values, i, j):
    return values[pair_index[i][j]]


def contract(gu, values):
    return total_of(
        [gu[n] * values[n] for n in (0, 3, 5)]
        + [2.0 * total_of(gu[n] * values[n] for n in (1, 2, 4))]
    )


def z_weights():
    weights = np.zeros((len(Z_FIELDS), 256, 256), np.float32)
    for n in range(len(Z_FIELDS)):
        for z in range(128):
            for step, one, two in ((-2, 1, -1), (-1, -8, 16), (0, 0, -30), (1, 8, 16), (2, -1, -1)):
                at = z + step
                row = at if 0 <= at < 128 else 128 + 4 * n + (at + 2 if at < 0 else at - 126)
                weights[n, row, z] = one
                weights[n, row, 128 + z] = two
    return weights


def split(value):
    high = value.astype(jnp.bfloat16)
    return high, (value - high.astype(jnp.float32)).astype(jnp.bfloat16)


def along_z(value, packed, weights):
    parts = [jnp.concatenate([a, b], 1) for a, b in zip(split(value), packed)]
    return sum(jnp.dot(part, weights, preferred_element_type=jnp.float32) for part in parts)


def inverse(metric):
    g00, g01, g02, g11, g12, g22 = metric
    m00 = g11 * g22 - g12 * g12
    m01 = g02 * g12 - g01 * g22
    m02 = g01 * g12 - g02 * g11
    m11 = g00 * g22 - g02 * g02
    m12 = g01 * g02 - g00 * g12
    m22 = g00 * g11 - g01 * g01
    scale = 1.0 / (g00 * m00 + g01 * m01 + g02 * m02)
    return [m * scale for m in (m00, m01, m02, m11, m12, m22)]


def cell_math(load, load_dx, load_dy, load_z, load_zz, load_xz, load_yz):
    zpos = {f: n for n, f in enumerate(Z_FIELDS)}
    gu = inverse([load(MET + n, 0, 0) for n in range(6)])
    gu_hess = [12.0 * gu[n] if n in (0, 3, 5) else 2.0 * gu[n] for n in range(6)]

    def geo(f):
        c = load(f, 0, 0)
        xs = [load(f, s, 0) for s in (-2, -1, 1, 2)]
        ys = [load(f, 0, s) for s in (-2, -1, 1, 2)]
        n = zpos[f]
        dx = load_dx(n, 0)
        dy, dz = load_dy(n), load_z(n)
        dxx = second(xs[0], xs[1], c, xs[2], xs[3])
        dyy = second(ys[0], ys[1], c, ys[2], ys[3])
        dzz = load_zz(n)
        dxy = first(*(load_dx(n, s) for s in (-2, -1, 1, 2)))
        dxz, dyz = load_xz(n), load_yz(n)
        hess = (dxx, dxy, dxz, dyy, dyz, dzz)
        return (dx, dy, dz), total_of(gu_hess[n] * hess[n] for n in range(6))

    chi = load(CHI, 0, 0)
    dchi, chi_box = geo(CHI)
    grads = [[None] * 6 for _ in range(3)]
    boxes = []
    for n in range(6):
        d, box = geo(MET + n)
        for a in range(3):
            grads[a][n] = d[a]
        boxes.append(box)
    metric_box = contract(gu, boxes)

    raised = [
        [[total_of(sym(gu, b, l) * sym(grads[k], l, j) for l in range(3)) for j in range(3)] for b in range(3)]
        for k in range(3)
    ]
    trace = [raised[k][0][0] + raised[k][1][1] + raised[k][2][2] for k in range(3)]
    lower = [
        raised[0][0][l] + raised[1][1][l] + raised[2][2][l] - 0.5 * trace[l] for l in range(3)
    ]
    gd = [total_of(sym(gu, k, l) * lower[l] for l in range(3)) for k in range(3)]

    def trace_of(k, l):
        return total_of(raised[k][a][b] * raised[l][b][a] for a in range(3) for b in range(3))

    square = contract(gu, [trace_of(k, l) for k in range(3) for l in range(k, 3)])

    def cross_of(k, b):
        left, right = raised[k][b], raised[b][k]
        up = [total_of(sym(gu, c, j) * right[j] for j in range(3)) for c in range(3)]
        return total_of(left[c] * up[c] for c in range(3))

    cross = (
        cross_of(0, 0)
        + cross_of(1, 1)
        + cross_of(2, 2)
        + 2.0 * (cross_of(0, 1) + cross_of(0, 2) + cross_of(1, 2))
    )
    chi_up = [total_of(sym(gu, k, l) * dchi[l] for l in range(3)) for k in range(3)]
    grad_sq = total_of(chi_up[k] * dchi[k] for k in range(3))
    laplace = chi_box - total_of(gd[k] * dchi[k] for k in range(3))
    drift = total_of(gd[k] * trace[k] for k in range(3))

    def dx_of(f):
        return first(*(load(f, s, 0) for s in (-2, -1, 1, 2)))

    def dy_of(f):
        return first(*(load(f, 0, s) for s in (-2, -1, 1, 2)))

    def dz_of(f):
        return load_z(zpos[f])

    div = dx_of(GX) + dy_of(GY) + dz_of(GZ)
    inv_chi = 1.0 / chi
    curv = [load(CURV + n, 0, 0) for n in range(6)]
    mixed = [
        [total_of(sym(curv, i, k) * sym(gu, k, j) for k in range(3)) for j in range(3)] for i in range(3)
    ]
    curv_up = [
        total_of(sym(gu, i, a) * mixed[a][j] for a in range(3)) for i in range(3) for j in range(i, 3)
    ]
    curv_sq = contract(curv, curv_up)
    trk = load(TRK, 0, 0)
    ham = (
        chi * ((0.25 * square + 0.5 * (cross + drift - metric_box)) * (1.0 / 144.0) + div * (1.0 / 12.0))
        + (2.0 * laplace - 2.5 * grad_sq * inv_chi) * (1.0 / 144.0)
        + (2.0 / 3.0) * trk * trk
        - curv_sq
    )
    push = [gd[l] + 1.5 * inv_chi * chi_up[l] for l in range(3)]
    curv_grads = [[op(CURV + n) for n in range(6)] for op in (dx_of, dy_of, dz_of)]
    trace_grads = [op(TRK) for op in (dx_of, dy_of, dz_of)]
    momentum = []
    for i in range(3):
        parts = total_of(sym(gu, j, k) * sym(curv_grads[j], k, i) for j in range(3) for k in range(3))
        parts = parts - total_of(sym(curv, l, i) * push[l] for l in range(3))
        parts = parts - 0.5 * contract(curv_up, grads[i]) - (2.0 / 3.0) * trace_grads[i]
        momentum.append(parts * (1.0 / 12.0))
    return ham, momentum


def kernel(
    sizes,
    chi_in, met_in, curv_in, trk_in, gam_in, weights_in,
    ham_out, mom_out, total_out,
    cells, packed, pack_own, pack_left, pack_right, edge_own, edge_left, edge_right, slope, sums,
    part_out, part, weights, z_one, z_two, y_one, yz_two, xz_two, mid_split, dy_split, dx_split,
    slots_x,
    load_sem, xs, xr, ys, yr, zs, zr, es, er, pys, pyr, ezs, ezr,
    rxs, rxr, cs, cr, ready,
):
    nx, ny, nz = sizes
    cx, cy = chi_in.shape[0], chi_in.shape[1]
    names = ("gx", "gy", "gz")
    me = [lax.axis_index(a) for a in names]

    def moved(axis, step):
        return lax.rem(me[axis] + step + sizes[axis], sizes[axis])

    def peer(axes, steps):
        where = list(me)
        if isinstance(axes, int):
            axes, steps = (axes,), (steps,)
        for axis, step in zip(axes, steps):
            where[axis] = moved(axis, step)
        return tuple(where)

    def hops(axes):
        return [step for step in np.ndindex(*(sizes[a] for a in axes)) if any(step)]

    def place_in(axes, steps=None):
        index = 0
        for axis, step in zip(axes, steps or (0,) * len(axes)):
            index = index * sizes[axis] + moved(axis, step)
        return index

    own_x, own_y = pl.ds(2, cx), pl.ds(TOP, cy)
    loads = [
        pltpu.make_async_copy(src, dst, load_sem.at[n])
        for n, (src, dst) in enumerate(
            (
                (met_in, cells.at[pl.ds(MET, 6), own_x, own_y]),
                (chi_in, cells.at[CHI, own_x, own_y]),
                (gam_in.at[0], cells.at[GX, own_x, own_y]),
                (curv_in, cells.at[pl.ds(CURV, 6), own_x, own_y]),
                (trk_in, cells.at[TRK, own_x, own_y]),
                (gam_in.at[pl.ds(1, 2)], cells.at[pl.ds(GY, 2), own_x, own_y]),
                (weights_in, weights),
            )
        )
    ]
    for copy in loads[:6]:
        copy.start()
    barrier = pltpu.get_barrier_semaphore()
    for axes in ((1, 2), (0,)):
        for step in hops(axes):
            pl.semaphore_signal(barrier, inc=1, device_id=peer(axes, step), device_id_type=MESH)
    pl.semaphore_wait(barrier, ny * nz + nx - 2)

    for step in hops((1, 2)):
        pl.semaphore_signal(ready, inc=1, device_id=peer((1, 2), step), device_id_type=MESH)

    def send(src, dst, send_sem, recv_sem, axis, step):
        copy = pltpu.make_async_remote_copy(
            src_ref=src, dst_ref=dst, send_sem=send_sem, recv_sem=recv_sem,
            device_id=peer(axis, step), device_id_type=MESH,
        )
        copy.start()
        return copy

    low_x, high_x = pl.ds(2, 2), pl.ds(cx, 2)
    before_x, after_x = pl.ds(0, 2), pl.ds(cx + 2, 2)
    low_y, high_y = pl.ds(TOP, 2), pl.ds(TOP + cy - 2, 2)
    before_y, after_y = pl.ds(TOP - 2, 2), pl.ds(TOP + cy, 2)
    x_faces, y_faces = [], []

    def send_x(fields):
        n = len(x_faces)
        x_faces.extend((
            send(cells.at[fields, high_x, own_y], cells.at[fields, before_x, own_y], xs.at[n], xr.at[n], 0, 1),
            send(cells.at[fields, low_x, own_y], cells.at[fields, after_x, own_y], xs.at[n + 1], xr.at[n + 1], 0, -1),
        ))

    def send_y(fields):
        n = len(y_faces)
        y_faces.extend((
            send(cells.at[fields, own_x, high_y], cells.at[fields, own_x, before_y], ys.at[n], yr.at[n], 1, 1),
            send(cells.at[fields, own_x, low_y], cells.at[fields, own_x, after_y], ys.at[n + 1], yr.at[n + 1], 1, -1),
        ))

    loads[0].wait()
    send_x(pl.ds(MET, 6))
    loads[1].wait()
    send_x(pl.ds(CHI, 1))
    send_y(pl.ds(CHI, GEO))
    loads[2].wait()
    send_x(pl.ds(GX, 1))
    for copy in loads[3:6]:
        copy.wait()
    send_y(pl.ds(CURV, 8))
    loads[6].start()

    tiles = cy // 8
    group = lax.shift_right_logical(lax.broadcasted_iota(jnp.int32, (8, 128), 1), 2)
    far_side = (lax.broadcasted_iota(jnp.int32, (cy, 128), 1) & 2) != 0

    def packing(fields, target, layer):
        def pack(step, carry):
            at, y = step // tiles, lax.rem(step, tiles) * 8
            rows = pl.ds(pl.multiple_of(TOP + y, 8), 8)
            x = layer(at)
            picked = [
                jnp.where(group == n, pltpu.roll(cells[f, x, rows], 4 * n + 2, 1), 0.0)
                for n, f in enumerate(fields)
                if f is not None
            ]
            target[at, pl.ds(pl.multiple_of(y, 8), 8)] = total_of(picked)
            return carry

        lax.fori_loop(0, target.shape[0] * tiles, pack, 0, unroll=4)

    packing(Z_FIELDS, pack_own, lambda at: at + 2)

    def send_z(own, left, right, send_sem, recv_sem):
        faces = [send(own, left, send_sem.at[0], recv_sem.at[0], 2, 1)]
        if nz > 2:
            faces.append(send(own, right, send_sem.at[1], recv_sem.at[1], 2, -1))
        return faces

    def joined(left, right, at):
        return jnp.where(far_side, right[at], left[at]) if nz > 2 else left[at]

    z_faces = send_z(pack_own, pack_left, pack_right, zs, zr)
    sums[...] = jnp.zeros_like(sums)
    missing = jnp.zeros((7, 2, cy, 128), jnp.float32)
    cells[pl.ds(CURV, 7), before_x, own_y] = missing
    cells[pl.ds(CURV, 7), after_x, own_y] = missing
    for copy in z_faces:
        copy.wait_recv()

    def keep_split(target, value, at=0):
        for n, half in enumerate(split(value)):
            target[n, pl.ds(at, value.shape[0])] = half

    def merge(x, carry):
        value = joined(pack_left, pack_right, x)
        packed[x + 2, own_y] = value
        keep_split(mid_split, value, pl.multiple_of(x * cy, cy))
        return carry

    lax.fori_loop(0, cx, merge, 0)
    py_faces = [
        send(packed.at[own_x, high_y], packed.at[own_x, before_y], pys.at[0], pyr.at[0], 1, 1),
        send(packed.at[own_x, low_y], packed.at[own_x, after_y], pys.at[1], pyr.at[1], 1, -1),
    ]
    loads[6].wait()
    flat = (cx * cy, 128)

    def geo_z(n, carry):
        both = along_z(cells[n + CHI, own_x, own_y].reshape(flat), mid_split[...], weights[n])
        z_one[n] = both[:, :128].reshape(cx, cy, 128)
        z_two[n] = both[:, 128:].reshape(cx, cy, 128)
        return carry

    lax.fori_loop(0, GEO, geo_z, 0, unroll=7)

    def rest_z(n, carry):
        f = n + CHI + n // (GY - CHI)
        z_one[n] = along_z(
            cells[f, own_x, own_y].reshape(flat), mid_split[...], weights[n, :, :128]
        ).reshape(cx, cy, 128)
        return carry

    lax.fori_loop(GEO, len(Z_FIELDS), rest_z, 0, unroll=8)

    def rises(pieces):
        rows = [cx * count for _, count in pieces]
        at = 0
        for (row, count), size in zip(pieces, rows):
            values = first(*(packed[own_x, pl.ds(TOP + row + s, count)] for s in (-2, -1, 1, 2)))
            keep_split(dy_split, values.reshape(size, 128), at)
            at += size
        total = at

        def one(n, carry):
            values = []
            for (row, count), size in zip(pieces, rows):
                dy = first(*(cells[n + CHI, own_x, pl.ds(TOP + row + s, count)] for s in (-2, -1, 1, 2)))
                y_one[n, :, pl.ds(row, count)] = dy
                values.append(dy.reshape(size, 128))
            both = along_z(jnp.concatenate(values, 0), dy_split[:, :total], weights[n, :, :128])
            at = 0
            for (row, count), size in zip(pieces, rows):
                yz_two[n, :, pl.ds(row, count)] = both[at : at + size].reshape(cx, count, 128)
                at += size
            return carry

        lax.fori_loop(0, GEO, one, 0, unroll=7)

    def slopes(pieces):
        rows = [count * cy for _, count in pieces]
        at = 0
        for (base, count), size in zip(pieces, rows):
            values = first(*(packed[pl.ds(base + 2 + s, count), own_y] for s in (-2, -1, 1, 2)))
            keep_split(dx_split, values.reshape(size, 128), at)
            at += size
        total = at

        def one(n, carry):
            values = []
            for (base, count), size in zip(pieces, rows):
                dx = first(*(cells[n + CHI, pl.ds(base + 2 + s, count), own_y] for s in (-2, -1, 1, 2)))
                slope[n, pl.ds(base, count), own_y] = dx
                values.append(dx.reshape(size, 128))
            both = along_z(jnp.concatenate(values, 0), dx_split[:, :total], weights[n, :, :128])
            at = 0
            for (base, count), size in zip(pieces, rows):
                xz_two[n, pl.ds(base, count)] = both[at : at + size].reshape(count, cy, 128)
                at += size
            return carry

        lax.fori_loop(0, GEO, one, 0, unroll=7)

    def tile_at(x, y):
        rows = pl.ds(pl.multiple_of(y, 8), 8)
        ham, momentum = cell_math(
            lambda f, sx, sy: cells[f, x + 2 + sx, pl.ds(TOP + y + sy, 8)],
            lambda n, sy: slope[n, x, pl.ds(TOP + y + sy, 8)],
            lambda n: y_one[n, x, rows],
            lambda n: z_one[n, x, rows],
            lambda n: z_two[n, x, rows],
            lambda n: xz_two[n, x, rows],
            lambda n: yz_two[n, x, rows],
        )
        ham_out[x, rows] = ham
        for i in range(3):
            mom_out[i, x, rows] = momentum[i]
        sums[0] += ham * ham
        return momentum

    def rims(pieces):
        def one(n, carry):
            for base, count in pieces:
                for rows in (pl.ds(TOP - 8, 8), pl.ds(TOP + cy, 8)):
                    slope[n, pl.ds(base, count), rows] = first(
                        *(cells[n + CHI, pl.ds(base + 2 + s, count), rows] for s in (-2, -1, 1, 2))
                    )
            return carry

        lax.fori_loop(0, GEO, one, 0, unroll=7)

    def outer_x(at):
        return at + at // 2 * (cx - 4)

    def run(layers, layer, count, row, square):
        def one(n, carry):
            momentum = tile_at(layer(n // count), row(lax.rem(n, count)))
            if square:
                sums[1] += momentum[0] * momentum[0] + momentum[1] * momentum[1] + momentum[2] * momentum[2]
            return carry

        lax.fori_loop(0, layers * count, one, 0)

    inner = (cx - 4, lambda at: at + 2)
    outer = (4, outer_x)
    middle = (tiles - 2, lambda at: 8 * at + 8)
    rim = (2, lambda at: at * (cy - 8))
    rises(((8, cy - 16),))
    slopes(((2, cx - 4),))
    run(*inner, *middle, True)
    for copy in y_faces[:2] + py_faces:
        copy.wait_recv()
    rises(((0, 8), (cy - 8, 8)))
    rims(((2, cx - 4),))
    for copy in y_faces[2:]:
        copy.wait_recv()
    run(*inner, *rim, True)
    for copy in x_faces[:2]:
        copy.wait_recv()

    def offer(t, carry):
        rows = pl.ds(pl.multiple_of(TOP + t * 8, 8), 8)
        out_rows = pl.ds(pl.multiple_of(t * 8, 8), 8)
        for side, far, near, at, behind, sign in ((0, 0, 1, 2, 3, 1.0), (1, cx + 3, cx + 2, cx + 1, cx, -1.0)):
            edge = [cells[CURV + n, at, rows] * sign for n in range(7)]
            second_edge = [cells[CURV + n, behind, rows] * sign for n in range(7)]
            for place, slot, values in (
                (near, 1 - side, [8.0 * a - b for a, b in zip(edge, second_edge)]),
                (far, side, [-a for a in edge]),
            ):
                gu = inverse([cells[MET + n, place, rows] for n in range(6)])
                for i in range(3):
                    value = total_of(sym(gu, 0, k) * sym(values, k, i) for k in range(3))
                    if i == 0:
                        value = value - (2.0 / 3.0) * values[6]
                    part_out[side, i, slot, out_rows] = value * (1.0 / 12.0)
        return carry

    lax.fori_loop(0, tiles, offer, 0)
    part_faces = [
        send(part_out.at[0], part.at[:, pl.ds(2, 2)], cs.at[0], cr.at[0], 0, -1),
        send(part_out.at[1], part.at[:, pl.ds(0, 2)], cs.at[1], cr.at[1], 0, 1),
    ]
    edges, edge_z = [], []

    def relay(fields):
        for layers in (before_x, after_x):
            n = len(edges)
            edges.extend((
                send(cells.at[fields, layers, high_y], cells.at[fields, layers, before_y], es.at[n], er.at[n], 1, 1),
                send(cells.at[fields, layers, low_y], cells.at[fields, layers, after_y], es.at[n + 1], er.at[n + 1], 1, -1),
            ))

    def relay_z(fields):
        n = len(edge_z)
        packing(fields, edge_own.at[n], lambda at: at + at // 2 * cx)
        edge_z.append(send_z(edge_own.at[n], edge_left.at[n], edge_right.at[n], ezs.at[n], ezr.at[n]))

    relay(pl.ds(MET, 6))
    relay_z((None,) + tuple(range(MET, CURV)))
    for copy in x_faces[2:4]:
        copy.wait_recv()
    relay(pl.ds(CHI, 1))
    relay_z((CHI,))
    for copy in edge_z[0] + edge_z[1]:
        copy.wait_recv()
    for at in range(4):
        packed[at + at // 2 * cx, own_y] = joined(edge_left.at[0], edge_right.at[0], at) + joined(edge_left.at[1], edge_right.at[1], at)
    slopes(((0, 2), (cx - 2, 2)))
    for copy in x_faces[4:]:
        copy.wait_recv()
    run(*outer, *middle, False)
    for copy in edges:
        copy.wait_recv()
    rims(((0, 2), (cx - 2, 2)))
    run(*outer, *rim, False)
    for copy in part_faces:
        copy.wait_recv()

    def finish(n, carry):
        at, rows = n // tiles, pl.ds(pl.multiple_of(lax.rem(n, tiles) * 8, 8), 8)
        x = outer_x(at)
        momentum = [mom_out[i, x, rows] + part[i, at, rows] for i in range(3)]
        for i in range(3):
            mom_out[i, x, rows] = momentum[i]
        sums[1] += momentum[0] * momentum[0] + momentum[1] * momentum[1] + momentum[2] * momentum[2]
        return carry

    lax.fori_loop(0, 4 * tiles, finish, 0, unroll=4)

    lane = lax.broadcasted_iota(jnp.int32, (8, 128), 1)
    folded = [sums[n] + pltpu.roll(sums[n], 64, 1) for n in range(2)]
    total = jnp.sum(jnp.where(lane < 64, folded[0], folded[1]), axis=0, keepdims=True)
    line = pl.ds(0, 1)
    pl.semaphore_wait(ready, ny * nz - 1)
    pending = []
    for axes, slots, ss, rs in (((0, 1, 2), slots_x, rxs, rxr),):
        here = place_in(axes)
        slots[here, line] = total
        others = sorted(hops(axes), key=lambda step: -sum(min(a, b - a) for a, b in zip(step, sizes)))
        for n, step in enumerate(others):
            pending.append(send(slots.at[here, line], slots.at[here, line], ss.at[n], rs.at[here], axes, step))
        for n, step in enumerate(others):
            source = place_in(axes, step)
            pltpu.make_async_remote_copy(
                src_ref=slots.at[source, line], dst_ref=slots.at[source, line], send_sem=ss.at[n],
                recv_sem=rs.at[source], device_id=peer(axes, step), device_id_type=MESH,
            ).wait_recv()
        total = total_of(slots[n, line] for n in range(len(others) + 1))
    total_out[...] = total
    for copy in x_faces + y_faces + z_faces + py_faces + edges + edge_z[0] + edge_z[1] + part_faces + pending:
        copy.wait_send()


def deliver(count, ham_in, mom_in, total_in, ham_out, mom_out, norm_out, norm, sems):
    copies = [
        pltpu.make_async_copy(mom_in, mom_out, sems.at[0]),
        pltpu.make_async_copy(ham_in, ham_out, sems.at[1]),
    ]
    for copy in copies:
        copy.start()
    total = total_in[...]
    lane = lax.broadcasted_iota(jnp.int32, total.shape, 1)
    for n, (part, cells) in enumerate(((lane < 64, count), (lane >= 64, 3.0 * count))):
        root = jnp.sqrt(jnp.sum(jnp.where(part, total, 0.0), axis=1, keepdims=True) * (1.0 / cells))
        norm[n] = root[0, 0]
    copies.append(pltpu.make_async_copy(norm, norm_out, sems.at[2]))
    copies[2].start()
    for copy in copies:
        copy.wait()


def on_device(chi_field, metric, curvature, trace_curvature, gamma_field):
    sizes = tuple(lax.axis_size(a) for a in ("gx", "gy", "gz"))
    cx, cy, cz = chi_field.shape
    dma = pltpu.SemaphoreType.DMA
    vmem = pl.BlockSpec(memory_space=pltpu.VMEM)
    block = (cx + 4, cy + 2 * TOP, cz)
    hbm = pl.BlockSpec(memory_space=pltpu.HBM)
    ham, momentum, total = pl.pallas_call(
        functools.partial(kernel, sizes),
        out_shape=(
            pltpu.VMEM(chi_field.shape, jnp.float32),
            pltpu.VMEM(gamma_field.shape, jnp.float32),
            pltpu.VMEM((1, 128), jnp.float32),
        ),
        in_specs=[pl.BlockSpec(memory_space=pltpu.HBM)] * 6,
        out_specs=(vmem, vmem, vmem),
        scratch_shapes=[
            pltpu.VMEM((17,) + block, jnp.float32),
            pltpu.VMEM(block, jnp.float32),
        ]
        + [pltpu.VMEM((cx, cy, cz), jnp.float32)] * 3
        + [pltpu.VMEM((2, 4, cy, cz), jnp.float32)] * 3
        + [
            pltpu.VMEM((GEO, cx) + block[1:], jnp.float32),
            pltpu.VMEM((2, 8, 128), jnp.float32),
            pltpu.VMEM((2, 3, 2, cy, cz), jnp.float32),
            pltpu.VMEM((3, 4, cy, cz), jnp.float32),
            pltpu.VMEM((len(Z_FIELDS), 256, 256), jnp.bfloat16),
            pltpu.VMEM((len(Z_FIELDS), cx, cy, cz), jnp.float32),
        ]
        + [pltpu.VMEM((GEO, cx, cy, cz), jnp.float32)] * 4
        + [pltpu.VMEM((2, cx * cy, cz), jnp.bfloat16)] * 3
        + [pltpu.VMEM((n, 8, 128), jnp.float32) for n in (np.prod(sizes),)]
        + [dma((n,)) for n in (7, 6, 6, 4, 4, 2, 2, 8, 8, 2, 2)]
        + [dma((2, 2))] * 2
        + [dma((n,)) for n in (np.prod(sizes), 2) for _ in range(2)]
        + [pltpu.SemaphoreType.REGULAR],
        compiler_params=pltpu.CompilerParams(
            collective_id=0, has_side_effects=True, vmem_limit_bytes=67043328 - 16 * chi_field.size - 16384
        ),
    )(chi_field, metric, curvature, trace_curvature, gamma_field, jnp.asarray(z_weights(), jnp.bfloat16))
    count = float(chi_field.size * sizes[0] * sizes[1] * sizes[2])
    return pl.pallas_call(
        functools.partial(deliver, count),
        out_shape=(
            jax.ShapeDtypeStruct(chi_field.shape, jnp.float32),
            jax.ShapeDtypeStruct(gamma_field.shape, jnp.float32),
            jax.ShapeDtypeStruct((2,), jnp.float32),
        ),
        in_specs=[vmem, vmem, vmem],
        out_specs=(hbm, hbm, hbm),
        scratch_shapes=[pltpu.SMEM((2,), jnp.float32), pltpu.SemaphoreType.DMA((3,))],
    )(*(pltpu.with_memory_space_constraint(v, pltpu.VMEM) for v in (ham, momentum, total)))


def solution(mesh):
    return jax.shard_map(
        on_device,
        mesh=mesh,
        in_specs=(
            P("gx", "gy", "gz"),
            P(None, "gx", "gy", "gz"),
            P(None, "gx", "gy", "gz"),
            P("gx", "gy", "gz"),
            P(None, "gx", "gy", "gz"),
        ),
        out_specs=(P("gx", "gy", "gz"), P(None, "gx", "gy", "gz"), P()),
        check_vma=False,
    )
```

```python
import functools

import jax
import jax.numpy as jnp
import numpy as np
from jax import lax
from jax.experimental import pallas as pl
from jax.experimental.pallas import tpu as pltpu
from jax.sharding import PartitionSpec as P

pair_index = ((0, 1, 2), (1, 3, 4), (2, 4, 5))
MESH = pl.DeviceIdType.MESH
GX, CHI, MET, CURV, TRK, GY, GZ = 0, 1, 2, 8, 14, 15, 16
GEO = 7
X_MET, X_CHI, X_GX, Y_GEO, Y_REST, Y_PACK, Z_PACK, EDGE_Y, EDGE_Z, PART, NORM = range(11)
Z_FIELDS = tuple(range(CHI, GY)) + (GZ,)
TOP = 8


def first(m2, m1, p1, p2):
    return 8.0 * (p1 - m1) - (p2 - m2)


def second(m2, m1, c, p1, p2):
    return 16.0 * (p1 + m1) - (p2 + m2) - 30.0 * c


def total_of(terms):
    terms = list(terms)
    while len(terms) > 1:
        terms = [
            terms[n] + terms[n + 1] if n + 1 < len(terms) else terms[n]
            for n in range(0, len(terms), 2)
        ]
    return terms[0]


def sym(values, i, j):
    return values[pair_index[i][j]]


def contract(gu, values):
    return total_of(
        [gu[n] * values[n] for n in (0, 3, 5)]
        + [2.0 * total_of(gu[n] * values[n] for n in (1, 2, 4))]
    )


def z_weights():
    weights = np.zeros((len(Z_FIELDS), 256, 256), np.float32)
    for n in range(len(Z_FIELDS)):
        for z in range(128):
            for step, one, two in ((-2, 1, -1), (-1, -8, 16), (0, 0, -30), (1, 8, 16), (2, -1, -1)):
                at = z + step
                row = at if 0 <= at < 128 else 128 + 4 * n + (at + 2 if at < 0 else at - 126)
                weights[n, row, z] = one
                weights[n, row, 128 + z] = two
    return weights


def split(value):
    high = value.astype(jnp.bfloat16)
    return high, (value - high.astype(jnp.float32)).astype(jnp.bfloat16)


def along_z(value, packed, weights):
    parts = [jnp.concatenate([a, b], 1) for a, b in zip(split(value), packed)]
    return sum(jnp.dot(part, weights, preferred_element_type=jnp.float32) for part in parts)


def inverse(metric):
    g00, g01, g02, g11, g12, g22 = metric
    m00 = g11 * g22 - g12 * g12
    m01 = g02 * g12 - g01 * g22
    m02 = g01 * g12 - g02 * g11
    m11 = g00 * g22 - g02 * g02
    m12 = g01 * g02 - g00 * g12
    m22 = g00 * g11 - g01 * g01
    scale = 1.0 / (g00 * m00 + g01 * m01 + g02 * m02)
    return [m * scale for m in (m00, m01, m02, m11, m12, m22)]


def cell_math(load, load_dx, load_dy, load_z, load_zz, load_xz, load_yz):
    zpos = {f: n for n, f in enumerate(Z_FIELDS)}
    gu = inverse([load(MET + n, 0, 0) for n in range(6)])
    gu_hess = [12.0 * gu[n] if n in (0, 3, 5) else 2.0 * gu[n] for n in range(6)]

    def geo(f):
        c = load(f, 0, 0)
        xs = [load(f, s, 0) for s in (-2, -1, 1, 2)]
        ys = [load(f, 0, s) for s in (-2, -1, 1, 2)]
        n = zpos[f]
        dx = load_dx(n, 0)
        dy, dz = load_dy(n), load_z(n)
        dxx = second(xs[0], xs[1], c, xs[2], xs[3])
        dyy = second(ys[0], ys[1], c, ys[2], ys[3])
        dzz = load_zz(n)
        dxy = first(*(load_dx(n, s) for s in (-2, -1, 1, 2)))
        dxz, dyz = load_xz(n), load_yz(n)
        hess = (dxx, dxy, dxz, dyy, dyz, dzz)
        return (dx, dy, dz), total_of(gu_hess[n] * hess[n] for n in range(6))

    chi = load(CHI, 0, 0)
    dchi, chi_box = geo(CHI)
    grads = [[None] * 6 for _ in range(3)]
    boxes = []
    for n in range(6):
        d, box = geo(MET + n)
        for a in range(3):
            grads[a][n] = d[a]
        boxes.append(box)
    metric_box = contract(gu, boxes)

    raised = [
        [[total_of(sym(gu, b, l) * sym(grads[k], l, j) for l in range(3)) for j in range(3)] for b in range(3)]
        for k in range(3)
    ]
    trace = [raised[k][0][0] + raised[k][1][1] + raised[k][2][2] for k in range(3)]
    lower = [
        raised[0][0][l] + raised[1][1][l] + raised[2][2][l] - 0.5 * trace[l] for l in range(3)
    ]
    gd = [total_of(sym(gu, k, l) * lower[l] for l in range(3)) for k in range(3)]

    def trace_of(k, l):
        return total_of(raised[k][a][b] * raised[l][b][a] for a in range(3) for b in range(3))

    square = contract(gu, [trace_of(k, l) for k in range(3) for l in range(k, 3)])

    def cross_of(k, b):
        left, right = raised[k][b], raised[b][k]
        up = [total_of(sym(gu, c, j) * right[j] for j in range(3)) for c in range(3)]
        return total_of(left[c] * up[c] for c in range(3))

    cross = (
        cross_of(0, 0)
        + cross_of(1, 1)
        + cross_of(2, 2)
        + 2.0 * (cross_of(0, 1) + cross_of(0, 2) + cross_of(1, 2))
    )
    chi_up = [total_of(sym(gu, k, l) * dchi[l] for l in range(3)) for k in range(3)]
    grad_sq = total_of(chi_up[k] * dchi[k] for k in range(3))
    laplace = chi_box - total_of(gd[k] * dchi[k] for k in range(3))
    drift = total_of(gd[k] * trace[k] for k in range(3))

    def dx_of(f):
        return first(*(load(f, s, 0) for s in (-2, -1, 1, 2)))

    def dy_of(f):
        return first(*(load(f, 0, s) for s in (-2, -1, 1, 2)))

    def dz_of(f):
        return load_z(zpos[f])

    div = dx_of(GX) + dy_of(GY) + dz_of(GZ)
    inv_chi = 1.0 / chi
    curv = [load(CURV + n, 0, 0) for n in range(6)]
    mixed = [
        [total_of(sym(curv, i, k) * sym(gu, k, j) for k in range(3)) for j in range(3)] for i in range(3)
    ]
    curv_up = [
        total_of(sym(gu, i, a) * mixed[a][j] for a in range(3)) for i in range(3) for j in range(i, 3)
    ]
    curv_sq = contract(curv, curv_up)
    trk = load(TRK, 0, 0)
    ham = (
        chi * ((0.25 * square + 0.5 * (cross + drift - metric_box)) * (1.0 / 144.0) + div * (1.0 / 12.0))
        + (2.0 * laplace - 2.5 * grad_sq * inv_chi) * (1.0 / 144.0)
        + (2.0 / 3.0) * trk * trk
        - curv_sq
    )
    push = [gd[l] + 1.5 * inv_chi * chi_up[l] for l in range(3)]
    curv_grads = [[op(CURV + n) for n in range(6)] for op in (dx_of, dy_of, dz_of)]
    trace_grads = [op(TRK) for op in (dx_of, dy_of, dz_of)]
    momentum = []
    for i in range(3):
        parts = total_of(sym(gu, j, k) * sym(curv_grads[j], k, i) for j in range(3) for k in range(3))
        parts = parts - total_of(sym(curv, l, i) * push[l] for l in range(3))
        parts = parts - 0.5 * contract(curv_up, grads[i]) - (2.0 / 3.0) * trace_grads[i]
        momentum.append(parts * (1.0 / 12.0))
    return ham, momentum


def kernel(
    sizes,
    chi_in, met_in, curv_in, trk_in, gam_in, weights_in,
    ham_out, mom_out, total_out,
    cells, packed, pack_own, pack_in, edge_own, edge_in, slope, sums,
    part_out, part, weights, z_one, z_two, y_one, yz_two, xz_two, mid_split, dy_split, dx_split,
    slots, load_sem, sent, got, ready,
):
    nx, ny, nz = sizes
    cx, cy = chi_in.shape[0], chi_in.shape[1]
    names = ("gx", "gy", "gz")
    me = [lax.axis_index(a) for a in names]

    def moved(axis, step):
        return lax.rem(me[axis] + step + sizes[axis], sizes[axis])

    def peer(axes, steps):
        where = list(me)
        if isinstance(axes, int):
            axes, steps = (axes,), (steps,)
        for axis, step in zip(axes, steps):
            where[axis] = moved(axis, step)
        return tuple(where)

    def hops(axes):
        return [step for step in np.ndindex(*(sizes[a] for a in axes)) if any(step)]

    def place_in(axes, steps=None):
        index = 0
        for axis, step in zip(axes, steps or (0,) * len(axes)):
            index = index * sizes[axis] + moved(axis, step)
        return index

    own_x, own_y = pl.ds(2, cx), pl.ds(TOP, cy)
    loads = [
        pltpu.make_async_copy(src, dst, load_sem.at[n])
        for n, src, dst in (
            (0, met_in, cells.at[pl.ds(MET, 6), own_x, own_y]),
            (1, chi_in, cells.at[CHI, own_x, own_y]),
            (1, gam_in.at[0], cells.at[GX, own_x, own_y]),
            (2, curv_in, cells.at[pl.ds(CURV, 6), own_x, own_y]),
            (2, trk_in, cells.at[TRK, own_x, own_y]),
            (2, gam_in.at[pl.ds(1, 2)], cells.at[pl.ds(GY, 2), own_x, own_y]),
            (3, weights_in, weights),
        )
    ]
    for copy in loads[:6]:
        copy.start()
    barrier = pltpu.get_barrier_semaphore()
    for axes in ((1, 2), (0,)):
        for step in hops(axes):
            pl.semaphore_signal(barrier, inc=1, device_id=peer(axes, step), device_id_type=MESH)
    pl.semaphore_wait(barrier, ny * nz + nx - 2)

    for step in hops((1, 2)):
        pl.semaphore_signal(ready, inc=1, device_id=peer((1, 2), step), device_id_type=MESH)

    def loaded(n, ref):
        pltpu.make_async_copy(ref, ref, load_sem.at[n]).wait()

    def copy_to(src, dst, n, axes, step):
        return pltpu.make_async_remote_copy(
            src_ref=src, dst_ref=dst, send_sem=sent.at[n], recv_sem=got.at[n],
            device_id=peer(axes, step), device_id_type=MESH,
        )

    def send(src, dst, n, axes, step):
        copy_to(src, dst, n, axes, step).start()

    low_x, high_x = pl.ds(2, 2), pl.ds(cx, 2)
    before_x, after_x = pl.ds(0, 2), pl.ds(cx + 2, 2)
    low_y, high_y = pl.ds(TOP, 2), pl.ds(TOP + cy - 2, 2)
    before_y, after_y = pl.ds(TOP - 2, 2), pl.ds(TOP + cy, 2)
    geo = pl.ds(CHI, GEO)
    several = nz > 2
    bulk = {
        X_MET: cells.at[pl.ds(MET, 6), pl.ds(0, 4), own_y],
        X_CHI: cells.at[pl.ds(CHI, 1), pl.ds(0, 4), own_y],
        X_GX: cells.at[pl.ds(GX, 1), pl.ds(0, 4), own_y],
        Y_GEO: cells.at[geo, own_x, pl.ds(0, 4)],
        Y_REST: cells.at[pl.ds(CURV, 8), own_x, pl.ds(0, 4)],
        Y_PACK: packed.at[own_x, pl.ds(0, 4)],
        Z_PACK: pack_in if several else pack_in.at[0],
        EDGE_Y: cells.at[geo, pl.ds(0, 4), pl.ds(0, 4)],
        EDGE_Z: edge_in if several else edge_in.at[0],
        PART: part,
        NORM: slots.at[pl.ds(0, nx * ny * nz - 1)],
    }

    def wait_for(n):
        copy_to(bulk[n], bulk[n], n, 0, 1).wait_recv()

    def send_x(fields, n):
        send(cells.at[fields, high_x, own_y], cells.at[fields, before_x, own_y], n, 0, 1)
        send(cells.at[fields, low_x, own_y], cells.at[fields, after_x, own_y], n, 0, -1)

    def send_y(fields, n, layers=own_x):
        send(cells.at[fields, layers, high_y], cells.at[fields, layers, before_y], n, 1, 1)
        send(cells.at[fields, layers, low_y], cells.at[fields, layers, after_y], n, 1, -1)

    loaded(0, cells.at[pl.ds(MET, 6), own_x, own_y])
    send_x(pl.ds(MET, 6), X_MET)
    loaded(1, cells.at[pl.ds(GX, 2), own_x, own_y])
    send_x(pl.ds(CHI, 1), X_CHI)
    send_y(geo, Y_GEO)
    send_x(pl.ds(GX, 1), X_GX)
    loaded(2, cells.at[pl.ds(CURV, 9), own_x, own_y])
    send_y(pl.ds(CURV, 8), Y_REST)
    loads[6].start()

    tiles = cy // 8
    group = lax.shift_right_logical(lax.broadcasted_iota(jnp.int32, (8, 128), 1), 2)
    far_side = (lax.broadcasted_iota(jnp.int32, (cy, 128), 1) & 2) != 0

    def packing(fields, target, layer):
        def pack(step, carry):
            at, y = step // tiles, lax.rem(step, tiles) * 8
            rows = pl.ds(pl.multiple_of(TOP + y, 8), 8)
            x = layer(at)
            picked = [
                jnp.where(group == n, pltpu.roll(cells[f, x, rows], 4 * n + 2, 1), 0.0)
                for n, f in enumerate(fields)
                if f is not None
            ]
            target[at, pl.ds(pl.multiple_of(y, 8), 8)] = total_of(picked)
            return carry

        lax.fori_loop(0, target.shape[0] * tiles, pack, 0, unroll=4)

    packing(Z_FIELDS, pack_own, lambda at: at + 2)

    def send_z(own, target, n):
        send(own, target(0), n, 2, 1)
        if several:
            send(own, target(1), n, 2, -1)

    def joined(both):
        return jnp.where(far_side, both(1), both(0)) if several else both(0)

    send_z(pack_own, lambda side: pack_in.at[side], Z_PACK)
    sums[...] = jnp.zeros_like(sums)
    missing = jnp.zeros((7, 2, cy, 128), jnp.float32)
    cells[pl.ds(CURV, 7), before_x, own_y] = missing
    cells[pl.ds(CURV, 7), after_x, own_y] = missing
    wait_for(Z_PACK)

    def keep_split(target, value, at=0):
        for n, half in enumerate(split(value)):
            target[n, pl.ds(at, value.shape[0])] = half

    def merge(x, carry):
        value = joined(lambda side: pack_in[side, x])
        packed[x + 2, own_y] = value
        keep_split(mid_split, value, pl.multiple_of(x * cy, cy))
        return carry

    lax.fori_loop(0, cx, merge, 0)
    send(packed.at[own_x, high_y], packed.at[own_x, before_y], Y_PACK, 1, 1)
    send(packed.at[own_x, low_y], packed.at[own_x, after_y], Y_PACK, 1, -1)
    loads[6].wait()
    flat = (cx * cy, 128)

    def geo_z(n, carry):
        both = along_z(cells[n + CHI, own_x, own_y].reshape(flat), mid_split[...], weights[n])
        z_one[n] = both[:, :128].reshape(cx, cy, 128)
        z_two[n] = both[:, 128:].reshape(cx, cy, 128)
        return carry

    lax.fori_loop(0, GEO, geo_z, 0, unroll=7)

    def rest_z(n, carry):
        f = n + CHI + n // (GY - CHI)
        z_one[n] = along_z(
            cells[f, own_x, own_y].reshape(flat), mid_split[...], weights[n, :, :128]
        ).reshape(cx, cy, 128)
        return carry

    lax.fori_loop(GEO, len(Z_FIELDS), rest_z, 0, unroll=8)

    def rises(pieces):
        rows = [cx * count for _, count in pieces]
        at = 0
        for (row, count), size in zip(pieces, rows):
            values = first(*(packed[own_x, pl.ds(TOP + row + s, count)] for s in (-2, -1, 1, 2)))
            keep_split(dy_split, values.reshape(size, 128), at)
            at += size
        total = at

        def one(n, carry):
            values = []
            for (row, count), size in zip(pieces, rows):
                dy = first(*(cells[n + CHI, own_x, pl.ds(TOP + row + s, count)] for s in (-2, -1, 1, 2)))
                y_one[n, :, pl.ds(row, count)] = dy
                values.append(dy.reshape(size, 128))
            both = along_z(jnp.concatenate(values, 0), dy_split[:, :total], weights[n, :, :128])
            at = 0
            for (row, count), size in zip(pieces, rows):
                yz_two[n, :, pl.ds(row, count)] = both[at : at + size].reshape(cx, count, 128)
                at += size
            return carry

        lax.fori_loop(0, GEO, one, 0, unroll=7)

    def slopes(pieces):
        rows = [count * cy for _, count in pieces]
        at = 0
        for (base, count), size in zip(pieces, rows):
            values = first(*(packed[pl.ds(base + 2 + s, count), own_y] for s in (-2, -1, 1, 2)))
            keep_split(dx_split, values.reshape(size, 128), at)
            at += size
        total = at

        def one(n, carry):
            values = []
            for (base, count), size in zip(pieces, rows):
                dx = first(*(cells[n + CHI, pl.ds(base + 2 + s, count), own_y] for s in (-2, -1, 1, 2)))
                slope[n, pl.ds(base, count), own_y] = dx
                values.append(dx.reshape(size, 128))
            both = along_z(jnp.concatenate(values, 0), dx_split[:, :total], weights[n, :, :128])
            at = 0
            for (base, count), size in zip(pieces, rows):
                xz_two[n, pl.ds(base, count)] = both[at : at + size].reshape(count, cy, 128)
                at += size
            return carry

        lax.fori_loop(0, GEO, one, 0, unroll=7)

    def tile_at(x, y):
        rows = pl.ds(pl.multiple_of(y, 8), 8)
        ham, momentum = cell_math(
            lambda f, sx, sy: cells[f, x + 2 + sx, pl.ds(TOP + y + sy, 8)],
            lambda n, sy: slope[n, x, pl.ds(TOP + y + sy, 8)],
            lambda n: y_one[n, x, rows],
            lambda n: z_one[n, x, rows],
            lambda n: z_two[n, x, rows],
            lambda n: xz_two[n, x, rows],
            lambda n: yz_two[n, x, rows],
        )
        ham_out[x, rows] = ham
        for i in range(3):
            mom_out[i, x, rows] = momentum[i]
        sums[0] += ham * ham
        return momentum

    def rims(pieces):
        def one(n, carry):
            for base, count in pieces:
                for rows in (pl.ds(TOP - 8, 8), pl.ds(TOP + cy, 8)):
                    slope[n, pl.ds(base, count), rows] = first(
                        *(cells[n + CHI, pl.ds(base + 2 + s, count), rows] for s in (-2, -1, 1, 2))
                    )
            return carry

        lax.fori_loop(0, GEO, one, 0, unroll=7)

    def outer_x(at):
        return at + at // 2 * (cx - 4)

    def run(layers, layer, count, row, square):
        def one(n, carry):
            momentum = tile_at(layer(n // count), row(lax.rem(n, count)))
            if square:
                sums[1] += momentum[0] * momentum[0] + momentum[1] * momentum[1] + momentum[2] * momentum[2]
            return carry

        lax.fori_loop(0, layers * count, one, 0)

    inner = (cx - 4, lambda at: at + 2)
    outer = (4, outer_x)
    middle = (tiles - 2, lambda at: 8 * at + 8)
    rim = (2, lambda at: at * (cy - 8))
    rises(((8, cy - 16),))
    slopes(((2, cx - 4),))
    run(*inner, *middle, True)
    wait_for(Y_GEO)
    wait_for(Y_PACK)
    rises(((0, 8), (cy - 8, 8)))
    rims(((2, cx - 4),))
    wait_for(Y_REST)
    run(*inner, *rim, True)
    wait_for(X_MET)

    def offer(t, carry):
        rows = pl.ds(pl.multiple_of(TOP + t * 8, 8), 8)
        out_rows = pl.ds(pl.multiple_of(t * 8, 8), 8)
        for side, far, near, at, behind, sign in ((0, 0, 1, 2, 3, 1.0), (1, cx + 3, cx + 2, cx + 1, cx, -1.0)):
            edge = [cells[CURV + n, at, rows] * sign for n in range(7)]
            second_edge = [cells[CURV + n, behind, rows] * sign for n in range(7)]
            for place, slot, values in (
                (near, 1 - side, [8.0 * a - b for a, b in zip(edge, second_edge)]),
                (far, side, [-a for a in edge]),
            ):
                gu = inverse([cells[MET + n, place, rows] for n in range(6)])
                for i in range(3):
                    value = total_of(sym(gu, 0, k) * sym(values, k, i) for k in range(3))
                    if i == 0:
                        value = value - (2.0 / 3.0) * values[6]
                    part_out[side, i, slot, out_rows] = value * (1.0 / 12.0)
        return carry

    lax.fori_loop(0, tiles, offer, 0)
    send(part_out.at[0], part.at[:, pl.ds(2, 2)], PART, 0, -1)
    send(part_out.at[1], part.at[:, pl.ds(0, 2)], PART, 0, 1)

    def relay(n, fields, sliced):
        for layers in (before_x, after_x):
            send_y(sliced, EDGE_Y, layers)
        packing(fields, edge_own.at[n], lambda at: at + at // 2 * cx)
        send_z(edge_own.at[n], lambda side: edge_in.at[side, n], EDGE_Z)

    relay(0, (None,) + tuple(range(MET, CURV)), pl.ds(MET, 6))
    wait_for(X_CHI)
    relay(1, (CHI,), pl.ds(CHI, 1))
    wait_for(EDGE_Z)
    for at in range(4):
        packed[at + at // 2 * cx, own_y] = joined(lambda side: edge_in[side, 0, at] + edge_in[side, 1, at])
    slopes(((0, 2), (cx - 2, 2)))
    wait_for(X_GX)
    run(*outer, *middle, False)
    wait_for(EDGE_Y)
    rims(((0, 2), (cx - 2, 2)))
    run(*outer, *rim, False)
    wait_for(PART)

    def finish(n, carry):
        at, rows = n // tiles, pl.ds(pl.multiple_of(lax.rem(n, tiles) * 8, 8), 8)
        x = outer_x(at)
        momentum = [mom_out[i, x, rows] + part[i, at, rows] for i in range(3)]
        for i in range(3):
            mom_out[i, x, rows] = momentum[i]
        sums[1] += momentum[0] * momentum[0] + momentum[1] * momentum[1] + momentum[2] * momentum[2]
        return carry

    lax.fori_loop(0, 4 * tiles, finish, 0, unroll=4)

    lane = lax.broadcasted_iota(jnp.int32, (8, 128), 1)
    folded = [sums[n] + pltpu.roll(sums[n], 64, 1) for n in range(2)]
    total = jnp.sum(jnp.where(lane < 64, folded[0], folded[1]), axis=0, keepdims=True)
    pl.semaphore_wait(ready, ny * nz - 1)
    axes = (0, 1, 2)
    here = pl.ds(place_in(axes), 1)
    slots[here] = total
    for step in sorted(hops(axes), key=lambda step: -sum(min(a, b - a) for a, b in zip(step, sizes))):
        send(slots.at[here], slots.at[here], NORM, axes, step)
    wait_for(NORM)
    total_out[...] = jnp.sum(slots[...], axis=0, keepdims=True)
    for n, ref in bulk.items():
        copy_to(ref, ref, n, 0, 1).wait_send()


def deliver(count, ham_in, mom_in, total_in, ham_out, mom_out, norm_out, norm, sems):
    copies = [
        pltpu.make_async_copy(mom_in, mom_out, sems.at[0]),
        pltpu.make_async_copy(ham_in, ham_out, sems.at[1]),
    ]
    for copy in copies:
        copy.start()
    total = total_in[...]
    lane = lax.broadcasted_iota(jnp.int32, total.shape, 1)
    for n, (part, cells) in enumerate(((lane < 64, count), (lane >= 64, 3.0 * count))):
        root = jnp.sqrt(jnp.sum(jnp.where(part, total, 0.0), axis=1, keepdims=True) * (1.0 / cells))
        norm[n] = root[0, 0]
    copies.append(pltpu.make_async_copy(norm, norm_out, sems.at[2]))
    copies[2].start()
    for copy in copies:
        copy.wait()


def on_device(chi_field, metric, curvature, trace_curvature, gamma_field):
    sizes = tuple(lax.axis_size(a) for a in ("gx", "gy", "gz"))
    cx, cy, cz = chi_field.shape
    dma = pltpu.SemaphoreType.DMA
    vmem = pl.BlockSpec(memory_space=pltpu.VMEM)
    block = (cx + 4, cy + 2 * TOP, cz)
    hbm = pl.BlockSpec(memory_space=pltpu.HBM)
    ham, momentum, total = pl.pallas_call(
        functools.partial(kernel, sizes),
        out_shape=(
            pltpu.VMEM(chi_field.shape, jnp.float32),
            pltpu.VMEM(gamma_field.shape, jnp.float32),
            pltpu.VMEM((1, 128), jnp.float32),
        ),
        in_specs=[pl.BlockSpec(memory_space=pltpu.HBM)] * 6,
        out_specs=(vmem, vmem, vmem),
        scratch_shapes=[
            pltpu.VMEM((17,) + block, jnp.float32),
            pltpu.VMEM(block, jnp.float32),
        ]
        + [pltpu.VMEM(shape + (cy, cz), jnp.float32) for shape in ((cx,), (2, cx), (2, 4), (2, 2, 4))]
        + [
            pltpu.VMEM((GEO, cx) + block[1:], jnp.float32),
            pltpu.VMEM((2, 8, 128), jnp.float32),
            pltpu.VMEM((2, 3, 2, cy, cz), jnp.float32),
            pltpu.VMEM((3, 4, cy, cz), jnp.float32),
            pltpu.VMEM((len(Z_FIELDS), 256, 256), jnp.bfloat16),
            pltpu.VMEM((len(Z_FIELDS), cx, cy, cz), jnp.float32),
        ]
        + [pltpu.VMEM((GEO, cx, cy, cz), jnp.float32)] * 4
        + [pltpu.VMEM((2, cx * cy, cz), jnp.bfloat16)] * 3
        + [pltpu.VMEM((np.prod(sizes), 128), jnp.float32), dma((4,)), dma((11,)), dma((11,))]
        + [pltpu.SemaphoreType.REGULAR],
        compiler_params=pltpu.CompilerParams(
            collective_id=0, has_side_effects=True, vmem_limit_bytes=67043328 - 16 * chi_field.size - 16384
        ),
    )(chi_field, metric, curvature, trace_curvature, gamma_field, jnp.asarray(z_weights(), jnp.bfloat16))
    count = float(chi_field.size * sizes[0] * sizes[1] * sizes[2])
    return pl.pallas_call(
        functools.partial(deliver, count),
        out_shape=(
            jax.ShapeDtypeStruct(chi_field.shape, jnp.float32),
            jax.ShapeDtypeStruct(gamma_field.shape, jnp.float32),
            jax.ShapeDtypeStruct((2,), jnp.float32),
        ),
        in_specs=[vmem, vmem, vmem],
        out_specs=(hbm, hbm, hbm),
        scratch_shapes=[pltpu.SMEM((2,), jnp.float32), pltpu.SemaphoreType.DMA((3,))],
    )(*(pltpu.with_memory_space_constraint(v, pltpu.VMEM) for v in (ham, momentum, total)))


def solution(mesh):
    return jax.shard_map(
        on_device,
        mesh=mesh,
        in_specs=(
            P("gx", "gy", "gz"),
            P(None, "gx", "gy", "gz"),
            P(None, "gx", "gy", "gz"),
            P("gx", "gy", "gz"),
            P(None, "gx", "gy", "gz"),
        ),
        out_specs=(P("gx", "gy", "gz"), P(None, "gx", "gy", "gz"), P()),
        check_vma=False,
    )
```

```python
import functools

import jax
import jax.numpy as jnp
import numpy as np
from jax import lax
from jax.experimental import pallas as pl
from jax.experimental.pallas import tpu as pltpu
from jax.sharding import PartitionSpec as P

pair_index = ((0, 1, 2), (1, 3, 4), (2, 4, 5))
MESH = pl.DeviceIdType.MESH
GX, CHI, MET, CURV, TRK, GY, GZ = 0, 1, 2, 8, 14, 15, 16
GEO = 7
X_MET, X_CHI, X_GX, Y_GEO, Y_REST, Y_PACK, Z_PACK, EDGE_Y, EDGE_Z, PART, NORM = range(11)
Z_FIELDS = tuple(range(CHI, GY)) + (GZ,)
TOP = 8


def first(m2, m1, p1, p2):
    return 8.0 * (p1 - m1) - (p2 - m2)


def second(m2, m1, c, p1, p2):
    return 16.0 * (p1 + m1) - (p2 + m2) - 30.0 * c


def total_of(terms):
    terms = list(terms)
    while len(terms) > 1:
        terms = [
            terms[n] + terms[n + 1] if n + 1 < len(terms) else terms[n]
            for n in range(0, len(terms), 2)
        ]
    return terms[0]


def sym(values, i, j):
    return values[pair_index[i][j]]


def contract(gu, values):
    return total_of(
        [gu[n] * values[n] for n in (0, 3, 5)]
        + [2.0 * total_of(gu[n] * values[n] for n in (1, 2, 4))]
    )


def z_weights():
    weights = np.zeros((len(Z_FIELDS), 256, 256), np.float32)
    for n in range(len(Z_FIELDS)):
        for z in range(128):
            for step, one, two in ((-2, 1, -1), (-1, -8, 16), (0, 0, -30), (1, 8, 16), (2, -1, -1)):
                at = z + step
                row = at if 0 <= at < 128 else 128 + 4 * n + (at + 2 if at < 0 else at - 126)
                weights[n, row, z] = one
                weights[n, row, 128 + z] = two
    return weights


def split(value):
    high = value.astype(jnp.bfloat16)
    return high, (value - high.astype(jnp.float32)).astype(jnp.bfloat16)


def along_z(value, packed, weights):
    parts = [jnp.concatenate([a, b], 1) for a, b in zip(split(value), packed)]
    return sum(jnp.dot(part, weights, preferred_element_type=jnp.float32) for part in parts)


def inverse(metric):
    g00, g01, g02, g11, g12, g22 = metric
    m00 = g11 * g22 - g12 * g12
    m01 = g02 * g12 - g01 * g22
    m02 = g01 * g12 - g02 * g11
    m11 = g00 * g22 - g02 * g02
    m12 = g01 * g02 - g00 * g12
    m22 = g00 * g11 - g01 * g01
    scale = 1.0 / (g00 * m00 + g01 * m01 + g02 * m02)
    return [m * scale for m in (m00, m01, m02, m11, m12, m22)]


def cell_math(load, load_dx, load_dy, load_z, load_zz, load_xz, load_yz, whole):
    zpos = {f: n for n, f in enumerate(Z_FIELDS)}
    gu = inverse([load(MET + n, 0, 0) for n in range(6)])
    gu_hess = [12.0 * gu[n] if n in (0, 3, 5) else 2.0 * gu[n] for n in range(6)]

    def geo(f):
        c = load(f, 0, 0)
        xs = [load(f, s, 0) for s in (-2, -1, 1, 2)]
        ys = [load(f, 0, s) for s in (-2, -1, 1, 2)]
        n = zpos[f]
        dx = load_dx(n, 0)
        dy, dz = load_dy(n), load_z(n)
        dxx = second(xs[0], xs[1], c, xs[2], xs[3])
        dyy = second(ys[0], ys[1], c, ys[2], ys[3])
        hess = {0: dxx, 3: dyy, 4: load_yz(n), 5: load_zz(n)}
        if whole:
            hess[1] = first(*(load_dx(n, s) for s in (-2, -1, 1, 2)))
            hess[2] = load_xz(n)
        return (dx, dy, dz), total_of(gu_hess[k] * hess[k] for k in sorted(hess))

    chi = load(CHI, 0, 0)
    dchi, chi_box = geo(CHI)
    grads = [[None] * 6 for _ in range(3)]
    boxes = []
    for n in range(6):
        d, box = geo(MET + n)
        for a in range(3):
            grads[a][n] = d[a]
        boxes.append(box)
    metric_box = contract(gu, boxes)

    raised = [
        [[total_of(sym(gu, b, l) * sym(grads[k], l, j) for l in range(3)) for j in range(3)] for b in range(3)]
        for k in range(3)
    ]
    trace = [raised[k][0][0] + raised[k][1][1] + raised[k][2][2] for k in range(3)]
    lower = [
        raised[0][0][l] + raised[1][1][l] + raised[2][2][l] - 0.5 * trace[l] for l in range(3)
    ]
    gd = [total_of(sym(gu, k, l) * lower[l] for l in range(3)) for k in range(3)]

    def trace_of(k, l):
        return total_of(raised[k][a][b] * raised[l][b][a] for a in range(3) for b in range(3))

    square = contract(gu, [trace_of(k, l) for k in range(3) for l in range(k, 3)])

    def cross_of(k, b):
        left, right = raised[k][b], raised[b][k]
        up = [total_of(sym(gu, c, j) * right[j] for j in range(3)) for c in range(3)]
        return total_of(left[c] * up[c] for c in range(3))

    cross = (
        cross_of(0, 0)
        + cross_of(1, 1)
        + cross_of(2, 2)
        + 2.0 * (cross_of(0, 1) + cross_of(0, 2) + cross_of(1, 2))
    )
    chi_up = [total_of(sym(gu, k, l) * dchi[l] for l in range(3)) for k in range(3)]
    grad_sq = total_of(chi_up[k] * dchi[k] for k in range(3))
    laplace = chi_box - total_of(gd[k] * dchi[k] for k in range(3))
    drift = total_of(gd[k] * trace[k] for k in range(3))

    def dx_of(f):
        return first(*(load(f, s, 0) for s in (-2, -1, 1, 2)))

    def dy_of(f):
        return first(*(load(f, 0, s) for s in (-2, -1, 1, 2)))

    def dz_of(f):
        return load_z(zpos[f])

    div = dy_of(GY) + dz_of(GZ)
    if whole:
        div = dx_of(GX) + div
    inv_chi = 1.0 / chi
    curv = [load(CURV + n, 0, 0) for n in range(6)]
    mixed = [
        [total_of(sym(curv, i, k) * sym(gu, k, j) for k in range(3)) for j in range(3)] for i in range(3)
    ]
    curv_up = [
        total_of(sym(gu, i, a) * mixed[a][j] for a in range(3)) for i in range(3) for j in range(i, 3)
    ]
    curv_sq = contract(curv, curv_up)
    trk = load(TRK, 0, 0)
    ham = (
        chi * ((0.25 * square + 0.5 * (cross + drift - metric_box)) * (1.0 / 144.0) + div * (1.0 / 12.0))
        + (2.0 * laplace - 2.5 * grad_sq * inv_chi) * (1.0 / 144.0)
        + (2.0 / 3.0) * trk * trk
        - curv_sq
    )
    push = [gd[l] + 1.5 * inv_chi * chi_up[l] for l in range(3)]
    curv_grads = [[op(CURV + n) for n in range(6)] for op in (dx_of, dy_of, dz_of)]
    trace_grads = [op(TRK) for op in (dx_of, dy_of, dz_of)]
    momentum = []
    for i in range(3):
        parts = total_of(sym(gu, j, k) * sym(curv_grads[j], k, i) for j in range(3) for k in range(3))
        parts = parts - total_of(sym(curv, l, i) * push[l] for l in range(3))
        parts = parts - 0.5 * contract(curv_up, grads[i]) - (2.0 / 3.0) * trace_grads[i]
        momentum.append(parts * (1.0 / 12.0))
    return ham, momentum


def kernel(
    sizes,
    chi_in, met_in, curv_in, trk_in, gam_in, weights_in,
    ham_out, mom_out, total_out,
    cells, packed, pack_own, pack_in, edge_own, edge_in, slope, sums,
    part_out, part, weights, z_one, z_two, y_one, yz_two, xz_two, mid_split, dy_split, dx_split,
    slots, load_sem, sent, got, ready,
):
    nx, ny, nz = sizes
    cx, cy = chi_in.shape[0], chi_in.shape[1]
    names = ("gx", "gy", "gz")
    me = [lax.axis_index(a) for a in names]

    def moved(axis, step):
        return lax.rem(me[axis] + step + sizes[axis], sizes[axis])

    def peer(axes, steps):
        where = list(me)
        if isinstance(axes, int):
            axes, steps = (axes,), (steps,)
        for axis, step in zip(axes, steps):
            where[axis] = moved(axis, step)
        return tuple(where)

    def hops(axes):
        return [step for step in np.ndindex(*(sizes[a] for a in axes)) if any(step)]

    def place_in(axes, steps=None):
        index = 0
        for axis, step in zip(axes, steps or (0,) * len(axes)):
            index = index * sizes[axis] + moved(axis, step)
        return index

    own_x, own_y = pl.ds(2, cx), pl.ds(TOP, cy)
    loads = [
        pltpu.make_async_copy(src, dst, load_sem.at[n])
        for n, src, dst in (
            (0, met_in, cells.at[pl.ds(MET, 6), own_x, own_y]),
            (1, chi_in, cells.at[CHI, own_x, own_y]),
            (1, gam_in.at[0], cells.at[GX, own_x, own_y]),
            (2, curv_in, cells.at[pl.ds(CURV, 6), own_x, own_y]),
            (2, trk_in, cells.at[TRK, own_x, own_y]),
            (2, gam_in.at[pl.ds(1, 2)], cells.at[pl.ds(GY, 2), own_x, own_y]),
            (3, weights_in, weights),
        )
    ]
    for copy in loads[:6]:
        copy.start()
    barrier = pltpu.get_barrier_semaphore()
    for axes in ((1, 2), (0,)):
        for step in hops(axes):
            pl.semaphore_signal(barrier, inc=1, device_id=peer(axes, step), device_id_type=MESH)
    pl.semaphore_wait(barrier, ny * nz + nx - 2)

    for step in hops((1, 2)):
        pl.semaphore_signal(ready, inc=1, device_id=peer((1, 2), step), device_id_type=MESH)

    def loaded(n, ref):
        pltpu.make_async_copy(ref, ref, load_sem.at[n]).wait()

    def copy_to(src, dst, n, axes, step):
        return pltpu.make_async_remote_copy(
            src_ref=src, dst_ref=dst, send_sem=sent.at[n], recv_sem=got.at[n],
            device_id=peer(axes, step), device_id_type=MESH,
        )

    def send(src, dst, n, axes, step):
        copy_to(src, dst, n, axes, step).start()

    low_x, high_x = pl.ds(2, 2), pl.ds(cx, 2)
    before_x, after_x = pl.ds(0, 2), pl.ds(cx + 2, 2)
    low_y, high_y = pl.ds(TOP, 2), pl.ds(TOP + cy - 2, 2)
    before_y, after_y = pl.ds(TOP - 2, 2), pl.ds(TOP + cy, 2)
    geo = pl.ds(CHI, GEO)
    several = nz > 2
    bulk = {
        X_MET: cells.at[pl.ds(MET, 6), pl.ds(0, 4), own_y],
        X_CHI: cells.at[pl.ds(CHI, 1), pl.ds(0, 4), own_y],
        X_GX: cells.at[pl.ds(GX, 1), pl.ds(0, 4), own_y],
        Y_GEO: cells.at[geo, own_x, pl.ds(0, 4)],
        Y_REST: cells.at[pl.ds(CURV, 8), own_x, pl.ds(0, 4)],
        Y_PACK: packed.at[own_x, pl.ds(0, 4)],
        Z_PACK: pack_in if several else pack_in.at[0],
        EDGE_Y: cells.at[geo, pl.ds(0, 4), pl.ds(0, 4)],
        EDGE_Z: edge_in if several else edge_in.at[0],
        PART: part,
        NORM: slots.at[pl.ds(0, nx * ny * nz - 1)],
    }

    def wait_for(n):
        copy_to(bulk[n], bulk[n], n, 0, 1).wait_recv()

    def each_way(axis, ahead, back):
        odd = lax.rem(me[axis], 2) == 1

        @pl.when(odd)
        def _():
            ahead()
            back()

        @pl.when(jnp.logical_not(odd))
        def _():
            back()
            ahead()

    def send_x(fields, n):
        each_way(
            0,
            lambda: send(cells.at[fields, high_x, own_y], cells.at[fields, before_x, own_y], n, 0, 1),
            lambda: send(cells.at[fields, low_x, own_y], cells.at[fields, after_x, own_y], n, 0, -1),
        )

    def send_y(fields, n, layers=own_x):
        each_way(
            1,
            lambda: send(cells.at[fields, layers, high_y], cells.at[fields, layers, before_y], n, 1, 1),
            lambda: send(cells.at[fields, layers, low_y], cells.at[fields, layers, after_y], n, 1, -1),
        )

    loaded(0, cells.at[pl.ds(MET, 6), own_x, own_y])
    send_x(pl.ds(MET, 6), X_MET)
    loaded(1, cells.at[pl.ds(GX, 2), own_x, own_y])
    send_x(pl.ds(CHI, 1), X_CHI)
    send_y(geo, Y_GEO)
    send_x(pl.ds(GX, 1), X_GX)
    loaded(2, cells.at[pl.ds(CURV, 9), own_x, own_y])
    send_y(pl.ds(CURV, 8), Y_REST)
    loads[6].start()

    tiles = cy // 8
    group = lax.shift_right_logical(lax.broadcasted_iota(jnp.int32, (8, 128), 1), 2)
    far_side = (lax.broadcasted_iota(jnp.int32, (cy, 128), 1) & 2) != 0

    def packing(fields, target, layer, unroll):
        def pack(step, carry):
            at, y = step // tiles, lax.rem(step, tiles) * 8
            rows = pl.ds(pl.multiple_of(TOP + y, 8), 8)
            x = layer(at)
            picked = [
                jnp.where(group == n, pltpu.roll(cells[f, x, rows], 4 * n + 2, 1), 0.0)
                for n, f in enumerate(fields)
                if f is not None
            ]
            target[at, pl.ds(pl.multiple_of(y, 8), 8)] = total_of(picked)
            return carry

        lax.fori_loop(0, target.shape[0] * tiles, pack, 0, unroll=unroll)

    packing(Z_FIELDS, pack_own, lambda at: at + 2, 4)

    def send_z(own, target, n):
        send(own, target(0), n, 2, 1)
        if several:
            send(own, target(1), n, 2, -1)

    def joined(both):
        return jnp.where(far_side, both(1), both(0)) if several else both(0)

    send_z(pack_own, lambda side: pack_in.at[side], Z_PACK)
    sums[...] = jnp.zeros_like(sums)
    missing = jnp.zeros((7, 2, cy, 128), jnp.float32)
    cells[pl.ds(CURV, 7), before_x, own_y] = missing
    cells[pl.ds(CURV, 7), after_x, own_y] = missing
    wait_for(Z_PACK)

    def keep_split(target, value, at=0):
        for n, half in enumerate(split(value)):
            target[n, pl.ds(at, value.shape[0])] = half

    def merge(x, carry):
        value = joined(lambda side: pack_in[side, x])
        packed[x + 2, own_y] = value
        keep_split(mid_split, value, pl.multiple_of(x * cy, cy))
        return carry

    lax.fori_loop(0, cx, merge, 0)
    send(packed.at[own_x, high_y], packed.at[own_x, before_y], Y_PACK, 1, 1)
    send(packed.at[own_x, low_y], packed.at[own_x, after_y], Y_PACK, 1, -1)
    loads[6].wait()
    flat = (cx * cy, 128)

    def geo_z(n, carry):
        both = along_z(cells[n + CHI, own_x, own_y].reshape(flat), mid_split[...], weights[n])
        z_one[n] = both[:, :128].reshape(cx, cy, 128)
        z_two[n] = both[:, 128:].reshape(cx, cy, 128)
        return carry

    lax.fori_loop(0, GEO, geo_z, 0, unroll=7)

    def rest_z(n, carry):
        f = n + CHI + n // (GY - CHI)
        z_one[n] = along_z(
            cells[f, own_x, own_y].reshape(flat), mid_split[...], weights[n, :, :128]
        ).reshape(cx, cy, 128)
        return carry

    lax.fori_loop(GEO, len(Z_FIELDS), rest_z, 0, unroll=8)

    def rises(pieces):
        rows = [cx * count for _, count in pieces]
        at = 0
        for (row, count), size in zip(pieces, rows):
            values = first(*(packed[own_x, pl.ds(TOP + row + s, count)] for s in (-2, -1, 1, 2)))
            keep_split(dy_split, values.reshape(size, 128), at)
            at += size
        total = at

        def one(n, carry):
            values = []
            for (row, count), size in zip(pieces, rows):
                dy = first(*(cells[n + CHI, own_x, pl.ds(TOP + row + s, count)] for s in (-2, -1, 1, 2)))
                y_one[n, :, pl.ds(row, count)] = dy
                values.append(dy.reshape(size, 128))
            both = along_z(jnp.concatenate(values, 0), dy_split[:, :total], weights[n, :, :128])
            at = 0
            for (row, count), size in zip(pieces, rows):
                yz_two[n, :, pl.ds(row, count)] = both[at : at + size].reshape(cx, count, 128)
                at += size
            return carry

        lax.fori_loop(0, GEO, one, 0, unroll=7)

    def climbs(pieces, fields):
        def one(n, carry):
            for base, count in pieces:
                slope[n, pl.ds(base, count), own_y] = first(
                    *(cells[n + CHI, pl.ds(base + 2 + s, count), own_y] for s in (-2, -1, 1, 2))
                )
            return carry

        lax.fori_loop(*fields, one, 0, unroll=fields[1] - fields[0])

    def slopes(pieces):
        rows = [count * cy for _, count in pieces]
        at = 0
        for (base, count), size in zip(pieces, rows):
            values = first(*(packed[pl.ds(base + 2 + s, count), own_y] for s in (-2, -1, 1, 2)))
            keep_split(dx_split, values.reshape(size, 128), at)
            at += size
        total = at

        def one(n, carry):
            values = [slope[n, pl.ds(base, count), own_y].reshape(size, 128) for (base, count), size in zip(pieces, rows)]
            both = along_z(jnp.concatenate(values, 0), dx_split[:, :total], weights[n, :, :128])
            at = 0
            for (base, count), size in zip(pieces, rows):
                xz_two[n, pl.ds(base, count)] = both[at : at + size].reshape(count, cy, 128)
                at += size
            return carry

        lax.fori_loop(0, GEO, one, 0, unroll=7)

    def tile_at(x, y, whole):
        rows = pl.ds(pl.multiple_of(y, 8), 8)
        ham, momentum = cell_math(
            lambda f, sx, sy: cells[f, x + 2 + sx, pl.ds(TOP + y + sy, 8)],
            lambda n, sy: slope[n, x, pl.ds(TOP + y + sy, 8)],
            lambda n: y_one[n, x, rows],
            lambda n: z_one[n, x, rows],
            lambda n: z_two[n, x, rows],
            lambda n: xz_two[n, x, rows],
            lambda n: yz_two[n, x, rows],
            whole,
        )
        ham_out[x, rows] = ham
        for i in range(3):
            mom_out[i, x, rows] = momentum[i]
        if whole:
            sums[0] += ham * ham
            sums[1] += momentum[0] * momentum[0] + momentum[1] * momentum[1] + momentum[2] * momentum[2]

    def rims(pieces):
        def one(n, carry):
            for base, count in pieces:
                for rows in (pl.ds(TOP - 8, 8), pl.ds(TOP + cy, 8)):
                    slope[n, pl.ds(base, count), rows] = first(
                        *(cells[n + CHI, pl.ds(base + 2 + s, count), rows] for s in (-2, -1, 1, 2))
                    )
            return carry

        lax.fori_loop(0, GEO, one, 0, unroll=7)

    def outer_x(at):
        return at + at // 2 * (cx - 4)

    def run(layers, layer, count, row, whole):
        def one(n, carry):
            tile_at(layer(n // count), row(lax.rem(n, count)), whole)
            return carry

        lax.fori_loop(0, layers * count, one, 0)

    inner = (cx - 4, lambda at: at + 2)
    outer = (4, outer_x)
    every = (tiles, lambda at: 8 * at)
    middle = (tiles - 2, lambda at: 8 * at + 8)
    rim = (2, lambda at: at * (cy - 8))
    rises(((8, cy - 16),))
    climbs(((2, cx - 4),), (0, GEO))
    slopes(((2, cx - 4),))
    run(*inner, *middle, True)
    wait_for(Y_GEO)
    wait_for(Y_PACK)
    rises(((0, 8), (cy - 8, 8)))
    rims(((2, cx - 4),))
    wait_for(Y_REST)
    run(*inner, *rim, True)
    wait_for(X_MET)

    def offer(t, carry):
        rows = pl.ds(pl.multiple_of(TOP + t * 8, 8), 8)
        out_rows = pl.ds(pl.multiple_of(t * 8, 8), 8)
        for side, far, near, at, behind, sign in ((0, 0, 1, 2, 3, 1.0), (1, cx + 3, cx + 2, cx + 1, cx, -1.0)):
            edge = [cells[CURV + n, at, rows] * sign for n in range(7)]
            second_edge = [cells[CURV + n, behind, rows] * sign for n in range(7)]
            for place, slot, values in (
                (near, 1 - side, [8.0 * a - b for a, b in zip(edge, second_edge)]),
                (far, side, [-a for a in edge]),
            ):
                gu = inverse([cells[MET + n, place, rows] for n in range(6)])
                for i in range(3):
                    value = total_of(sym(gu, 0, k) * sym(values, k, i) for k in range(3))
                    if i == 0:
                        value = value - (2.0 / 3.0) * values[6]
                    part_out[side, i, slot, out_rows] = value * (1.0 / 12.0)
        return carry

    lax.fori_loop(0, tiles, offer, 0)
    each_way(
        0,
        lambda: send(part_out.at[1], part.at[:, pl.ds(0, 2)], PART, 0, 1),
        lambda: send(part_out.at[0], part.at[:, pl.ds(2, 2)], PART, 0, -1),
    )

    def relay(n, fields, sliced, unroll):
        for layers in (before_x, after_x):
            send_y(sliced, EDGE_Y, layers)
        packing(fields, edge_own.at[n], lambda at: at + at // 2 * cx, unroll)
        send_z(edge_own.at[n], lambda side: edge_in.at[side, n], EDGE_Z)

    ends = ((0, 2), (cx - 2, 2))
    relay(0, (None,) + tuple(range(MET, CURV)), pl.ds(MET, 6), 4)
    climbs(ends, (1, GEO))
    wait_for(X_CHI)
    relay(1, (CHI,), pl.ds(CHI, 1), 4)
    climbs(ends, (0, 1))
    run(*outer, *every, False)
    wait_for(EDGE_Z)
    for at in range(4):
        packed[at + at // 2 * cx, own_y] = joined(lambda side: edge_in[side, 0, at] + edge_in[side, 1, at])
    slopes(ends)
    wait_for(EDGE_Y)
    rims(ends)
    wait_for(X_GX)

    def mend(n, carry):
        x, y = outer_x(n // tiles), lax.rem(n, tiles) * 8
        rows = pl.ds(pl.multiple_of(y, 8), 8)
        here = pl.ds(pl.multiple_of(TOP + y, 8), 8)
        chi, *metric = [cells[CHI + k, x + 2, here] for k in range(GEO)]
        gu = inverse(metric)
        chi_part, *parts = [
            gu[1] * first(*(slope[k, x, pl.ds(TOP + y + s, 8)] for s in (-2, -1, 1, 2))) + gu[2] * xz_two[k, x, rows]
            for k in range(GEO)
        ]
        div = first(*(cells[GX, x + 2 + s, here] for s in (-2, -1, 1, 2)))
        ham = ham_out[x, rows] + (
            (4.0 * chi_part - chi * contract(gu, parts)) * (1.0 / 144.0) + chi * div * (1.0 / 12.0)
        )
        ham_out[x, rows] = ham
        sums[0] += ham * ham
        return carry

    lax.fori_loop(0, 4 * tiles, mend, 0, unroll=2)
    wait_for(PART)

    def finish(n, carry):
        at, rows = n // tiles, pl.ds(pl.multiple_of(lax.rem(n, tiles) * 8, 8), 8)
        x = outer_x(at)
        momentum = [mom_out[i, x, rows] + part[i, at, rows] for i in range(3)]
        for i in range(3):
            mom_out[i, x, rows] = momentum[i]
        sums[1] += momentum[0] * momentum[0] + momentum[1] * momentum[1] + momentum[2] * momentum[2]
        return carry

    lax.fori_loop(0, 4 * tiles, finish, 0, unroll=16)

    lane = lax.broadcasted_iota(jnp.int32, (8, 128), 1)
    folded = [sums[n] + pltpu.roll(sums[n], 64, 1) for n in range(2)]
    total = jnp.sum(jnp.where(lane < 64, folded[0], folded[1]), axis=0, keepdims=True)
    pl.semaphore_wait(ready, ny * nz - 1)
    axes = (0, 1, 2)
    here = pl.ds(place_in(axes), 1)
    slots[here] = total
    for step in sorted(hops(axes), key=lambda step: -sum(min(a, b - a) for a, b in zip(step, sizes))):
        send(slots.at[here], slots.at[here], NORM, axes, step)
    wait_for(NORM)
    total_out[...] = jnp.sum(slots[...], axis=0, keepdims=True)
    for n, ref in bulk.items():
        copy_to(ref, ref, n, 0, 1).wait_send()


def deliver(count, ham_in, mom_in, total_in, ham_out, mom_out, norm_out, norm, sems):
    copies = [
        pltpu.make_async_copy(mom_in, mom_out, sems.at[0]),
        pltpu.make_async_copy(ham_in, ham_out, sems.at[1]),
    ]
    for copy in copies:
        copy.start()
    total = total_in[...]
    lane = lax.broadcasted_iota(jnp.int32, total.shape, 1)
    for n, (part, cells) in enumerate(((lane < 64, count), (lane >= 64, 3.0 * count))):
        root = jnp.sqrt(jnp.sum(jnp.where(part, total, 0.0), axis=1, keepdims=True) * (1.0 / cells))
        norm[n] = root[0, 0]
    copies.append(pltpu.make_async_copy(norm, norm_out, sems.at[2]))
    copies[2].start()
    for copy in copies:
        copy.wait()


def on_device(chi_field, metric, curvature, trace_curvature, gamma_field):
    sizes = tuple(lax.axis_size(a) for a in ("gx", "gy", "gz"))
    cx, cy, cz = chi_field.shape
    dma = pltpu.SemaphoreType.DMA
    vmem = pl.BlockSpec(memory_space=pltpu.VMEM)
    block = (cx + 4, cy + 2 * TOP, cz)
    hbm = pl.BlockSpec(memory_space=pltpu.HBM)
    ham, momentum, total = pl.pallas_call(
        functools.partial(kernel, sizes),
        out_shape=(
            pltpu.VMEM(chi_field.shape, jnp.float32),
            pltpu.VMEM(gamma_field.shape, jnp.float32),
            pltpu.VMEM((1, 128), jnp.float32),
        ),
        in_specs=[pl.BlockSpec(memory_space=pltpu.HBM)] * 6,
        out_specs=(vmem, vmem, vmem),
        scratch_shapes=[
            pltpu.VMEM((17,) + block, jnp.float32),
            pltpu.VMEM(block, jnp.float32),
        ]
        + [pltpu.VMEM(shape + (cy, cz), jnp.float32) for shape in ((cx,), (2, cx), (2, 4), (2, 2, 4))]
        + [
            pltpu.VMEM((GEO, cx) + block[1:], jnp.float32),
            pltpu.VMEM((2, 8, 128), jnp.float32),
            pltpu.VMEM((2, 3, 2, cy, cz), jnp.float32),
            pltpu.VMEM((3, 4, cy, cz), jnp.float32),
            pltpu.VMEM((len(Z_FIELDS), 256, 256), jnp.bfloat16),
            pltpu.VMEM((len(Z_FIELDS), cx, cy, cz), jnp.float32),
        ]
        + [pltpu.VMEM((GEO, cx, cy, cz), jnp.float32)] * 4
        + [pltpu.VMEM((2, cx * cy, cz), jnp.bfloat16)] * 3
        + [pltpu.VMEM((np.prod(sizes), 128), jnp.float32), dma((4,)), dma((11,)), dma((11,))]
        + [pltpu.SemaphoreType.REGULAR],
        compiler_params=pltpu.CompilerParams(
            collective_id=0, has_side_effects=True, vmem_limit_bytes=67043328 - 16 * chi_field.size - 16384
        ),
    )(chi_field, metric, curvature, trace_curvature, gamma_field, jnp.asarray(z_weights(), jnp.bfloat16))
    count = float(chi_field.size * sizes[0] * sizes[1] * sizes[2])
    return pl.pallas_call(
        functools.partial(deliver, count),
        out_shape=(
            jax.ShapeDtypeStruct(chi_field.shape, jnp.float32),
            jax.ShapeDtypeStruct(gamma_field.shape, jnp.float32),
            jax.ShapeDtypeStruct((2,), jnp.float32),
        ),
        in_specs=[vmem, vmem, vmem],
        out_specs=(hbm, hbm, hbm),
        scratch_shapes=[pltpu.SMEM((2,), jnp.float32), pltpu.SemaphoreType.DMA((3,))],
    )(*(pltpu.with_memory_space_constraint(v, pltpu.VMEM) for v in (ham, momentum, total)))


def solution(mesh):
    return jax.shard_map(
        on_device,
        mesh=mesh,
        in_specs=(
            P("gx", "gy", "gz"),
            P(None, "gx", "gy", "gz"),
            P(None, "gx", "gy", "gz"),
            P("gx", "gy", "gz"),
            P(None, "gx", "gy", "gz"),
        ),
        out_specs=(P("gx", "gy", "gz"), P(None, "gx", "gy", "gz"), P()),
        check_vma=False,
    )
```

```python
import functools

import jax
import jax.numpy as jnp
import numpy as np
from jax import lax
from jax.experimental import pallas as pl
from jax.experimental.pallas import tpu as pltpu
from jax.sharding import PartitionSpec as P

pair_index = ((0, 1, 2), (1, 3, 4), (2, 4, 5))
MESH = pl.DeviceIdType.MESH
GX, CHI, MET, CURV, TRK, GY, GZ = 0, 1, 2, 8, 14, 15, 16
GEO = 7
X_MET, X_CHI, X_GX, Y_GEO, Y_REST, Y_PACK, Z_PACK, EDGE_Y, EDGE_Z, PART, NORM = range(11)
Z_FIELDS = tuple(range(CHI, GY)) + (GZ,)
TOP = 8


def first(m2, m1, p1, p2):
    return 8.0 * (p1 - m1) - (p2 - m2)


def second(m2, m1, c, p1, p2):
    return 16.0 * (p1 + m1) - (p2 + m2) - 30.0 * c


def total_of(terms):
    terms = list(terms)
    while len(terms) > 1:
        terms = [
            terms[n] + terms[n + 1] if n + 1 < len(terms) else terms[n]
            for n in range(0, len(terms), 2)
        ]
    return terms[0]


def sym(values, i, j):
    return values[pair_index[i][j]]


def contract(gu, values):
    return total_of(
        [gu[n] * values[n] for n in (0, 3, 5)]
        + [2.0 * total_of(gu[n] * values[n] for n in (1, 2, 4))]
    )


def z_weights():
    weights = np.zeros((len(Z_FIELDS), 256, 256), np.float32)
    for n in range(len(Z_FIELDS)):
        for z in range(128):
            for step, one, two in ((-2, 1, -1), (-1, -8, 16), (0, 0, -30), (1, 8, 16), (2, -1, -1)):
                at = z + step
                row = at if 0 <= at < 128 else 128 + 4 * n + (at + 2 if at < 0 else at - 126)
                weights[n, row, z] = one
                weights[n, row, 128 + z] = two
    return weights


def split(value):
    high = value.astype(jnp.bfloat16)
    return high, (value - high.astype(jnp.float32)).astype(jnp.bfloat16)


def along_z(value, packed, weights):
    parts = [jnp.concatenate([a, b], 1) for a, b in zip(split(value), packed)]
    return sum(jnp.dot(part, weights, preferred_element_type=jnp.float32) for part in parts)


def inverse(metric):
    g00, g01, g02, g11, g12, g22 = metric
    m00 = g11 * g22 - g12 * g12
    m01 = g02 * g12 - g01 * g22
    m02 = g01 * g12 - g02 * g11
    m11 = g00 * g22 - g02 * g02
    m12 = g01 * g02 - g00 * g12
    m22 = g00 * g11 - g01 * g01
    scale = 1.0 / (g00 * m00 + g01 * m01 + g02 * m02)
    return [m * scale for m in (m00, m01, m02, m11, m12, m22)]


def cell_math(load, load_dx, load_dy, load_z, load_zz, load_xz, load_yz, whole):
    zpos = {f: n for n, f in enumerate(Z_FIELDS)}
    gu = inverse([load(MET + n, 0, 0) for n in range(6)])
    gu_hess = [12.0 * gu[n] if n in (0, 3, 5) else 2.0 * gu[n] for n in range(6)]

    def geo(f):
        c = load(f, 0, 0)
        xs = [load(f, s, 0) for s in (-2, -1, 1, 2)]
        ys = [load(f, 0, s) for s in (-2, -1, 1, 2)]
        n = zpos[f]
        dx = load_dx(n, 0)
        dy, dz = load_dy(n), load_z(n)
        dxx = second(xs[0], xs[1], c, xs[2], xs[3])
        dyy = second(ys[0], ys[1], c, ys[2], ys[3])
        hess = {0: dxx, 3: dyy, 4: load_yz(n), 5: load_zz(n)}
        if whole:
            hess[1] = first(*(load_dx(n, s) for s in (-2, -1, 1, 2)))
            hess[2] = load_xz(n)
        return (dx, dy, dz), total_of(gu_hess[k] * hess[k] for k in sorted(hess))

    chi = load(CHI, 0, 0)
    dchi, chi_box = geo(CHI)
    grads = [[None] * 6 for _ in range(3)]
    boxes = []
    for n in range(6):
        d, box = geo(MET + n)
        for a in range(3):
            grads[a][n] = d[a]
        boxes.append(box)
    metric_box = contract(gu, boxes)

    raised = [
        [[total_of(sym(gu, b, l) * sym(grads[k], l, j) for l in range(3)) for j in range(3)] for b in range(3)]
        for k in range(3)
    ]
    trace = [raised[k][0][0] + raised[k][1][1] + raised[k][2][2] for k in range(3)]
    lower = [
        raised[0][0][l] + raised[1][1][l] + raised[2][2][l] - 0.5 * trace[l] for l in range(3)
    ]
    gd = [total_of(sym(gu, k, l) * lower[l] for l in range(3)) for k in range(3)]

    def trace_of(k, l):
        return total_of(raised[k][a][b] * raised[l][b][a] for a in range(3) for b in range(3))

    square = contract(gu, [trace_of(k, l) for k in range(3) for l in range(k, 3)])

    def cross_of(k, b):
        left, right = raised[k][b], raised[b][k]
        up = [total_of(sym(gu, c, j) * right[j] for j in range(3)) for c in range(3)]
        return total_of(left[c] * up[c] for c in range(3))

    cross = (
        cross_of(0, 0)
        + cross_of(1, 1)
        + cross_of(2, 2)
        + 2.0 * (cross_of(0, 1) + cross_of(0, 2) + cross_of(1, 2))
    )
    chi_up = [total_of(sym(gu, k, l) * dchi[l] for l in range(3)) for k in range(3)]
    grad_sq = total_of(chi_up[k] * dchi[k] for k in range(3))
    laplace = chi_box - total_of(gd[k] * dchi[k] for k in range(3))
    drift = total_of(gd[k] * trace[k] for k in range(3))

    def dx_of(f):
        return first(*(load(f, s, 0) for s in (-2, -1, 1, 2)))

    def dy_of(f):
        return first(*(load(f, 0, s) for s in (-2, -1, 1, 2)))

    def dz_of(f):
        return load_z(zpos[f])

    div = dy_of(GY) + dz_of(GZ)
    if whole:
        div = dx_of(GX) + div
    inv_chi = 1.0 / chi
    curv = [load(CURV + n, 0, 0) for n in range(6)]
    mixed = [
        [total_of(sym(curv, i, k) * sym(gu, k, j) for k in range(3)) for j in range(3)] for i in range(3)
    ]
    curv_up = [
        total_of(sym(gu, i, a) * mixed[a][j] for a in range(3)) for i in range(3) for j in range(i, 3)
    ]
    curv_sq = contract(curv, curv_up)
    trk = load(TRK, 0, 0)
    ham = (
        chi * ((0.25 * square + 0.5 * (cross + drift - metric_box)) * (1.0 / 144.0) + div * (1.0 / 12.0))
        + (2.0 * laplace - 2.5 * grad_sq * inv_chi) * (1.0 / 144.0)
        + (2.0 / 3.0) * trk * trk
        - curv_sq
    )
    push = [gd[l] + 1.5 * inv_chi * chi_up[l] for l in range(3)]
    curv_grads = [[op(CURV + n) for n in range(6)] for op in (dx_of, dy_of, dz_of)]
    trace_grads = [op(TRK) for op in (dx_of, dy_of, dz_of)]
    momentum = []
    for i in range(3):
        parts = total_of(sym(gu, j, k) * sym(curv_grads[j], k, i) for j in range(3) for k in range(3))
        parts = parts - total_of(sym(curv, l, i) * push[l] for l in range(3))
        parts = parts - 0.5 * contract(curv_up, grads[i]) - (2.0 / 3.0) * trace_grads[i]
        momentum.append(parts * (1.0 / 12.0))
    return ham, momentum


def kernel(
    sizes,
    chi_in, met_in, curv_in, trk_in, gam_in, weights_in,
    ham_out, mom_out, total_out,
    cells, packed, pack_own, pack_in, edge_own, edge_in, slope, sums,
    part_out, part, weights, z_one, z_two, y_one, yz_two, xz_two, mid_split, dy_split, dx_split,
    slots, load_sem, sent, got, ready,
):
    nx, ny, nz = sizes
    cx, cy = chi_in.shape[0], chi_in.shape[1]
    names = ("gx", "gy", "gz")
    me = [lax.axis_index(a) for a in names]

    def moved(axis, step):
        return lax.rem(me[axis] + step + sizes[axis], sizes[axis])

    def peer(axes, steps):
        where = list(me)
        if isinstance(axes, int):
            axes, steps = (axes,), (steps,)
        for axis, step in zip(axes, steps):
            where[axis] = moved(axis, step)
        return tuple(where)

    def hops(axes):
        return [step for step in np.ndindex(*(sizes[a] for a in axes)) if any(step)]

    def place_in(axes, steps=None):
        index = 0
        for axis, step in zip(axes, steps or (0,) * len(axes)):
            index = index * sizes[axis] + moved(axis, step)
        return index

    own_x, own_y = pl.ds(2, cx), pl.ds(TOP, cy)
    loads = [
        pltpu.make_async_copy(src, dst, load_sem.at[n])
        for n, src, dst in (
            (0, met_in, cells.at[pl.ds(MET, 6), own_x, own_y]),
            (1, chi_in, cells.at[CHI, own_x, own_y]),
            (1, gam_in.at[0], cells.at[GX, own_x, own_y]),
            (2, curv_in, cells.at[pl.ds(CURV, 6), own_x, own_y]),
            (2, trk_in, cells.at[TRK, own_x, own_y]),
            (2, gam_in.at[pl.ds(1, 2)], cells.at[pl.ds(GY, 2), own_x, own_y]),
            (3, weights_in, weights),
        )
    ]
    for copy in loads[:6]:
        copy.start()
    barrier = pltpu.get_barrier_semaphore()
    for axes in ((1, 2), (0,)):
        for step in hops(axes):
            pl.semaphore_signal(barrier, inc=1, device_id=peer(axes, step), device_id_type=MESH)
    pl.semaphore_wait(barrier, ny * nz + nx - 2)

    for step in hops((1, 2)):
        pl.semaphore_signal(ready, inc=1, device_id=peer((1, 2), step), device_id_type=MESH)

    def loaded(n, ref):
        pltpu.make_async_copy(ref, ref, load_sem.at[n]).wait()

    def copy_to(src, dst, n, axes, step):
        return pltpu.make_async_remote_copy(
            src_ref=src, dst_ref=dst, send_sem=sent.at[n], recv_sem=got.at[n],
            device_id=peer(axes, step), device_id_type=MESH,
        )

    def send(src, dst, n, axes, step):
        copy_to(src, dst, n, axes, step).start()

    low_x, high_x = pl.ds(2, 2), pl.ds(cx, 2)
    before_x, after_x = pl.ds(0, 2), pl.ds(cx + 2, 2)
    low_y, high_y = pl.ds(TOP, 2), pl.ds(TOP + cy - 2, 2)
    before_y, after_y = pl.ds(TOP - 2, 2), pl.ds(TOP + cy, 2)
    geo = pl.ds(CHI, GEO)
    several = nz > 2
    bulk = {
        X_MET: cells.at[pl.ds(MET, 6), pl.ds(0, 4), own_y],
        X_CHI: cells.at[pl.ds(CHI, 1), pl.ds(0, 4), own_y],
        X_GX: cells.at[pl.ds(GX, 1), pl.ds(0, 4), own_y],
        Y_GEO: cells.at[geo, own_x, pl.ds(0, 4)],
        Y_REST: cells.at[pl.ds(CURV, 8), own_x, pl.ds(0, 4)],
        Y_PACK: packed.at[own_x, pl.ds(0, 4)],
        Z_PACK: pack_in if several else pack_in.at[0],
        EDGE_Y: cells.at[geo, pl.ds(0, 4), pl.ds(0, 4)],
        EDGE_Z: edge_in if several else edge_in.at[0],
        PART: part,
        NORM: slots.at[pl.ds(0, nx * ny * nz - 1)],
    }

    def wait_for(n):
        copy_to(bulk[n], bulk[n], n, 0, 1).wait_recv()

    def each_way(axis, ahead, back):
        odd = lax.rem(me[axis], 2) == 1

        @pl.when(odd)
        def _():
            ahead()
            back()

        @pl.when(jnp.logical_not(odd))
        def _():
            back()
            ahead()

    def send_x(fields, n):
        each_way(
            0,
            lambda: send(cells.at[fields, high_x, own_y], cells.at[fields, before_x, own_y], n, 0, 1),
            lambda: send(cells.at[fields, low_x, own_y], cells.at[fields, after_x, own_y], n, 0, -1),
        )

    def send_y(fields, n, layers=own_x):
        each_way(
            1,
            lambda: send(cells.at[fields, layers, high_y], cells.at[fields, layers, before_y], n, 1, 1),
            lambda: send(cells.at[fields, layers, low_y], cells.at[fields, layers, after_y], n, 1, -1),
        )

    loaded(0, cells.at[pl.ds(MET, 6), own_x, own_y])
    send_x(pl.ds(MET, 6), X_MET)
    loaded(1, cells.at[pl.ds(GX, 2), own_x, own_y])
    send_x(pl.ds(CHI, 1), X_CHI)
    send_y(geo, Y_GEO)
    send_x(pl.ds(GX, 1), X_GX)
    loaded(2, cells.at[pl.ds(CURV, 9), own_x, own_y])
    send_y(pl.ds(CURV, 8), Y_REST)
    loads[6].start()

    tiles = cy // 8
    group = lax.shift_right_logical(lax.broadcasted_iota(jnp.int32, (8, 128), 1), 2)
    far_side = (lax.broadcasted_iota(jnp.int32, (cy, 128), 1) & 2) != 0

    def packing(fields, target, layer, unroll):
        def pack(step, carry):
            at, y = step // tiles, lax.rem(step, tiles) * 8
            rows = pl.ds(pl.multiple_of(TOP + y, 8), 8)
            x = layer(at)
            picked = [
                jnp.where(group == n, pltpu.roll(cells[f, x, rows], 4 * n + 2, 1), 0.0)
                for n, f in enumerate(fields)
                if f is not None
            ]
            target[at, pl.ds(pl.multiple_of(y, 8), 8)] = total_of(picked)
            return carry

        lax.fori_loop(0, target.shape[0] * tiles, pack, 0, unroll=unroll)

    packing(Z_FIELDS, pack_own, lambda at: at + 2, 4)

    def send_z(own, target, n):
        send(own, target(0), n, 2, 1)
        if several:
            send(own, target(1), n, 2, -1)

    def joined(both):
        return jnp.where(far_side, both(1), both(0)) if several else both(0)

    send_z(pack_own, lambda side: pack_in.at[side], Z_PACK)
    sums[...] = jnp.zeros_like(sums)
    missing = jnp.zeros((7, 2, cy, 128), jnp.float32)
    cells[pl.ds(CURV, 7), before_x, own_y] = missing
    cells[pl.ds(CURV, 7), after_x, own_y] = missing
    wait_for(Z_PACK)

    def keep_split(target, value, at=0):
        for n, half in enumerate(split(value)):
            target[n, pl.ds(at, value.shape[0])] = half

    def merge(x, carry):
        value = joined(lambda side: pack_in[side, x])
        packed[x + 2, own_y] = value
        keep_split(mid_split, value, pl.multiple_of(x * cy, cy))
        return carry

    lax.fori_loop(0, cx, merge, 0)
    send(packed.at[own_x, high_y], packed.at[own_x, before_y], Y_PACK, 1, 1)
    send(packed.at[own_x, low_y], packed.at[own_x, after_y], Y_PACK, 1, -1)
    loads[6].wait()
    flat = (cx * cy, 128)

    def geo_z(n, carry):
        both = along_z(cells[n + CHI, own_x, own_y].reshape(flat), mid_split[...], weights[n])
        z_one[n] = both[:, :128].reshape(cx, cy, 128)
        z_two[n] = both[:, 128:].reshape(cx, cy, 128)
        return carry

    lax.fori_loop(0, GEO, geo_z, 0, unroll=7)

    def rest_z(n, carry):
        f = n + CHI + n // (GY - CHI)
        z_one[n] = along_z(
            cells[f, own_x, own_y].reshape(flat), mid_split[...], weights[n, :, :128]
        ).reshape(cx, cy, 128)
        return carry

    lax.fori_loop(GEO, len(Z_FIELDS), rest_z, 0, unroll=8)

    def rises(pieces):
        rows = [cx * count for _, count in pieces]
        at = 0
        for (row, count), size in zip(pieces, rows):
            values = first(*(packed[own_x, pl.ds(TOP + row + s, count)] for s in (-2, -1, 1, 2)))
            keep_split(dy_split, values.reshape(size, 128), at)
            at += size
        total = at

        def one(n, carry):
            values = []
            for (row, count), size in zip(pieces, rows):
                dy = first(*(cells[n + CHI, own_x, pl.ds(TOP + row + s, count)] for s in (-2, -1, 1, 2)))
                y_one[n, :, pl.ds(row, count)] = dy
                values.append(dy.reshape(size, 128))
            both = along_z(jnp.concatenate(values, 0), dy_split[:, :total], weights[n, :, :128])
            at = 0
            for (row, count), size in zip(pieces, rows):
                yz_two[n, :, pl.ds(row, count)] = both[at : at + size].reshape(cx, count, 128)
                at += size
            return carry

        lax.fori_loop(0, GEO, one, 0, unroll=7)

    def climbs(pieces, fields):
        def one(n, carry):
            for base, count in pieces:
                slope[n, pl.ds(base, count), own_y] = first(
                    *(cells[n + CHI, pl.ds(base + 2 + s, count), own_y] for s in (-2, -1, 1, 2))
                )
            return carry

        lax.fori_loop(*fields, one, 0, unroll=fields[1] - fields[0])

    def slopes(pieces):
        rows = [count * cy for _, count in pieces]
        at = 0
        for (base, count), size in zip(pieces, rows):
            values = first(*(packed[pl.ds(base + 2 + s, count), own_y] for s in (-2, -1, 1, 2)))
            keep_split(dx_split, values.reshape(size, 128), at)
            at += size
        total = at

        def one(n, carry):
            values = [slope[n, pl.ds(base, count), own_y].reshape(size, 128) for (base, count), size in zip(pieces, rows)]
            both = along_z(jnp.concatenate(values, 0), dx_split[:, :total], weights[n, :, :128])
            at = 0
            for (base, count), size in zip(pieces, rows):
                xz_two[n, pl.ds(base, count)] = both[at : at + size].reshape(count, cy, 128)
                at += size
            return carry

        lax.fori_loop(0, GEO, one, 0, unroll=7)

    def tile_at(x, y, whole):
        rows = pl.ds(pl.multiple_of(y, 8), 8)
        ham, momentum = cell_math(
            lambda f, sx, sy: cells[f, x + 2 + sx, pl.ds(TOP + y + sy, 8)],
            lambda n, sy: slope[n, x, pl.ds(TOP + y + sy, 8)],
            lambda n: y_one[n, x, rows],
            lambda n: z_one[n, x, rows],
            lambda n: z_two[n, x, rows],
            lambda n: xz_two[n, x, rows],
            lambda n: yz_two[n, x, rows],
            whole,
        )
        ham_out[x, rows] = ham
        for i in range(3):
            mom_out[i, x, rows] = momentum[i]
        if whole:
            sums[0] += ham * ham
            sums[1] += momentum[0] * momentum[0] + momentum[1] * momentum[1] + momentum[2] * momentum[2]

    def rims(pieces):
        def one(n, carry):
            for base, count in pieces:
                for rows in (pl.ds(TOP - 8, 8), pl.ds(TOP + cy, 8)):
                    slope[n, pl.ds(base, count), rows] = first(
                        *(cells[n + CHI, pl.ds(base + 2 + s, count), rows] for s in (-2, -1, 1, 2))
                    )
            return carry

        lax.fori_loop(0, GEO, one, 0, unroll=7)

    def outer_x(at):
        return at + at // 2 * (cx - 4)

    def run(layers, layer, count, row, whole):
        def one(n, carry):
            tile_at(layer(n // count), row(lax.rem(n, count)), whole)
            return carry

        lax.fori_loop(0, layers * count, one, 0)

    inner = (cx - 4, lambda at: at + 2)
    outer = (4, outer_x)
    every = (tiles, lambda at: 8 * at)
    middle = (tiles - 2, lambda at: 8 * at + 8)
    rim = (2, lambda at: at * (cy - 8))
    rises(((8, cy - 16),))
    climbs(((2, cx - 4),), (0, GEO))
    slopes(((2, cx - 4),))
    run(*inner, *middle, True)
    wait_for(Y_GEO)
    wait_for(Y_PACK)
    rises(((0, 8), (cy - 8, 8)))
    rims(((2, cx - 4),))
    wait_for(Y_REST)
    run(*inner, *rim, True)
    wait_for(X_MET)

    def offer(t, carry):
        rows = pl.ds(pl.multiple_of(TOP + t * 8, 8), 8)
        out_rows = pl.ds(pl.multiple_of(t * 8, 8), 8)
        for side, far, near, at, behind, sign in ((0, 0, 1, 2, 3, 1.0), (1, cx + 3, cx + 2, cx + 1, cx, -1.0)):
            edge = [cells[CURV + n, at, rows] * sign for n in range(7)]
            second_edge = [cells[CURV + n, behind, rows] * sign for n in range(7)]
            for place, slot, values in (
                (near, 1 - side, [8.0 * a - b for a, b in zip(edge, second_edge)]),
                (far, side, [-a for a in edge]),
            ):
                gu = inverse([cells[MET + n, place, rows] for n in range(6)])
                for i in range(3):
                    value = total_of(sym(gu, 0, k) * sym(values, k, i) for k in range(3))
                    if i == 0:
                        value = value - (2.0 / 3.0) * values[6]
                    part_out[side, i, slot, out_rows] = value * (1.0 / 12.0)
        return carry

    lax.fori_loop(0, tiles, offer, 0)
    each_way(
        0,
        lambda: send(part_out.at[1], part.at[:, pl.ds(0, 2)], PART, 0, 1),
        lambda: send(part_out.at[0], part.at[:, pl.ds(2, 2)], PART, 0, -1),
    )

    def relay(n, fields, sliced, unroll):
        for layers in (before_x, after_x):
            send_y(sliced, EDGE_Y, layers)
        packing(fields, edge_own.at[n], lambda at: at + at // 2 * cx, unroll)
        send_z(edge_own.at[n], lambda side: edge_in.at[side, n], EDGE_Z)

    ends = ((0, 2), (cx - 2, 2))
    relay(0, (None,) + tuple(range(MET, CURV)), pl.ds(MET, 6), 4)
    climbs(ends, (1, GEO))
    wait_for(X_CHI)
    relay(1, (CHI,), pl.ds(CHI, 1), 4)
    climbs(ends, (0, 1))
    run(*outer, *every, False)
    wait_for(EDGE_Z)
    for at in range(4):
        packed[at + at // 2 * cx, own_y] = joined(lambda side: edge_in[side, 0, at] + edge_in[side, 1, at])
    slopes(ends)
    wait_for(EDGE_Y)
    rims(ends)
    wait_for(X_GX)

    def mend(n, carry):
        x, y = outer_x(n // tiles), lax.rem(n, tiles) * 8
        rows = pl.ds(pl.multiple_of(y, 8), 8)
        here = pl.ds(pl.multiple_of(TOP + y, 8), 8)
        chi, *metric = [cells[CHI + k, x + 2, here] for k in range(GEO)]
        gu = inverse(metric)
        chi_part, *parts = [
            gu[1] * first(*(slope[k, x, pl.ds(TOP + y + s, 8)] for s in (-2, -1, 1, 2))) + gu[2] * xz_two[k, x, rows]
            for k in range(GEO)
        ]
        div = first(*(cells[GX, x + 2 + s, here] for s in (-2, -1, 1, 2)))
        ham = ham_out[x, rows] + (
            (4.0 * chi_part - chi * contract(gu, parts)) * (1.0 / 144.0) + chi * div * (1.0 / 12.0)
        )
        ham_out[x, rows] = ham
        sums[0] += ham * ham
        return carry

    lax.fori_loop(0, 4 * tiles, mend, 0, unroll=2)
    wait_for(PART)

    squares = []
    for at in range(4):
        x = outer_x(at)
        for i in range(3):
            momentum = mom_out[i, x] + part[i, at]
            mom_out[i, x] = momentum
            squares += [momentum[y : y + 8] * momentum[y : y + 8] for y in range(0, cy, 8)]
    sums[1] += total_of(squares)

    lane = lax.broadcasted_iota(jnp.int32, (8, 128), 1)
    folded = [sums[n] + pltpu.roll(sums[n], 64, 1) for n in range(2)]
    total = jnp.sum(jnp.where(lane < 64, folded[0], folded[1]), axis=0, keepdims=True)
    pl.semaphore_wait(ready, ny * nz - 1)
    axes = (0, 1, 2)
    here = pl.ds(place_in(axes), 1)
    slots[here] = total
    for step in sorted(hops(axes), key=lambda step: -sum(min(a, b - a) for a, b in zip(step, sizes))):
        send(slots.at[here], slots.at[here], NORM, axes, step)
    wait_for(NORM)
    total_out[...] = jnp.sum(slots[...], axis=0, keepdims=True)
    for n, ref in bulk.items():
        copy_to(ref, ref, n, 0, 1).wait_send()


def deliver(count, ham_in, mom_in, total_in, ham_out, mom_out, norm_out, norm, sems):
    copies = [
        pltpu.make_async_copy(mom_in, mom_out, sems.at[0]),
        pltpu.make_async_copy(ham_in, ham_out, sems.at[1]),
    ]
    for copy in copies:
        copy.start()
    total = total_in[...]
    lane = lax.broadcasted_iota(jnp.int32, total.shape, 1)
    for n, (part, cells) in enumerate(((lane < 64, count), (lane >= 64, 3.0 * count))):
        root = jnp.sqrt(jnp.sum(jnp.where(part, total, 0.0), axis=1, keepdims=True) * (1.0 / cells))
        norm[n] = root[0, 0]
    copies.append(pltpu.make_async_copy(norm, norm_out, sems.at[2]))
    copies[2].start()
    for copy in copies:
        copy.wait()


def on_device(chi_field, metric, curvature, trace_curvature, gamma_field):
    sizes = tuple(lax.axis_size(a) for a in ("gx", "gy", "gz"))
    cx, cy, cz = chi_field.shape
    dma = pltpu.SemaphoreType.DMA
    vmem = pl.BlockSpec(memory_space=pltpu.VMEM)
    block = (cx + 4, cy + 2 * TOP, cz)
    hbm = pl.BlockSpec(memory_space=pltpu.HBM)
    ham, momentum, total = pl.pallas_call(
        functools.partial(kernel, sizes),
        out_shape=(
            pltpu.VMEM(chi_field.shape, jnp.float32),
            pltpu.VMEM(gamma_field.shape, jnp.float32),
            pltpu.VMEM((1, 128), jnp.float32),
        ),
        in_specs=[pl.BlockSpec(memory_space=pltpu.HBM)] * 6,
        out_specs=(vmem, vmem, vmem),
        scratch_shapes=[
            pltpu.VMEM((17,) + block, jnp.float32),
            pltpu.VMEM(block, jnp.float32),
        ]
        + [pltpu.VMEM(shape + (cy, cz), jnp.float32) for shape in ((cx,), (2, cx), (2, 4), (2, 2, 4))]
        + [
            pltpu.VMEM((GEO, cx) + block[1:], jnp.float32),
            pltpu.VMEM((2, 8, 128), jnp.float32),
            pltpu.VMEM((2, 3, 2, cy, cz), jnp.float32),
            pltpu.VMEM((3, 4, cy, cz), jnp.float32),
            pltpu.VMEM((len(Z_FIELDS), 256, 256), jnp.bfloat16),
            pltpu.VMEM((len(Z_FIELDS), cx, cy, cz), jnp.float32),
        ]
        + [pltpu.VMEM((GEO, cx, cy, cz), jnp.float32)] * 4
        + [pltpu.VMEM((2, cx * cy, cz), jnp.bfloat16)] * 3
        + [pltpu.VMEM((np.prod(sizes), 128), jnp.float32), dma((4,)), dma((11,)), dma((11,))]
        + [pltpu.SemaphoreType.REGULAR],
        compiler_params=pltpu.CompilerParams(
            collective_id=0, has_side_effects=True, vmem_limit_bytes=67043328 - 16 * chi_field.size - 16384
        ),
    )(chi_field, metric, curvature, trace_curvature, gamma_field, jnp.asarray(z_weights(), jnp.bfloat16))
    count = float(chi_field.size * sizes[0] * sizes[1] * sizes[2])
    return pl.pallas_call(
        functools.partial(deliver, count),
        out_shape=(
            jax.ShapeDtypeStruct(chi_field.shape, jnp.float32),
            jax.ShapeDtypeStruct(gamma_field.shape, jnp.float32),
            jax.ShapeDtypeStruct((2,), jnp.float32),
        ),
        in_specs=[vmem, vmem, vmem],
        out_specs=(hbm, hbm, hbm),
        scratch_shapes=[pltpu.SMEM((2,), jnp.float32), pltpu.SemaphoreType.DMA((3,))],
    )(*(pltpu.with_memory_space_constraint(v, pltpu.VMEM) for v in (ham, momentum, total)))


def solution(mesh):
    return jax.shard_map(
        on_device,
        mesh=mesh,
        in_specs=(
            P("gx", "gy", "gz"),
            P(None, "gx", "gy", "gz"),
            P(None, "gx", "gy", "gz"),
            P("gx", "gy", "gz"),
            P(None, "gx", "gy", "gz"),
        ),
        out_specs=(P("gx", "gy", "gz"), P(None, "gx", "gy", "gz"), P()),
        check_vma=False,
    )
```

```python
import functools

import jax
import jax.numpy as jnp
import numpy as np
from jax import lax
from jax.experimental import pallas as pl
from jax.experimental.pallas import tpu as pltpu
from jax.sharding import PartitionSpec as P

pair_index = ((0, 1, 2), (1, 3, 4), (2, 4, 5))
MESH = pl.DeviceIdType.MESH
GX, CHI, MET, CURV, TRK, GY, GZ = 0, 1, 2, 8, 14, 15, 16
GEO = 7
X_MET, X_MET_BACK, X_CHI, X_GX, Y_GEO, Y_REST, Y_PACK, Z_PACK, EDGE_Y, EDGE_Z, PART, NORM = range(12)
Z_FIELDS = tuple(range(CHI, GY)) + (GZ,)
TOP = 8


def first(m2, m1, p1, p2):
    return 8.0 * (p1 - m1) - (p2 - m2)


def second(m2, m1, c, p1, p2):
    return 16.0 * (p1 + m1) - (p2 + m2) - 30.0 * c


def total_of(terms):
    terms = list(terms)
    while len(terms) > 1:
        terms = [
            terms[n] + terms[n + 1] if n + 1 < len(terms) else terms[n]
            for n in range(0, len(terms), 2)
        ]
    return terms[0]


def sym(values, i, j):
    return values[pair_index[i][j]]


def contract(gu, values):
    return total_of(
        [gu[n] * values[n] for n in (0, 3, 5)]
        + [2.0 * total_of(gu[n] * values[n] for n in (1, 2, 4))]
    )


def z_weights():
    weights = np.zeros((len(Z_FIELDS), 256, 256), np.float32)
    for n in range(len(Z_FIELDS)):
        for z in range(128):
            for step, one, two in ((-2, 1, -1), (-1, -8, 16), (0, 0, -30), (1, 8, 16), (2, -1, -1)):
                at = z + step
                row = at if 0 <= at < 128 else 128 + 4 * n + (at + 2 if at < 0 else at - 126)
                weights[n, row, z] = one
                weights[n, row, 128 + z] = two
    return weights


def split(value):
    high = value.astype(jnp.bfloat16)
    return high, (value - high.astype(jnp.float32)).astype(jnp.bfloat16)


def along_z(value, packed, weights):
    parts = [jnp.concatenate([a, b], 1) for a, b in zip(split(value), packed)]
    return sum(jnp.dot(part, weights, preferred_element_type=jnp.float32) for part in parts)


def inverse(metric):
    g00, g01, g02, g11, g12, g22 = metric
    m00 = g11 * g22 - g12 * g12
    m01 = g02 * g12 - g01 * g22
    m02 = g01 * g12 - g02 * g11
    m11 = g00 * g22 - g02 * g02
    m12 = g01 * g02 - g00 * g12
    m22 = g00 * g11 - g01 * g01
    scale = 1.0 / (g00 * m00 + g01 * m01 + g02 * m02)
    return [m * scale for m in (m00, m01, m02, m11, m12, m22)]


def cell_math(load, load_dx, load_dy, load_z, load_zz, load_xz, load_yz, whole):
    zpos = {f: n for n, f in enumerate(Z_FIELDS)}
    gu = inverse([load(MET + n, 0, 0) for n in range(6)])
    gu_hess = [12.0 * gu[n] if n in (0, 3, 5) else 2.0 * gu[n] for n in range(6)]

    def geo(f):
        c = load(f, 0, 0)
        xs = [load(f, s, 0) for s in (-2, -1, 1, 2)]
        ys = [load(f, 0, s) for s in (-2, -1, 1, 2)]
        n = zpos[f]
        dx = load_dx(n, 0)
        dy, dz = load_dy(n), load_z(n)
        dxx = second(xs[0], xs[1], c, xs[2], xs[3])
        dyy = second(ys[0], ys[1], c, ys[2], ys[3])
        hess = {0: dxx, 3: dyy, 4: load_yz(n), 5: load_zz(n)}
        if whole:
            hess[1] = first(*(load_dx(n, s) for s in (-2, -1, 1, 2)))
            hess[2] = load_xz(n)
        return (dx, dy, dz), total_of(gu_hess[k] * hess[k] for k in sorted(hess))

    chi = load(CHI, 0, 0)
    dchi, chi_box = geo(CHI)
    grads = [[None] * 6 for _ in range(3)]
    boxes = []
    for n in range(6):
        d, box = geo(MET + n)
        for a in range(3):
            grads[a][n] = d[a]
        boxes.append(box)
    metric_box = contract(gu, boxes)

    raised = [
        [[total_of(sym(gu, b, l) * sym(grads[k], l, j) for l in range(3)) for j in range(3)] for b in range(3)]
        for k in range(3)
    ]
    trace = [raised[k][0][0] + raised[k][1][1] + raised[k][2][2] for k in range(3)]
    lower = [
        raised[0][0][l] + raised[1][1][l] + raised[2][2][l] - 0.5 * trace[l] for l in range(3)
    ]
    gd = [total_of(sym(gu, k, l) * lower[l] for l in range(3)) for k in range(3)]

    def trace_of(k, l):
        return total_of(raised[k][a][b] * raised[l][b][a] for a in range(3) for b in range(3))

    square = contract(gu, [trace_of(k, l) for k in range(3) for l in range(k, 3)])

    def cross_of(k, b):
        left, right = raised[k][b], raised[b][k]
        up = [total_of(sym(gu, c, j) * right[j] for j in range(3)) for c in range(3)]
        return total_of(left[c] * up[c] for c in range(3))

    cross = (
        cross_of(0, 0)
        + cross_of(1, 1)
        + cross_of(2, 2)
        + 2.0 * (cross_of(0, 1) + cross_of(0, 2) + cross_of(1, 2))
    )
    chi_up = [total_of(sym(gu, k, l) * dchi[l] for l in range(3)) for k in range(3)]
    grad_sq = total_of(chi_up[k] * dchi[k] for k in range(3))
    laplace = chi_box - total_of(gd[k] * dchi[k] for k in range(3))
    drift = total_of(gd[k] * trace[k] for k in range(3))

    def dx_of(f):
        return first(*(load(f, s, 0) for s in (-2, -1, 1, 2)))

    def dy_of(f):
        return first(*(load(f, 0, s) for s in (-2, -1, 1, 2)))

    def dz_of(f):
        return load_z(zpos[f])

    div = dy_of(GY) + dz_of(GZ)
    if whole:
        div = dx_of(GX) + div
    inv_chi = 1.0 / chi
    curv = [load(CURV + n, 0, 0) for n in range(6)]
    mixed = [
        [total_of(sym(curv, i, k) * sym(gu, k, j) for k in range(3)) for j in range(3)] for i in range(3)
    ]
    curv_up = [
        total_of(sym(gu, i, a) * mixed[a][j] for a in range(3)) for i in range(3) for j in range(i, 3)
    ]
    curv_sq = contract(curv, curv_up)
    trk = load(TRK, 0, 0)
    ham = (
        chi * ((0.25 * square + 0.5 * (cross + drift - metric_box)) * (1.0 / 144.0) + div * (1.0 / 12.0))
        + (2.0 * laplace - 2.5 * grad_sq * inv_chi) * (1.0 / 144.0)
        + (2.0 / 3.0) * trk * trk
        - curv_sq
    )
    push = [gd[l] + 1.5 * inv_chi * chi_up[l] for l in range(3)]
    curv_grads = [[op(CURV + n) for n in range(6)] for op in (dx_of, dy_of, dz_of)]
    trace_grads = [op(TRK) for op in (dx_of, dy_of, dz_of)]
    momentum = []
    for i in range(3):
        parts = total_of(sym(gu, j, k) * sym(curv_grads[j], k, i) for j in range(3) for k in range(3))
        parts = parts - total_of(sym(curv, l, i) * push[l] for l in range(3))
        parts = parts - 0.5 * contract(curv_up, grads[i]) - (2.0 / 3.0) * trace_grads[i]
        momentum.append(parts * (1.0 / 12.0))
    return ham, momentum


def kernel(
    sizes,
    chi_in, met_in, curv_in, trk_in, gam_in, weights_in,
    ham_out, mom_out, total_out,
    cells, packed, pack_own, pack_in, edge_own, edge_in, slope, sums,
    part_out, part, weights, z_one, z_two, y_one, yz_two, xz_two, mid_split, dy_split, dx_split,
    slots, load_sem, sent, got, ready,
):
    nx, ny, nz = sizes
    cx, cy = chi_in.shape[0], chi_in.shape[1]
    names = ("gx", "gy", "gz")
    me = [lax.axis_index(a) for a in names]

    def moved(axis, step):
        return lax.rem(me[axis] + step + sizes[axis], sizes[axis])

    def peer(axes, steps):
        where = list(me)
        if isinstance(axes, int):
            axes, steps = (axes,), (steps,)
        for axis, step in zip(axes, steps):
            where[axis] = moved(axis, step)
        return tuple(where)

    def hops(axes):
        return [step for step in np.ndindex(*(sizes[a] for a in axes)) if any(step)]

    def place_in(axes, steps=None):
        index = 0
        for axis, step in zip(axes, steps or (0,) * len(axes)):
            index = index * sizes[axis] + moved(axis, step)
        return index

    own_x, own_y = pl.ds(2, cx), pl.ds(TOP, cy)
    loads = [
        pltpu.make_async_copy(src, dst, load_sem.at[n])
        for n, src, dst in (
            (0, met_in, cells.at[pl.ds(MET, 6), own_x, own_y]),
            (1, chi_in, cells.at[CHI, own_x, own_y]),
            (1, gam_in.at[0], cells.at[GX, own_x, own_y]),
            (2, curv_in, cells.at[pl.ds(CURV, 6), own_x, own_y]),
            (2, trk_in, cells.at[TRK, own_x, own_y]),
            (2, gam_in.at[pl.ds(1, 2)], cells.at[pl.ds(GY, 2), own_x, own_y]),
            (3, weights_in, weights),
        )
    ]
    for copy in loads[:6]:
        copy.start()
    barrier = pltpu.get_barrier_semaphore()
    for axes in ((1, 2), (0,)):
        for step in hops(axes):
            pl.semaphore_signal(barrier, inc=1, device_id=peer(axes, step), device_id_type=MESH)
    pl.semaphore_wait(barrier, ny * nz + nx - 2)

    for step in hops((1, 2)):
        pl.semaphore_signal(ready, inc=1, device_id=peer((1, 2), step), device_id_type=MESH)

    def loaded(n, ref):
        pltpu.make_async_copy(ref, ref, load_sem.at[n]).wait()

    def copy_to(src, dst, n, axes, step):
        return pltpu.make_async_remote_copy(
            src_ref=src, dst_ref=dst, send_sem=sent.at[n], recv_sem=got.at[n],
            device_id=peer(axes, step), device_id_type=MESH,
        )

    def send(src, dst, n, axes, step):
        copy_to(src, dst, n, axes, step).start()

    low_x, high_x = pl.ds(2, 2), pl.ds(cx, 2)
    before_x, after_x = pl.ds(0, 2), pl.ds(cx + 2, 2)
    low_y, high_y = pl.ds(TOP, 2), pl.ds(TOP + cy - 2, 2)
    before_y, after_y = pl.ds(TOP - 2, 2), pl.ds(TOP + cy, 2)
    geo = pl.ds(CHI, GEO)
    several = nz > 2
    bulk = {
        X_MET: cells.at[pl.ds(MET, 6), before_x, own_y],
        X_MET_BACK: cells.at[pl.ds(MET, 6), after_x, own_y],
        X_CHI: cells.at[pl.ds(CHI, 1), pl.ds(0, 4), own_y],
        X_GX: cells.at[pl.ds(GX, 1), pl.ds(0, 4), own_y],
        Y_GEO: cells.at[geo, own_x, pl.ds(0, 4)],
        Y_REST: cells.at[pl.ds(CURV, 8), own_x, pl.ds(0, 4)],
        Y_PACK: packed.at[own_x, pl.ds(0, 4)],
        Z_PACK: pack_in if several else pack_in.at[0],
        EDGE_Y: cells.at[geo, pl.ds(0, 4), pl.ds(0, 4)],
        EDGE_Z: edge_in if several else edge_in.at[0],
        PART: part,
        NORM: slots.at[pl.ds(0, nx * ny * nz - 1)],
    }

    def wait_for(n):
        copy_to(bulk[n], bulk[n], n, 0, 1).wait_recv()

    def each_way(axis, ahead, back):
        odd = lax.rem(me[axis], 2) == 1

        @pl.when(odd)
        def _():
            ahead()
            back()

        @pl.when(jnp.logical_not(odd))
        def _():
            back()
            ahead()

    def send_x(fields, n, n_back=None):
        each_way(
            0,
            lambda: send(cells.at[fields, high_x, own_y], cells.at[fields, before_x, own_y], n, 0, 1),
            lambda: send(cells.at[fields, low_x, own_y], cells.at[fields, after_x, own_y], n if n_back is None else n_back, 0, -1),
        )

    def send_y(fields, n, layers=own_x):
        each_way(
            1,
            lambda: send(cells.at[fields, layers, high_y], cells.at[fields, layers, before_y], n, 1, 1),
            lambda: send(cells.at[fields, layers, low_y], cells.at[fields, layers, after_y], n, 1, -1),
        )

    loaded(0, cells.at[pl.ds(MET, 6), own_x, own_y])
    send_x(pl.ds(MET, 6), X_MET, X_MET_BACK)
    loaded(1, cells.at[pl.ds(GX, 2), own_x, own_y])
    send_x(pl.ds(CHI, 1), X_CHI)
    send_y(geo, Y_GEO)
    send_x(pl.ds(GX, 1), X_GX)
    loaded(2, cells.at[pl.ds(CURV, 9), own_x, own_y])
    send_y(pl.ds(CURV, 8), Y_REST)
    loads[6].start()

    tiles = cy // 8
    group = lax.shift_right_logical(lax.broadcasted_iota(jnp.int32, (8, 128), 1), 2)
    far_side = (lax.broadcasted_iota(jnp.int32, (cy, 128), 1) & 2) != 0

    def packing(fields, target, layer, unroll):
        def pack(step, carry):
            at, y = step // tiles, lax.rem(step, tiles) * 8
            rows = pl.ds(pl.multiple_of(TOP + y, 8), 8)
            x = layer(at)
            picked = [
                jnp.where(group == n, pltpu.roll(cells[f, x, rows], 4 * n + 2, 1), 0.0)
                for n, f in enumerate(fields)
                if f is not None
            ]
            target[at, pl.ds(pl.multiple_of(y, 8), 8)] = total_of(picked)
            return carry

        lax.fori_loop(0, target.shape[0] * tiles, pack, 0, unroll=unroll)

    packing(Z_FIELDS, pack_own, lambda at: at + 2, 4)

    def send_z(own, target, n):
        send(own, target(0), n, 2, 1)
        if several:
            send(own, target(1), n, 2, -1)

    def joined(both):
        return jnp.where(far_side, both(1), both(0)) if several else both(0)

    send_z(pack_own, lambda side: pack_in.at[side], Z_PACK)
    sums[...] = jnp.zeros_like(sums)
    missing = jnp.zeros((7, 2, cy, 128), jnp.float32)
    cells[pl.ds(CURV, 7), before_x, own_y] = missing
    cells[pl.ds(CURV, 7), after_x, own_y] = missing
    wait_for(Z_PACK)

    def keep_split(target, value, at=0):
        for n, half in enumerate(split(value)):
            target[n, pl.ds(at, value.shape[0])] = half

    def merge(x, carry):
        value = joined(lambda side: pack_in[side, x])
        packed[x + 2, own_y] = value
        keep_split(mid_split, value, pl.multiple_of(x * cy, cy))
        return carry

    lax.fori_loop(0, cx, merge, 0)
    send(packed.at[own_x, high_y], packed.at[own_x, before_y], Y_PACK, 1, 1)
    send(packed.at[own_x, low_y], packed.at[own_x, after_y], Y_PACK, 1, -1)
    loads[6].wait()
    flat = (cx * cy, 128)

    def geo_z(n, carry):
        both = along_z(cells[n + CHI, own_x, own_y].reshape(flat), mid_split[...], weights[n])
        z_one[n] = both[:, :128].reshape(cx, cy, 128)
        z_two[n] = both[:, 128:].reshape(cx, cy, 128)
        return carry

    lax.fori_loop(0, GEO, geo_z, 0, unroll=7)

    def rest_z(n, carry):
        f = n + CHI + n // (GY - CHI)
        z_one[n] = along_z(
            cells[f, own_x, own_y].reshape(flat), mid_split[...], weights[n, :, :128]
        ).reshape(cx, cy, 128)
        return carry

    lax.fori_loop(GEO, len(Z_FIELDS), rest_z, 0, unroll=8)

    def rises(pieces):
        rows = [cx * count for _, count in pieces]
        at = 0
        for (row, count), size in zip(pieces, rows):
            values = first(*(packed[own_x, pl.ds(TOP + row + s, count)] for s in (-2, -1, 1, 2)))
            keep_split(dy_split, values.reshape(size, 128), at)
            at += size
        total = at

        def one(n, carry):
            values = []
            for (row, count), size in zip(pieces, rows):
                dy = first(*(cells[n + CHI, own_x, pl.ds(TOP + row + s, count)] for s in (-2, -1, 1, 2)))
                y_one[n, :, pl.ds(row, count)] = dy
                values.append(dy.reshape(size, 128))
            both = along_z(jnp.concatenate(values, 0), dy_split[:, :total], weights[n, :, :128])
            at = 0
            for (row, count), size in zip(pieces, rows):
                yz_two[n, :, pl.ds(row, count)] = both[at : at + size].reshape(cx, count, 128)
                at += size
            return carry

        lax.fori_loop(0, GEO, one, 0, unroll=7)

    def climbs(pieces, fields):
        def one(n, carry):
            for base, count in pieces:
                slope[n, pl.ds(base, count), own_y] = first(
                    *(cells[n + CHI, pl.ds(base + 2 + s, count), own_y] for s in (-2, -1, 1, 2))
                )
            return carry

        lax.fori_loop(*fields, one, 0, unroll=fields[1] - fields[0])

    def slopes(pieces):
        rows = [count * cy for _, count in pieces]
        at = 0
        for (base, count), size in zip(pieces, rows):
            values = first(*(packed[pl.ds(base + 2 + s, count), own_y] for s in (-2, -1, 1, 2)))
            keep_split(dx_split, values.reshape(size, 128), at)
            at += size
        total = at

        def one(n, carry):
            values = [slope[n, pl.ds(base, count), own_y].reshape(size, 128) for (base, count), size in zip(pieces, rows)]
            both = along_z(jnp.concatenate(values, 0), dx_split[:, :total], weights[n, :, :128])
            at = 0
            for (base, count), size in zip(pieces, rows):
                xz_two[n, pl.ds(base, count)] = both[at : at + size].reshape(count, cy, 128)
                at += size
            return carry

        lax.fori_loop(0, GEO, one, 0, unroll=7)

    def tile_at(x, y, whole):
        rows = pl.ds(pl.multiple_of(y, 8), 8)
        ham, momentum = cell_math(
            lambda f, sx, sy: cells[f, x + 2 + sx, pl.ds(TOP + y + sy, 8)],
            lambda n, sy: slope[n, x, pl.ds(TOP + y + sy, 8)],
            lambda n: y_one[n, x, rows],
            lambda n: z_one[n, x, rows],
            lambda n: z_two[n, x, rows],
            lambda n: xz_two[n, x, rows],
            lambda n: yz_two[n, x, rows],
            whole,
        )
        ham_out[x, rows] = ham
        for i in range(3):
            mom_out[i, x, rows] = momentum[i]
        if whole:
            sums[0] += ham * ham
            sums[1] += momentum[0] * momentum[0] + momentum[1] * momentum[1] + momentum[2] * momentum[2]

    def rims(pieces):
        def one(n, carry):
            for base, count in pieces:
                for rows in (pl.ds(TOP - 8, 8), pl.ds(TOP + cy, 8)):
                    slope[n, pl.ds(base, count), rows] = first(
                        *(cells[n + CHI, pl.ds(base + 2 + s, count), rows] for s in (-2, -1, 1, 2))
                    )
            return carry

        lax.fori_loop(0, GEO, one, 0, unroll=7)

    def outer_x(at):
        return at + at // 2 * (cx - 4)

    def run(layers, layer, count, row, whole):
        def one(n, carry):
            tile_at(layer(n // count), row(lax.rem(n, count)), whole)
            return carry

        lax.fori_loop(0, layers * count, one, 0)

    inner = (cx - 4, lambda at: at + 2)
    outer = (4, outer_x)
    every = (tiles, lambda at: 8 * at)
    middle = (tiles - 2, lambda at: 8 * at + 8)
    rim = (2, lambda at: at * (cy - 8))
    rises(((8, cy - 16),))
    climbs(((2, cx - 4),), (0, GEO))
    slopes(((2, cx - 4),))
    run(*inner, *middle, True)
    wait_for(Y_GEO)
    wait_for(Y_PACK)
    rises(((0, 8), (cy - 8, 8)))
    rims(((2, cx - 4),))
    wait_for(Y_REST)
    run(*inner, *rim, True)

    def offer(side, far, near, at, behind, sign):
        def one(t, carry):
            rows = pl.ds(pl.multiple_of(TOP + t * 8, 8), 8)
            out_rows = pl.ds(pl.multiple_of(t * 8, 8), 8)
            edge = [cells[CURV + n, at, rows] * sign for n in range(7)]
            second_edge = [cells[CURV + n, behind, rows] * sign for n in range(7)]
            for place, slot, values in (
                (near, 1 - side, [8.0 * a - b for a, b in zip(edge, second_edge)]),
                (far, side, [-a for a in edge]),
            ):
                gu = inverse([cells[MET + n, place, rows] for n in range(6)])
                for i in range(3):
                    value = total_of(sym(gu, 0, k) * sym(values, k, i) for k in range(3))
                    if i == 0:
                        value = value - (2.0 / 3.0) * values[6]
                    part_out[side, i, slot, out_rows] = value * (1.0 / 12.0)
            return carry

        lax.fori_loop(0, tiles, one, 0)

    def offer_back():
        wait_for(X_MET)
        offer(0, 0, 1, 2, 3, 1.0)
        send(part_out.at[0], part.at[:, pl.ds(2, 2)], PART, 0, -1)

    def offer_ahead():
        wait_for(X_MET_BACK)
        offer(1, cx + 3, cx + 2, cx + 1, cx, -1.0)
        send(part_out.at[1], part.at[:, pl.ds(0, 2)], PART, 0, 1)

    each_way(0, offer_ahead, offer_back)

    def relay(n, fields, sliced, unroll):
        for layers in (before_x, after_x):
            send_y(sliced, EDGE_Y, layers)
        packing(fields, edge_own.at[n], lambda at: at + at // 2 * cx, unroll)
        send_z(edge_own.at[n], lambda side: edge_in.at[side, n], EDGE_Z)

    ends = ((0, 2), (cx - 2, 2))
    relay(0, (None,) + tuple(range(MET, CURV)), pl.ds(MET, 6), 4)
    climbs(ends, (1, GEO))
    wait_for(X_CHI)
    relay(1, (CHI,), pl.ds(CHI, 1), 4)
    climbs(ends, (0, 1))
    run(*outer, *every, False)
    wait_for(EDGE_Z)
    for at in range(4):
        packed[at + at // 2 * cx, own_y] = joined(lambda side: edge_in[side, 0, at] + edge_in[side, 1, at])
    slopes(ends)
    wait_for(EDGE_Y)
    rims(ends)
    wait_for(X_GX)

    def mend(n, carry):
        x, y = outer_x(n // tiles), lax.rem(n, tiles) * 8
        rows = pl.ds(pl.multiple_of(y, 8), 8)
        here = pl.ds(pl.multiple_of(TOP + y, 8), 8)
        chi, *metric = [cells[CHI + k, x + 2, here] for k in range(GEO)]
        gu = inverse(metric)
        chi_part, *parts = [
            gu[1] * first(*(slope[k, x, pl.ds(TOP + y + s, 8)] for s in (-2, -1, 1, 2))) + gu[2] * xz_two[k, x, rows]
            for k in range(GEO)
        ]
        div = first(*(cells[GX, x + 2 + s, here] for s in (-2, -1, 1, 2)))
        ham = ham_out[x, rows] + (
            (4.0 * chi_part - chi * contract(gu, parts)) * (1.0 / 144.0) + chi * div * (1.0 / 12.0)
        )
        ham_out[x, rows] = ham
        sums[0] += ham * ham
        return carry

    lax.fori_loop(0, 4 * tiles, mend, 0, unroll=2)
    wait_for(PART)

    squares = []
    for at in range(4):
        x = outer_x(at)
        for i in range(3):
            momentum = mom_out[i, x] + part[i, at]
            mom_out[i, x] = momentum
            squares += [momentum[y : y + 8] * momentum[y : y + 8] for y in range(0, cy, 8)]
    sums[1] += total_of(squares)

    lane = lax.broadcasted_iota(jnp.int32, (8, 128), 1)
    folded = [sums[n] + pltpu.roll(sums[n], 64, 1) for n in range(2)]
    total = jnp.sum(jnp.where(lane < 64, folded[0], folded[1]), axis=0, keepdims=True)
    pl.semaphore_wait(ready, ny * nz - 1)
    axes = (0, 1, 2)
    here = pl.ds(place_in(axes), 1)
    slots[here] = total
    for step in sorted(hops(axes), key=lambda step: -sum(min(a, b - a) for a, b in zip(step, sizes))):
        send(slots.at[here], slots.at[here], NORM, axes, step)
    wait_for(NORM)
    total_out[...] = jnp.sum(slots[...], axis=0, keepdims=True)
    for n, ref in bulk.items():
        copy_to(ref, ref, n, 0, 1).wait_send()


def deliver(count, ham_in, mom_in, total_in, ham_out, mom_out, norm_out, norm, sems):
    copies = [
        pltpu.make_async_copy(mom_in, mom_out, sems.at[0]),
        pltpu.make_async_copy(ham_in, ham_out, sems.at[1]),
    ]
    for copy in copies:
        copy.start()
    total = total_in[...]
    lane = lax.broadcasted_iota(jnp.int32, total.shape, 1)
    for n, (part, cells) in enumerate(((lane < 64, count), (lane >= 64, 3.0 * count))):
        root = jnp.sqrt(jnp.sum(jnp.where(part, total, 0.0), axis=1, keepdims=True) * (1.0 / cells))
        norm[n] = root[0, 0]
    copies.append(pltpu.make_async_copy(norm, norm_out, sems.at[2]))
    copies[2].start()
    for copy in copies:
        copy.wait()


def on_device(chi_field, metric, curvature, trace_curvature, gamma_field):
    sizes = tuple(lax.axis_size(a) for a in ("gx", "gy", "gz"))
    cx, cy, cz = chi_field.shape
    dma = pltpu.SemaphoreType.DMA
    vmem = pl.BlockSpec(memory_space=pltpu.VMEM)
    block = (cx + 4, cy + 2 * TOP, cz)
    hbm = pl.BlockSpec(memory_space=pltpu.HBM)
    ham, momentum, total = pl.pallas_call(
        functools.partial(kernel, sizes),
        out_shape=(
            pltpu.VMEM(chi_field.shape, jnp.float32),
            pltpu.VMEM(gamma_field.shape, jnp.float32),
            pltpu.VMEM((1, 128), jnp.float32),
        ),
        in_specs=[pl.BlockSpec(memory_space=pltpu.HBM)] * 6,
        out_specs=(vmem, vmem, vmem),
        scratch_shapes=[
            pltpu.VMEM((17,) + block, jnp.float32),
            pltpu.VMEM(block, jnp.float32),
        ]
        + [pltpu.VMEM(shape + (cy, cz), jnp.float32) for shape in ((cx,), (2, cx), (2, 4), (2, 2, 4))]
        + [
            pltpu.VMEM((GEO, cx) + block[1:], jnp.float32),
            pltpu.VMEM((2, 8, 128), jnp.float32),
            pltpu.VMEM((2, 3, 2, cy, cz), jnp.float32),
            pltpu.VMEM((3, 4, cy, cz), jnp.float32),
            pltpu.VMEM((len(Z_FIELDS), 256, 256), jnp.bfloat16),
            pltpu.VMEM((len(Z_FIELDS), cx, cy, cz), jnp.float32),
        ]
        + [pltpu.VMEM((GEO, cx, cy, cz), jnp.float32)] * 4
        + [pltpu.VMEM((2, cx * cy, cz), jnp.bfloat16)] * 3
        + [pltpu.VMEM((np.prod(sizes), 128), jnp.float32), dma((4,)), dma((12,)), dma((12,))]
        + [pltpu.SemaphoreType.REGULAR],
        compiler_params=pltpu.CompilerParams(
            collective_id=0, has_side_effects=True, vmem_limit_bytes=67043328 - 16 * chi_field.size - 16384
        ),
    )(chi_field, metric, curvature, trace_curvature, gamma_field, jnp.asarray(z_weights(), jnp.bfloat16))
    count = float(chi_field.size * sizes[0] * sizes[1] * sizes[2])
    return pl.pallas_call(
        functools.partial(deliver, count),
        out_shape=(
            jax.ShapeDtypeStruct(chi_field.shape, jnp.float32),
            jax.ShapeDtypeStruct(gamma_field.shape, jnp.float32),
            jax.ShapeDtypeStruct((2,), jnp.float32),
        ),
        in_specs=[vmem, vmem, vmem],
        out_specs=(hbm, hbm, hbm),
        scratch_shapes=[pltpu.SMEM((2,), jnp.float32), pltpu.SemaphoreType.DMA((3,))],
    )(*(pltpu.with_memory_space_constraint(v, pltpu.VMEM) for v in (ham, momentum, total)))


def solution(mesh):
    return jax.shard_map(
        on_device,
        mesh=mesh,
        in_specs=(
            P("gx", "gy", "gz"),
            P(None, "gx", "gy", "gz"),
            P(None, "gx", "gy", "gz"),
            P("gx", "gy", "gz"),
            P(None, "gx", "gy", "gz"),
        ),
        out_specs=(P("gx", "gy", "gz"), P(None, "gx", "gy", "gz"), P()),
        check_vma=False,
    )
```

```python
import functools

import jax
import jax.numpy as jnp
import numpy as np
from jax import lax
from jax.experimental import pallas as pl
from jax.experimental.pallas import tpu as pltpu
from jax.sharding import PartitionSpec as P

pair_index = ((0, 1, 2), (1, 3, 4), (2, 4, 5))
MESH = pl.DeviceIdType.MESH
GX, CHI, MET, CURV, TRK, GY, GZ = 0, 1, 2, 8, 14, 15, 16
GEO = 7
X_MET, X_CHI, X_GX, Y_GEO, Y_REST, Y_PACK, Z_PACK, EDGE_Y, EDGE_Z, PART, NORM = range(11)
Z_FIELDS = tuple(range(CHI, GY)) + (GZ,)
TOP = 8


def first(m2, m1, p1, p2):
    return 8.0 * (p1 - m1) - (p2 - m2)


def second(m2, m1, c, p1, p2):
    return 16.0 * (p1 + m1) - (p2 + m2) - 30.0 * c


def total_of(terms):
    terms = list(terms)
    while len(terms) > 1:
        terms = [
            terms[n] + terms[n + 1] if n + 1 < len(terms) else terms[n]
            for n in range(0, len(terms), 2)
        ]
    return terms[0]


def sym(values, i, j):
    return values[pair_index[i][j]]


def contract(gu, values):
    return total_of(
        [gu[n] * values[n] for n in (0, 3, 5)]
        + [2.0 * total_of(gu[n] * values[n] for n in (1, 2, 4))]
    )


def z_weights():
    weights = np.zeros((len(Z_FIELDS), 256, 256), np.float32)
    for n in range(len(Z_FIELDS)):
        for z in range(128):
            for step, one, two in ((-2, 1, -1), (-1, -8, 16), (0, 0, -30), (1, 8, 16), (2, -1, -1)):
                at = z + step
                row = at if 0 <= at < 128 else 128 + 4 * n + (at + 2 if at < 0 else at - 126)
                weights[n, row, z] = one
                weights[n, row, 128 + z] = two
    return weights


def split(value):
    high = value.astype(jnp.bfloat16)
    return high, (value - high.astype(jnp.float32)).astype(jnp.bfloat16)


def along_z(value, packed, weights):
    parts = [jnp.concatenate([a, b], 1) for a, b in zip(split(value), packed)]
    return sum(jnp.dot(part, weights, preferred_element_type=jnp.float32) for part in parts)


def inverse(metric):
    g00, g01, g02, g11, g12, g22 = metric
    m00 = g11 * g22 - g12 * g12
    m01 = g02 * g12 - g01 * g22
    m02 = g01 * g12 - g02 * g11
    m11 = g00 * g22 - g02 * g02
    m12 = g01 * g02 - g00 * g12
    m22 = g00 * g11 - g01 * g01
    scale = 1.0 / (g00 * m00 + g01 * m01 + g02 * m02)
    return [m * scale for m in (m00, m01, m02, m11, m12, m22)]


def cell_math(load, load_dx, load_dy, load_z, load_zz, load_xz, load_yz, whole):
    zpos = {f: n for n, f in enumerate(Z_FIELDS)}
    gu = inverse([load(MET + n, 0, 0) for n in range(6)])
    gu_hess = [12.0 * gu[n] if n in (0, 3, 5) else 2.0 * gu[n] for n in range(6)]

    def geo(f):
        c = load(f, 0, 0)
        xs = [load(f, s, 0) for s in (-2, -1, 1, 2)]
        ys = [load(f, 0, s) for s in (-2, -1, 1, 2)]
        n = zpos[f]
        dx = load_dx(n, 0)
        dy, dz = load_dy(n), load_z(n)
        dxx = second(xs[0], xs[1], c, xs[2], xs[3])
        dyy = second(ys[0], ys[1], c, ys[2], ys[3])
        hess = {0: dxx, 3: dyy, 4: load_yz(n), 5: load_zz(n)}
        if whole:
            hess[1] = first(*(load_dx(n, s) for s in (-2, -1, 1, 2)))
            hess[2] = load_xz(n)
        return (dx, dy, dz), total_of(gu_hess[k] * hess[k] for k in sorted(hess))

    chi = load(CHI, 0, 0)
    dchi, chi_box = geo(CHI)
    grads = [[None] * 6 for _ in range(3)]
    boxes = []
    for n in range(6):
        d, box = geo(MET + n)
        for a in range(3):
            grads[a][n] = d[a]
        boxes.append(box)
    metric_box = contract(gu, boxes)

    raised = [
        [[total_of(sym(gu, b, l) * sym(grads[k], l, j) for l in range(3)) for j in range(3)] for b in range(3)]
        for k in range(3)
    ]
    trace = [raised[k][0][0] + raised[k][1][1] + raised[k][2][2] for k in range(3)]
    lower = [
        raised[0][0][l] + raised[1][1][l] + raised[2][2][l] - 0.5 * trace[l] for l in range(3)
    ]
    gd = [total_of(sym(gu, k, l) * lower[l] for l in range(3)) for k in range(3)]

    def trace_of(k, l):
        return total_of(raised[k][a][b] * raised[l][b][a] for a in range(3) for b in range(3))

    square = contract(gu, [trace_of(k, l) for k in range(3) for l in range(k, 3)])

    def cross_of(k, b):
        left, right = raised[k][b], raised[b][k]
        up = [total_of(sym(gu, c, j) * right[j] for j in range(3)) for c in range(3)]
        return total_of(left[c] * up[c] for c in range(3))

    cross = (
        cross_of(0, 0)
        + cross_of(1, 1)
        + cross_of(2, 2)
        + 2.0 * (cross_of(0, 1) + cross_of(0, 2) + cross_of(1, 2))
    )
    chi_up = [total_of(sym(gu, k, l) * dchi[l] for l in range(3)) for k in range(3)]
    grad_sq = total_of(chi_up[k] * dchi[k] for k in range(3))
    laplace = chi_box - total_of(gd[k] * dchi[k] for k in range(3))
    drift = total_of(gd[k] * trace[k] for k in range(3))

    def dx_of(f):
        return first(*(load(f, s, 0) for s in (-2, -1, 1, 2)))

    def dy_of(f):
        return first(*(load(f, 0, s) for s in (-2, -1, 1, 2)))

    def dz_of(f):
        return load_z(zpos[f])

    div = dy_of(GY) + dz_of(GZ)
    if whole:
        div = dx_of(GX) + div
    inv_chi = 1.0 / chi
    curv = [load(CURV + n, 0, 0) for n in range(6)]
    mixed = [
        [total_of(sym(curv, i, k) * sym(gu, k, j) for k in range(3)) for j in range(3)] for i in range(3)
    ]
    curv_up = [
        total_of(sym(gu, i, a) * mixed[a][j] for a in range(3)) for i in range(3) for j in range(i, 3)
    ]
    curv_sq = contract(curv, curv_up)
    trk = load(TRK, 0, 0)
    ham = (
        chi * ((0.25 * square + 0.5 * (cross + drift - metric_box)) * (1.0 / 144.0) + div * (1.0 / 12.0))
        + (2.0 * laplace - 2.5 * grad_sq * inv_chi) * (1.0 / 144.0)
        + (2.0 / 3.0) * trk * trk
        - curv_sq
    )
    push = [gd[l] + 1.5 * inv_chi * chi_up[l] for l in range(3)]
    curv_grads = [[op(CURV + n) for n in range(6)] for op in (dx_of, dy_of, dz_of)]
    trace_grads = [op(TRK) for op in (dx_of, dy_of, dz_of)]
    momentum = []
    for i in range(3):
        parts = total_of(sym(gu, j, k) * sym(curv_grads[j], k, i) for j in range(3) for k in range(3))
        parts = parts - total_of(sym(curv, l, i) * push[l] for l in range(3))
        parts = parts - 0.5 * contract(curv_up, grads[i]) - (2.0 / 3.0) * trace_grads[i]
        momentum.append(parts * (1.0 / 12.0))
    return ham, momentum


def kernel(
    sizes,
    chi_in, met_in, curv_in, trk_in, gam_in, weights_in,
    ham_out, mom_out, total_out,
    cells, packed, pack_own, pack_in, edge_own, edge_in, slope, sums,
    part_out, part, weights, z_one, z_two, y_one, yz_two, xz_two, mid_split, dy_split, dx_split,
    slots, load_sem, sent, got, ready,
):
    nx, ny, nz = sizes
    cx, cy = chi_in.shape[0], chi_in.shape[1]
    names = ("gx", "gy", "gz")
    me = [lax.axis_index(a) for a in names]

    def moved(axis, step):
        return lax.rem(me[axis] + step + sizes[axis], sizes[axis])

    def peer(axes, steps):
        where = list(me)
        if isinstance(axes, int):
            axes, steps = (axes,), (steps,)
        for axis, step in zip(axes, steps):
            where[axis] = moved(axis, step)
        return tuple(where)

    def hops(axes):
        return [step for step in np.ndindex(*(sizes[a] for a in axes)) if any(step)]

    def place_in(axes, steps=None):
        index = 0
        for axis, step in zip(axes, steps or (0,) * len(axes)):
            index = index * sizes[axis] + moved(axis, step)
        return index

    own_x, own_y = pl.ds(2, cx), pl.ds(TOP, cy)
    loads = [
        pltpu.make_async_copy(src, dst, load_sem.at[n])
        for n, src, dst in (
            (0, met_in, cells.at[pl.ds(MET, 6), own_x, own_y]),
            (1, chi_in, cells.at[CHI, own_x, own_y]),
            (1, gam_in.at[0], cells.at[GX, own_x, own_y]),
            (2, curv_in, cells.at[pl.ds(CURV, 6), own_x, own_y]),
            (2, trk_in, cells.at[TRK, own_x, own_y]),
            (2, gam_in.at[pl.ds(1, 2)], cells.at[pl.ds(GY, 2), own_x, own_y]),
            (3, weights_in, weights),
        )
    ]
    for copy in loads[:6]:
        copy.start()
    barrier = pltpu.get_barrier_semaphore()
    for axes in ((1, 2), (0,)):
        for step in hops(axes):
            pl.semaphore_signal(barrier, inc=1, device_id=peer(axes, step), device_id_type=MESH)
    pl.semaphore_wait(barrier, ny * nz + nx - 2)

    for step in hops((1, 2)):
        pl.semaphore_signal(ready, inc=1, device_id=peer((1, 2), step), device_id_type=MESH)

    def loaded(n, ref):
        pltpu.make_async_copy(ref, ref, load_sem.at[n]).wait()

    def copy_to(src, dst, n, axes, step):
        return pltpu.make_async_remote_copy(
            src_ref=src, dst_ref=dst, send_sem=sent.at[n], recv_sem=got.at[n],
            device_id=peer(axes, step), device_id_type=MESH,
        )

    def send(src, dst, n, axes, step):
        copy_to(src, dst, n, axes, step).start()

    low_x, high_x = pl.ds(2, 2), pl.ds(cx, 2)
    before_x, after_x = pl.ds(0, 2), pl.ds(cx + 2, 2)
    low_y, high_y = pl.ds(TOP, 2), pl.ds(TOP + cy - 2, 2)
    before_y, after_y = pl.ds(TOP - 2, 2), pl.ds(TOP + cy, 2)
    geo = pl.ds(CHI, GEO)
    several = nz > 2
    bulk = {
        X_MET: cells.at[pl.ds(MET, 6), pl.ds(0, 4), own_y],
        X_CHI: cells.at[pl.ds(CHI, 1), pl.ds(0, 4), own_y],
        X_GX: cells.at[pl.ds(GX, 1), pl.ds(0, 4), own_y],
        Y_GEO: cells.at[geo, own_x, pl.ds(0, 4)],
        Y_REST: cells.at[pl.ds(CURV, 8), own_x, pl.ds(0, 4)],
        Y_PACK: packed.at[own_x, pl.ds(0, 4)],
        Z_PACK: pack_in if several else pack_in.at[0],
        EDGE_Y: cells.at[geo, pl.ds(0, 4), pl.ds(0, 4)],
        EDGE_Z: edge_in if several else edge_in.at[0],
        PART: part,
        NORM: slots.at[pl.ds(0, nx * ny * nz - 1)],
    }

    def wait_for(n):
        copy_to(bulk[n], bulk[n], n, 0, 1).wait_recv()

    def each_way(axis, ahead, back):
        odd = lax.rem(me[axis], 2) == 1

        @pl.when(odd)
        def _():
            ahead()
            back()

        @pl.when(jnp.logical_not(odd))
        def _():
            back()
            ahead()

    def send_x(fields, n):
        each_way(
            0,
            lambda: send(cells.at[fields, high_x, own_y], cells.at[fields, before_x, own_y], n, 0, 1),
            lambda: send(cells.at[fields, low_x, own_y], cells.at[fields, after_x, own_y], n, 0, -1),
        )

    def send_y(fields, n, layers=own_x):
        each_way(
            1,
            lambda: send(cells.at[fields, layers, high_y], cells.at[fields, layers, before_y], n, 1, 1),
            lambda: send(cells.at[fields, layers, low_y], cells.at[fields, layers, after_y], n, 1, -1),
        )

    loaded(0, cells.at[pl.ds(MET, 6), own_x, own_y])
    send_x(pl.ds(MET, 6), X_MET)
    loaded(1, cells.at[pl.ds(GX, 2), own_x, own_y])
    send_x(pl.ds(CHI, 1), X_CHI)
    send_y(geo, Y_GEO)
    send_x(pl.ds(GX, 1), X_GX)
    loaded(2, cells.at[pl.ds(CURV, 9), own_x, own_y])
    send_y(pl.ds(CURV, 8), Y_REST)
    loads[6].start()

    tiles = cy // 8
    group = lax.shift_right_logical(lax.broadcasted_iota(jnp.int32, (8, 128), 1), 2)
    far_side = (lax.broadcasted_iota(jnp.int32, (cy, 128), 1) & 2) != 0

    def packing(fields, target, layer, unroll):
        def pack(step, carry):
            at, y = step // tiles, lax.rem(step, tiles) * 8
            rows = pl.ds(pl.multiple_of(TOP + y, 8), 8)
            x = layer(at)
            picked = [
                jnp.where(group == n, pltpu.roll(cells[f, x, rows], 4 * n + 2, 1), 0.0)
                for n, f in enumerate(fields)
                if f is not None
            ]
            target[at, pl.ds(pl.multiple_of(y, 8), 8)] = total_of(picked)
            return carry

        lax.fori_loop(0, target.shape[0] * tiles, pack, 0, unroll=unroll)

    packing(Z_FIELDS, pack_own, lambda at: at + 2, 4)

    def send_z(own, target, n):
        send(own, target(0), n, 2, 1)
        if several:
            send(own, target(1), n, 2, -1)

    def joined(both):
        return jnp.where(far_side, both(1), both(0)) if several else both(0)

    send_z(pack_own, lambda side: pack_in.at[side], Z_PACK)
    sums[...] = jnp.zeros_like(sums)
    missing = jnp.zeros((7, 2, cy, 128), jnp.float32)
    cells[pl.ds(CURV, 7), before_x, own_y] = missing
    cells[pl.ds(CURV, 7), after_x, own_y] = missing
    wait_for(Z_PACK)

    def keep_split(target, value, at=0):
        for n, half in enumerate(split(value)):
            target[n, pl.ds(at, value.shape[0])] = half

    def merge(x, carry):
        value = joined(lambda side: pack_in[side, x])
        packed[x + 2, own_y] = value
        keep_split(mid_split, value, pl.multiple_of(x * cy, cy))
        return carry

    lax.fori_loop(0, cx, merge, 0)
    send(packed.at[own_x, high_y], packed.at[own_x, before_y], Y_PACK, 1, 1)
    send(packed.at[own_x, low_y], packed.at[own_x, after_y], Y_PACK, 1, -1)
    loads[6].wait()
    flat = (cx * cy, 128)

    def geo_z(n, carry):
        both = along_z(cells[n + CHI, own_x, own_y].reshape(flat), mid_split[...], weights[n])
        z_one[n] = both[:, :128].reshape(cx, cy, 128)
        z_two[n] = both[:, 128:].reshape(cx, cy, 128)
        return carry

    lax.fori_loop(0, GEO, geo_z, 0, unroll=7)

    def rest_z(n, carry):
        f = n + CHI + n // (GY - CHI)
        z_one[n] = along_z(
            cells[f, own_x, own_y].reshape(flat), mid_split[...], weights[n, :, :128]
        ).reshape(cx, cy, 128)
        return carry

    lax.fori_loop(GEO, len(Z_FIELDS), rest_z, 0, unroll=8)

    def rises(pieces):
        rows = [cx * count for _, count in pieces]
        at = 0
        for (row, count), size in zip(pieces, rows):
            values = first(*(packed[own_x, pl.ds(TOP + row + s, count)] for s in (-2, -1, 1, 2)))
            keep_split(dy_split, values.reshape(size, 128), at)
            at += size
        total = at

        def one(n, carry):
            values = []
            for (row, count), size in zip(pieces, rows):
                dy = first(*(cells[n + CHI, own_x, pl.ds(TOP + row + s, count)] for s in (-2, -1, 1, 2)))
                y_one[n, :, pl.ds(row, count)] = dy
                values.append(dy.reshape(size, 128))
            both = along_z(jnp.concatenate(values, 0), dy_split[:, :total], weights[n, :, :128])
            at = 0
            for (row, count), size in zip(pieces, rows):
                yz_two[n, :, pl.ds(row, count)] = both[at : at + size].reshape(cx, count, 128)
                at += size
            return carry

        lax.fori_loop(0, GEO, one, 0, unroll=7)

    def climbs(pieces, fields):
        def one(n, carry):
            for base, count in pieces:
                slope[n, pl.ds(base, count), own_y] = first(
                    *(cells[n + CHI, pl.ds(base + 2 + s, count), own_y] for s in (-2, -1, 1, 2))
                )
            return carry

        lax.fori_loop(*fields, one, 0, unroll=fields[1] - fields[0])

    def slopes(pieces):
        rows = [count * cy for _, count in pieces]
        at = 0
        for (base, count), size in zip(pieces, rows):
            values = first(*(packed[pl.ds(base + 2 + s, count), own_y] for s in (-2, -1, 1, 2)))
            keep_split(dx_split, values.reshape(size, 128), at)
            at += size
        total = at

        def one(n, carry):
            values = [slope[n, pl.ds(base, count), own_y].reshape(size, 128) for (base, count), size in zip(pieces, rows)]
            both = along_z(jnp.concatenate(values, 0), dx_split[:, :total], weights[n, :, :128])
            at = 0
            for (base, count), size in zip(pieces, rows):
                xz_two[n, pl.ds(base, count)] = both[at : at + size].reshape(count, cy, 128)
                at += size
            return carry

        lax.fori_loop(0, GEO, one, 0, unroll=7)

    def tile_at(x, y, whole):
        rows = pl.ds(pl.multiple_of(y, 8), 8)
        ham, momentum = cell_math(
            lambda f, sx, sy: cells[f, x + 2 + sx, pl.ds(TOP + y + sy, 8)],
            lambda n, sy: slope[n, x, pl.ds(TOP + y + sy, 8)],
            lambda n: y_one[n, x, rows],
            lambda n: z_one[n, x, rows],
            lambda n: z_two[n, x, rows],
            lambda n: xz_two[n, x, rows],
            lambda n: yz_two[n, x, rows],
            whole,
        )
        ham_out[x, rows] = ham
        for i in range(3):
            mom_out[i, x, rows] = momentum[i]
        if whole:
            sums[0] += ham * ham
            sums[1] += momentum[0] * momentum[0] + momentum[1] * momentum[1] + momentum[2] * momentum[2]

    def rims(pieces):
        def one(n, carry):
            for base, count in pieces:
                for rows in (pl.ds(TOP - 8, 8), pl.ds(TOP + cy, 8)):
                    slope[n, pl.ds(base, count), rows] = first(
                        *(cells[n + CHI, pl.ds(base + 2 + s, count), rows] for s in (-2, -1, 1, 2))
                    )
            return carry

        lax.fori_loop(0, GEO, one, 0, unroll=7)

    def outer_x(at):
        return at + at // 2 * (cx - 4)

    def run(layers, layer, count, row, whole):
        def one(n, carry):
            tile_at(layer(n // count), row(lax.rem(n, count)), whole)
            return carry

        lax.fori_loop(0, layers * count, one, 0)

    inner = (cx - 4, lambda at: at + 2)
    outer = (4, outer_x)
    every = (tiles, lambda at: 8 * at)
    middle = (tiles - 2, lambda at: 8 * at + 8)
    rim = (2, lambda at: at * (cy - 8))
    rises(((8, cy - 16),))
    climbs(((2, cx - 4),), (0, GEO))
    slopes(((2, cx - 4),))
    run(*inner, *middle, True)
    wait_for(Y_GEO)
    wait_for(Y_PACK)
    rises(((0, 8), (cy - 8, 8)))
    rims(((2, cx - 4),))
    wait_for(Y_REST)
    run(*inner, *rim, True)
    wait_for(X_MET)

    def offer(t, carry):
        rows = pl.ds(pl.multiple_of(TOP + t * 8, 8), 8)
        out_rows = pl.ds(pl.multiple_of(t * 8, 8), 8)
        for side, far, near, at, behind, sign in ((0, 0, 1, 2, 3, 1.0), (1, cx + 3, cx + 2, cx + 1, cx, -1.0)):
            edge = [cells[CURV + n, at, rows] * sign for n in range(7)]
            second_edge = [cells[CURV + n, behind, rows] * sign for n in range(7)]
            for place, slot, values in (
                (near, 1 - side, [8.0 * a - b for a, b in zip(edge, second_edge)]),
                (far, side, [-a for a in edge]),
            ):
                gu = inverse([cells[MET + n, place, rows] for n in range(6)])
                for i in range(3):
                    value = total_of(sym(gu, 0, k) * sym(values, k, i) for k in range(3))
                    if i == 0:
                        value = value - (2.0 / 3.0) * values[6]
                    part_out[side, i, slot, out_rows] = value * (1.0 / 12.0)
        return carry

    lax.fori_loop(0, tiles, offer, 0)
    each_way(
        0,
        lambda: send(part_out.at[1], part.at[:, pl.ds(0, 2)], PART, 0, 1),
        lambda: send(part_out.at[0], part.at[:, pl.ds(2, 2)], PART, 0, -1),
    )

    def relay(n, fields, sliced, unroll):
        for layers in (before_x, after_x):
            send_y(sliced, EDGE_Y, layers)
        packing(fields, edge_own.at[n], lambda at: at + at // 2 * cx, unroll)
        send_z(edge_own.at[n], lambda side: edge_in.at[side, n], EDGE_Z)

    ends = ((0, 2), (cx - 2, 2))
    relay(0, (None,) + tuple(range(MET, CURV)), pl.ds(MET, 6), 4)
    climbs(ends, (1, GEO))
    wait_for(X_CHI)
    relay(1, (CHI,), pl.ds(CHI, 1), 4)
    climbs(ends, (0, 1))
    run(*outer, *every, False)
    wait_for(EDGE_Z)
    for at in range(4):
        packed[at + at // 2 * cx, own_y] = joined(lambda side: edge_in[side, 0, at] + edge_in[side, 1, at])
    slopes(ends)
    wait_for(EDGE_Y)
    rims(ends)
    wait_for(X_GX)

    def mend(n, carry):
        x, y = outer_x(n // tiles), lax.rem(n, tiles) * 8
        rows = pl.ds(pl.multiple_of(y, 8), 8)
        here = pl.ds(pl.multiple_of(TOP + y, 8), 8)
        chi, *metric = [cells[CHI + k, x + 2, here] for k in range(GEO)]
        gu = inverse(metric)
        chi_part, *parts = [
            gu[1] * first(*(slope[k, x, pl.ds(TOP + y + s, 8)] for s in (-2, -1, 1, 2))) + gu[2] * xz_two[k, x, rows]
            for k in range(GEO)
        ]
        div = first(*(cells[GX, x + 2 + s, here] for s in (-2, -1, 1, 2)))
        ham = ham_out[x, rows] + (
            (4.0 * chi_part - chi * contract(gu, parts)) * (1.0 / 144.0) + chi * div * (1.0 / 12.0)
        )
        ham_out[x, rows] = ham
        sums[0] += ham * ham
        return carry

    lax.fori_loop(0, 4 * tiles, mend, 0, unroll=2)
    lane = lax.broadcasted_iota(jnp.int32, (8, 128), 1)

    def folded(value):
        return value + pltpu.roll(value, 64, 1)

    ham_sum = jnp.where(lane < 64, folded(sums[0]), 0.0)
    pl.semaphore_wait(ready, ny * nz - 1)
    wait_for(PART)

    squares = []
    for at in range(4):
        x = outer_x(at)
        for i in range(3):
            momentum = mom_out[i, x] + part[i, at]
            mom_out[i, x] = momentum
            squares += [momentum[y : y + 8] * momentum[y : y + 8] for y in range(0, cy, 8)]

    mom_sum = folded(sums[1] + total_of(squares))
    total = jnp.sum(jnp.where(lane < 64, ham_sum, mom_sum), axis=0, keepdims=True)
    axes = (0, 1, 2)
    here = pl.ds(place_in(axes), 1)
    slots[here] = total
    for step in sorted(hops(axes), key=lambda step: -sum(min(a, b - a) for a, b in zip(step, sizes))):
        send(slots.at[here], slots.at[here], NORM, axes, step)
    wait_for(NORM)
    total_out[...] = jnp.sum(slots[...], axis=0, keepdims=True)
    for n, ref in bulk.items():
        copy_to(ref, ref, n, 0, 1).wait_send()


def deliver(count, ham_in, mom_in, total_in, ham_out, mom_out, norm_out, norm, sems):
    copies = [
        pltpu.make_async_copy(mom_in, mom_out, sems.at[0]),
        pltpu.make_async_copy(ham_in, ham_out, sems.at[1]),
    ]
    for copy in copies:
        copy.start()
    total = total_in[...]
    lane = lax.broadcasted_iota(jnp.int32, total.shape, 1)
    for n, (part, cells) in enumerate(((lane < 64, count), (lane >= 64, 3.0 * count))):
        root = jnp.sqrt(jnp.sum(jnp.where(part, total, 0.0), axis=1, keepdims=True) * (1.0 / cells))
        norm[n] = root[0, 0]
    copies.append(pltpu.make_async_copy(norm, norm_out, sems.at[2]))
    copies[2].start()
    for copy in copies:
        copy.wait()


def on_device(chi_field, metric, curvature, trace_curvature, gamma_field):
    sizes = tuple(lax.axis_size(a) for a in ("gx", "gy", "gz"))
    cx, cy, cz = chi_field.shape
    dma = pltpu.SemaphoreType.DMA
    vmem = pl.BlockSpec(memory_space=pltpu.VMEM)
    block = (cx + 4, cy + 2 * TOP, cz)
    hbm = pl.BlockSpec(memory_space=pltpu.HBM)
    ham, momentum, total = pl.pallas_call(
        functools.partial(kernel, sizes),
        out_shape=(
            pltpu.VMEM(chi_field.shape, jnp.float32),
            pltpu.VMEM(gamma_field.shape, jnp.float32),
            pltpu.VMEM((1, 128), jnp.float32),
        ),
        in_specs=[pl.BlockSpec(memory_space=pltpu.HBM)] * 6,
        out_specs=(vmem, vmem, vmem),
        scratch_shapes=[
            pltpu.VMEM((17,) + block, jnp.float32),
            pltpu.VMEM(block, jnp.float32),
        ]
        + [pltpu.VMEM(shape + (cy, cz), jnp.float32) for shape in ((cx,), (2, cx), (2, 4), (2, 2, 4))]
        + [
            pltpu.VMEM((GEO, cx) + block[1:], jnp.float32),
            pltpu.VMEM((2, 8, 128), jnp.float32),
            pltpu.VMEM((2, 3, 2, cy, cz), jnp.float32),
            pltpu.VMEM((3, 4, cy, cz), jnp.float32),
            pltpu.VMEM((len(Z_FIELDS), 256, 256), jnp.bfloat16),
            pltpu.VMEM((len(Z_FIELDS), cx, cy, cz), jnp.float32),
        ]
        + [pltpu.VMEM((GEO, cx, cy, cz), jnp.float32)] * 4
        + [pltpu.VMEM((2, cx * cy, cz), jnp.bfloat16)] * 3
        + [pltpu.VMEM((np.prod(sizes), 128), jnp.float32), dma((4,)), dma((11,)), dma((11,))]
        + [pltpu.SemaphoreType.REGULAR],
        compiler_params=pltpu.CompilerParams(
            collective_id=0, has_side_effects=True, vmem_limit_bytes=67043328 - 16 * chi_field.size - 16384
        ),
    )(chi_field, metric, curvature, trace_curvature, gamma_field, jnp.asarray(z_weights(), jnp.bfloat16))
    count = float(chi_field.size * sizes[0] * sizes[1] * sizes[2])
    return pl.pallas_call(
        functools.partial(deliver, count),
        out_shape=(
            jax.ShapeDtypeStruct(chi_field.shape, jnp.float32),
            jax.ShapeDtypeStruct(gamma_field.shape, jnp.float32),
            jax.ShapeDtypeStruct((2,), jnp.float32),
        ),
        in_specs=[vmem, vmem, vmem],
        out_specs=(hbm, hbm, hbm),
        scratch_shapes=[pltpu.SMEM((2,), jnp.float32), pltpu.SemaphoreType.DMA((3,))],
    )(*(pltpu.with_memory_space_constraint(v, pltpu.VMEM) for v in (ham, momentum, total)))


def solution(mesh):
    return jax.shard_map(
        on_device,
        mesh=mesh,
        in_specs=(
            P("gx", "gy", "gz"),
            P(None, "gx", "gy", "gz"),
            P(None, "gx", "gy", "gz"),
            P("gx", "gy", "gz"),
            P(None, "gx", "gy", "gz"),
        ),
        out_specs=(P("gx", "gy", "gz"), P(None, "gx", "gy", "gz"), P()),
        check_vma=False,
    )
```
